8 devices in a mesh: dp: 8 (over z, y, x, core).
Axes of the slice: x: 2, y: 2, z: 1, core: 2. Of those that a mesh axis runs over, the one named last changes fastest.
Arguments:
- tokens: bfloat16 [2048, 512], P('dp')
- w_one: bfloat16 [512, 2048], replicated
- w_two: bfloat16 [2048, 512], replicated
- wi_one: bfloat16 [512, 2048], replicated
- wi_two: bfloat16 [2048, 512], replicated
- item_table: bfloat16 [262144, 512], P('dp')
- cand_ids: int32 [16384], replicated
- log_q: float32 [16384], replicated
- targets: int32 [2048], P('dp')
Outputs:
- output 1: float32 [], replicated
- output 2: float32 [262144, 512], P('dp')
- output 3: float32 [512, 2048], replicated
- output 4: float32 [2048, 512], replicated
- output 5: float32 [512, 2048], replicated
- output 6: float32 [2048, 512], replicated
All inputs are finite; a program needn't handle non-finite values.
Results may differ from the reference program's by a relative error of at most 0.011808.
Values are sent between devices in bfloat16 or wider.
A program may use at most 1 GiB of HBM per device.

```python
import math
import jax
import jax.numpy as jnp
from jax import lax

DIN = 512
FF = 2048
D = 512
FF2 = 2048
TOK_DEV = 256
CANDS = 16384
ROWS_DEV = 32768
DEVS = 8

TOKENS = TOK_DEV * DEVS
ROWS = ROWS_DEV * DEVS
HEAD_ROWS = 4 * CANDS
SCORE_GAIN = 3.0
HIT_VALUE = -1e9


def setup_inputs(seed: int = 0) -> dict:
    root_key = jax.random.key(seed)
    val_keys = jax.random.split(root_key, 7)
    tokens = jax.random.normal(val_keys[0], (TOKENS, DIN), jnp.float32).astype(jnp.bfloat16)
    w_one = (jax.random.normal(val_keys[1], (DIN, FF), jnp.float32) * DIN ** -0.5).astype(jnp.bfloat16)
    w_two = (jax.random.normal(val_keys[2], (FF, D), jnp.float32) * FF ** -0.5).astype(jnp.bfloat16)
    wi_one = (jax.random.normal(val_keys[3], (D, FF2), jnp.float32) * D ** -0.5).astype(jnp.bfloat16)
    wi_two = (jax.random.normal(val_keys[4], (FF2, D), jnp.float32) * FF2 ** -0.5).astype(jnp.bfloat16)
    item_table = jax.random.normal(val_keys[5], (ROWS, D), jnp.float32).astype(jnp.bfloat16)
    log_q = math.log(CANDS) + jax.random.uniform(val_keys[6], (CANDS,), jnp.float32, -3.0, 3.0)
    int_keys = jax.random.split(jax.random.fold_in(root_key, 1), 7)
    head_ids = jax.random.permutation(int_keys[0], HEAD_ROWS)[: CANDS // 2]
    tail_ids = HEAD_ROWS + jax.random.permutation(int_keys[1], ROWS - HEAD_ROWS)[: CANDS - CANDS // 2]
    cand_ids = jnp.concatenate([head_ids, tail_ids])[jax.random.permutation(int_keys[2], CANDS)].astype(jnp.int32)
    pick_mode = jax.random.randint(int_keys[3], (TOKENS,), 0, 4)
    from_cands = cand_ids[jax.random.randint(int_keys[4], (TOKENS,), 0, CANDS)]
    from_head = jax.random.randint(int_keys[5], (TOKENS,), 0, HEAD_ROWS)
    from_all = jax.random.randint(int_keys[6], (TOKENS,), 0, ROWS)
    targets = jnp.where(pick_mode == 0, from_cands, jnp.where(pick_mode == 1, from_head, from_all)).astype(jnp.int32)
    return {"tokens": tokens, "w_one": w_one, "w_two": w_two, "wi_one": wi_one, "wi_two": wi_two, "item_table": item_table, "cand_ids": cand_ids, "log_q": log_q, "targets": targets}


def tower_fwd(row_block, w_in, w_out):
    pre_act = jnp.dot(row_block, w_in, preferred_element_type=jnp.float32)
    hidden = jax.nn.gelu(pre_act).astype(jnp.bfloat16)
    tower_out = jnp.dot(hidden, w_out, preferred_element_type=jnp.float32).astype(jnp.bfloat16)
    return pre_act, hidden, tower_out


def tower_back(row_block, w_out, pre_act, hidden, grad_out):
    dw_out = jnp.dot(hidden.T, grad_out, preferred_element_type=jnp.float32)
    grad_hidden = jnp.dot(grad_out, w_out.T, preferred_element_type=jnp.float32)
    gelu_back = jax.vjp(jax.nn.gelu, pre_act)[1]
    grad_pre = gelu_back(grad_hidden)[0].astype(jnp.bfloat16)
    dw_in = jnp.dot(row_block.T, grad_pre, preferred_element_type=jnp.float32)
    return grad_pre, dw_in, dw_out


def reference(tokens, w_one, w_two, wi_one, wi_two, item_table, cand_ids, log_q, targets):
    logit_scale = SCORE_GAIN / math.sqrt(D)
    cand_raw = item_table[cand_ids]
    c_pre, c_hidden, cand_vec = tower_fwd(cand_raw, wi_one, wi_two)

    def block_step(carry, blk):
        loss_acc, dcand_acc, dw_one_acc, dw_two_acc, dwi_one_acc, dwi_two_acc = carry
        tok_blk, targ_blk = blk
        q_pre, q_hidden, query = tower_fwd(tok_blk, w_one, w_two)
        targ_raw = item_table[targ_blk]
        t_pre, t_hidden, targ_vec = tower_fwd(targ_raw, wi_one, wi_two)
        z_targ = jnp.sum(query.astype(jnp.float32) * targ_vec.astype(jnp.float32), axis=1) * logit_scale
        z_cand = jnp.dot(query, cand_vec.T, preferred_element_type=jnp.float32) * logit_scale - log_q[None, :]
        z_cand = jnp.where(targ_blk[:, None] == cand_ids[None, :], HIT_VALUE, z_cand)
        row_max = jnp.maximum(z_targ, jnp.max(z_cand, axis=1))
        e_targ = jnp.exp(z_targ - row_max)
        e_cand = jnp.exp(z_cand - row_max[:, None])
        denom_sum = e_targ + jnp.sum(e_cand, axis=1)
        loss_blk = jnp.sum(jnp.log(denom_sum) + row_max - z_targ)
        dz_targ = ((e_targ / denom_sum - 1.0) / TOKENS).astype(jnp.bfloat16).astype(jnp.float32)
        dz_cand = (e_cand / denom_sum[:, None] / TOKENS).astype(jnp.bfloat16)
        d_query = ((dz_targ[:, None] * targ_vec.astype(jnp.float32) + jnp.dot(dz_cand, cand_vec, preferred_element_type=jnp.float32)) * logit_scale).astype(jnp.bfloat16)
        d_targ_vec = (logit_scale * dz_targ[:, None] * query.astype(jnp.float32)).astype(jnp.bfloat16)
        dcand_new = dcand_acc + jnp.dot(dz_cand.T, query, preferred_element_type=jnp.float32)
        dw_one_blk, dw_two_blk = tower_back(tok_blk, w_two, q_pre, q_hidden, d_query)[1:]
        t_grad_pre, dwi_one_blk, dwi_two_blk = tower_back(targ_raw, wi_two, t_pre, t_hidden, d_targ_vec)
        d_targ_raw = jnp.dot(t_grad_pre, wi_one.T, preferred_element_type=jnp.float32).astype(jnp.bfloat16)
        new_carry = (loss_acc + loss_blk, dcand_new, dw_one_acc + dw_one_blk, dw_two_acc + dw_two_blk, dwi_one_acc + dwi_one_blk, dwi_two_acc + dwi_two_blk)
        return new_carry, d_targ_raw

    init_carry = (jnp.zeros((), jnp.float32), jnp.zeros((CANDS, D), jnp.float32), jnp.zeros((DIN, FF), jnp.float32), jnp.zeros((FF, D), jnp.float32), jnp.zeros((D, FF2), jnp.float32), jnp.zeros((FF2, D), jnp.float32))
    tok_blocks = tokens.reshape(DEVS, TOK_DEV, DIN)
    targ_blocks = targets.reshape(DEVS, TOK_DEV)
    final_carry, d_targ_rows = lax.scan(block_step, init_carry, (tok_blocks, targ_blocks))
    loss_acc, dcand_acc, dw_one, dw_two, dwi_one_t, dwi_two_t = final_carry
    d_cand_vec = (logit_scale * dcand_acc).astype(jnp.bfloat16)
    c_grad_pre, dwi_one_c, dwi_two_c = tower_back(cand_raw, wi_two, c_pre, c_hidden, d_cand_vec)
    d_cand_raw = jnp.dot(c_grad_pre, wi_one.T, preferred_element_type=jnp.float32).astype(jnp.bfloat16)
    row_grads = jnp.concatenate([d_cand_raw, d_targ_rows.reshape(TOKENS, D)]).astype(jnp.float32)
    row_ids = jnp.concatenate([cand_ids, targets])
    d_table = jax.ops.segment_sum(row_grads, row_ids, num_segments=ROWS)
    return loss_acc / TOKENS, d_table, dw_one, dw_two, dwi_one_t + dwi_one_c, dwi_two_t + dwi_two_c
```

```python
import functools
import math
import jax
import jax.numpy as jnp
from jax import lax
from jax.experimental import pallas as pl
from jax.experimental.pallas import tpu as pltpu
from jax.sharding import PartitionSpec as P

SCORE_GAIN = 3.0
HIT_VALUE = -1e9
EXCLUDED = 3e38
NO_ROW = -1e9
CH = 512
BLK = 512
WIN = 128
FB = 256
TB = 256
GELU_C = math.sqrt(2.0 / math.pi)
BF, F32 = jnp.bfloat16, jnp.float32
VMEM_LIMIT = 60 * 1024 * 1024


def dot(a, b):
    return lax.dot_general(a, b, (((1,), (0,)), ((), ())), preferred_element_type=F32)


def dot_nt(a, b):
    return lax.dot_general(a, b, (((1,), (1,)), ((), ())), preferred_element_type=F32)


def gelu_pair(x):
    sq = x * x
    th = jnp.tanh(x * (GELU_C + (GELU_C * 0.044715) * sq))
    half = 0.5 * x
    act = half + half * th
    slope = 0.5 + 0.5 * th + half * (1.0 - th * th) * (GELU_C + (3.0 * 0.044715 * GELU_C) * sq)
    return act, slope


def column(attr_ref, index, first, count):
    tiles = [attr_ref[first + i].T[:, index : index + 1] for i in range(count)]
    return jnp.concatenate(tiles, axis=0) if count > 1 else tiles[0]


def windows(starts_ref, blk):
    lo, hi = starts_ref[blk], starts_ref[blk + 1]
    first = lax.div(lo, WIN)
    return first, jnp.where(hi > lo, lax.div(lax.div(hi - 1, WIN) - first, 2) + 1, 0)


def gather_kernel(starts_ref, nch_ref, tbl_ref, attr_ref, rows_hbm, rows, sem):
    blk = pl.program_id(0)

    @pl.when(blk == 0)
    def _():
        def zero(i, carry):
            rows[pl.ds(pl.multiple_of(i * CH, CH), CH), :] = jnp.zeros((CH, rows.shape[1]), BF)
            return carry

        lax.fori_loop(0, nch_ref[0] + 1, zero, 0)

    first, count = windows(starts_ref, blk)
    lane_row = (lax.broadcasted_iota(jnp.int32, (2 * WIN, BLK), 1) + blk * BLK).astype(F32)

    def take(i, carry):
        tile = first + 2 * i
        pick = jnp.where(column(attr_ref, 0, tile, 2) == lane_row, 1.0, 0.0).astype(BF)
        at = pl.ds(pl.multiple_of(tile * WIN, WIN), 2 * WIN)
        rows[at, :] = rows[at, :] + dot(pick, tbl_ref[...]).astype(BF)
        return carry

    lax.fori_loop(0, count, take, 0)

    @pl.when(blk == pl.num_programs(0) - 1)
    def _():
        def copy(i):
            at = pl.ds(pl.multiple_of(i * CH, CH), CH)
            return pltpu.make_async_copy(rows.at[at, :], rows_hbm.at[at, :], sem)

        def start(i, carry):
            copy(i).start()
            return carry

        def wait(i, carry):
            copy(i).wait()
            return carry

        lax.fori_loop(0, nch_ref[0], start, 0)
        lax.fori_loop(0, nch_ref[0], wait, 0)


def stream(nch_ref, body, ins, outs):
    specs = [[spec for spec, _ in part] for part in (ins, outs)]
    pltpu.emit_pipeline(body, grid=(nch_ref[0],), in_specs=specs[0], out_specs=specs[1])(*[ref for _, ref in ins + outs])


def fwd_kernel(scale, nch_ref, tid_ref, h_ref, w1_ref, w2_ref, rows_hbm, attr_hbm, u_hbm, act_hbm, slope_hbm, z_hbm, stat_ref, m8, s8):
    m8[...] = jnp.full_like(m8, -EXCLUDED)
    s8[...] = jnp.zeros_like(s8)
    dim, ff, toks = rows_hbm.shape[1], w1_ref.shape[1], h_ref.shape[0]

    def body(rows_ref, attr_ref, u_ref, act_ref, slope_ref, z_ref):
        rows = rows_ref[...]
        out = None
        for f in range(0, ff, FB):
            act, slope = gelu_pair(dot(rows, w1_ref[:, f : f + FB]))
            act = act.astype(BF)
            act_ref[:, f : f + FB] = act
            slope_ref[:, f : f + FB] = slope
            part = dot(act, w2_ref[f : f + FB, :])
            out = part if out is None else out + part
        vec = out.astype(BF)
        u_ref[...] = vec
        loc = column(attr_ref, 0, 0, CH // WIN)
        off = column(attr_ref, 1, 0, CH // WIN)
        is_targ = column(attr_ref, 2, 0, CH // WIN) > 0.5
        for t in range(0, toks, TB):
            raw = dot_nt(vec, h_ref[t : t + TB, :]) * scale
            same = loc == tid_ref[:, t : t + TB]
            z = jnp.where(same, jnp.where(is_targ, raw, HIT_VALUE), raw - off)
            z_ref[:, t : t + TB] = z
            z3 = z.reshape(CH // 8, 8, TB)
            old = m8[:, t : t + TB]
            new = jnp.maximum(old, jnp.max(z3, axis=0))
            s8[:, t : t + TB] = s8[:, t : t + TB] * jnp.exp(old - new) + jnp.sum(jnp.exp(z3 - new[None]), axis=0)
            m8[:, t : t + TB] = new

    stream(nch_ref, body, [(chunk(dim), rows_hbm), (ATTR_CHUNK, attr_hbm)],
           [(chunk(dim), u_hbm), (chunk(ff), act_hbm), (chunk(ff), slope_hbm), (chunk(toks), z_hbm)])
    top = jnp.max(m8[...], axis=0, keepdims=True)
    stat_ref[0:1, :] = top
    stat_ref[1:2, :] = jnp.sum(s8[...] * jnp.exp(m8[...] - top), axis=0, keepdims=True)


def logit_back_kernel(scale, nch_ref, tid_ref, lse_ref, h_ref, z_hbm, u_hbm, attr_hbm, g_hbm, dht_ref, zt_ref):
    dht_ref[...] = jnp.zeros_like(dht_ref)
    zt_ref[...] = jnp.zeros_like(zt_ref)
    dim, toks = u_hbm.shape[1], h_ref.shape[0]

    def body(z_ref, u_ref, attr_ref, g_ref):
        vec_t = u_ref[...].T
        loc = column(attr_ref, 0, 0, CH // WIN)
        is_targ = column(attr_ref, 2, 0, CH // WIN)
        shift = is_targ * (-1.0 / toks)
        grad = None
        for t in range(0, toks, TB):
            z = z_ref[:, t : t + TB]
            same = loc == tid_ref[:, t : t + TB]
            dz = (jnp.exp(z - lse_ref[:, t : t + TB]) + jnp.where(same, shift, 0.0)).astype(BF)
            part = dot(dz, h_ref[t : t + TB, :])
            grad = part if grad is None else grad + part
            dht_ref[:, t : t + TB] += dot(vec_t, dz)
            zt = jnp.where(same, z * is_targ, 0.0)
            zt_ref[:, t : t + TB] += jnp.sum(zt.reshape(CH // 8, 8, TB), axis=0)
        g_ref[...] = (grad * scale).astype(BF)

    stream(nch_ref, body, [(chunk(toks), z_hbm), (chunk(dim), u_hbm), (ATTR_CHUNK, attr_hbm)], [(chunk(dim), g_hbm)])


def dw_out_kernel(nch_ref, g_hbm, act_hbm, dw_ref, acc):
    acc[...] = jnp.zeros_like(acc)
    dim, ff = g_hbm.shape[1], act_hbm.shape[1]

    def body(g_ref, act_ref):
        g_t = g_ref[...].T
        for f in range(0, ff, FB):
            acc[:, f : f + FB] += dot(g_t, act_ref[:, f : f + FB])

    stream(nch_ref, body, [(chunk(dim), g_hbm), (chunk(ff), act_hbm)], [])
    for f in range(0, ff, FB):
        dw_ref[f : f + FB, :] = acc[:, f : f + FB].T


def tower_back_kernel(nch_ref, w1_ref, w2_ref, g_hbm, rows_hbm, slope_hbm, drow_hbm, dw_ref):
    dw_ref[...] = jnp.zeros_like(dw_ref)
    dim, ff = w1_ref.shape

    def body(g_ref, rows_ref, slope_ref, drow_ref):
        g = g_ref[...]
        rows_t = rows_ref[...].T
        out = None
        for f in range(0, ff, FB):
            q = (slope_ref[:, f : f + FB] * dot_nt(g, w2_ref[f : f + FB, :])).astype(BF)
            dw_ref[:, f : f + FB] += dot(rows_t, q)
            part = dot_nt(q, w1_ref[:, f : f + FB])
            out = part if out is None else out + part
        drow_ref[...] = out.astype(BF)

    stream(nch_ref, body, [(chunk(dim), g_hbm), (chunk(dim), rows_hbm), (chunk(ff), slope_hbm)], [(chunk(dim), drow_hbm)])


def table_kernel(starts_ref, nch_ref, attr_ref, drow_hbm, out_ref, drow, sem):
    blk = pl.program_id(0)

    @pl.when(blk == 0)
    def _():
        def copy(i):
            at = pl.ds(pl.multiple_of(i * CH, CH), CH)
            return pltpu.make_async_copy(drow_hbm.at[at, :], drow.at[at, :], sem)

        def start(i, carry):
            copy(i).start()
            return carry

        def wait(i, carry):
            copy(i).wait()
            return carry

        lax.fori_loop(0, nch_ref[0], start, 0)
        tail = pl.ds(pl.multiple_of(nch_ref[0] * CH, CH), 2 * WIN)
        drow[tail, :] = jnp.zeros((2 * WIN, drow.shape[1]), BF)
        lax.fori_loop(0, nch_ref[0], wait, 0)

    first, count = windows(starts_ref, blk)
    row = (lax.broadcasted_iota(jnp.int32, (BLK, WIN), 0) + blk * BLK).astype(F32)
    out_ref[...] = jnp.zeros_like(out_ref)

    def put(i, carry):
        tile = first + 2 * i
        pick = jnp.concatenate([jnp.where(attr_ref[tile + k][0:1, :] == row, 1.0, 0.0).astype(BF) for k in range(2)], axis=1)
        at = pl.ds(pl.multiple_of(tile * WIN, WIN), 2 * WIN)
        out_ref[...] += dot(pick, drow[at, :])
        return carry

    lax.fori_loop(0, count, put, 0)


def params(**kw):
    return pltpu.CompilerParams(vmem_limit_bytes=VMEM_LIMIT, dimension_semantics=("arbitrary",), **kw)


def whole(shape):
    return pl.BlockSpec(shape, lambda i, *_: (0,) * len(shape))


def chunk(width):
    return pl.BlockSpec((CH, width), lambda i, *_: (i, 0))


ATTR_CHUNK = pl.BlockSpec((CH // WIN, 8, WIN), lambda i, *_: (i, 0, 0))


def sds(*shape, dtype=F32):
    return jax.ShapeDtypeStruct(shape, dtype)


def query_fwd(x, w_in, w_out):
    pre = jnp.dot(x, w_in, preferred_element_type=F32)
    hidden = jax.nn.gelu(pre).astype(BF)
    return jnp.dot(hidden, w_out, preferred_element_type=F32).astype(BF)


def solution(mesh):
    num_dev = mesh.shape["dp"]

    def local_step(tokens, w_one, w_two, wi_one, wi_two, table, cand_ids, log_q, targ_loc):
        dim = table.shape[1]
        ff = wi_one.shape[1]
        rows_loc = table.shape[0]
        toks = tokens.shape[0] * num_dev
        cands = cand_ids.shape[0]
        cap = cands + toks
        n_blk = rows_loc // BLK
        scale = SCORE_GAIN / math.sqrt(dim)
        base = lax.axis_index("dp") * rows_loc

        query_loc = query_fwd(tokens, w_one, w_two)
        query = lax.all_gather(query_loc, "dp", axis=0, tiled=True)
        x_all = lax.all_gather(tokens, "dp", axis=0, tiled=True)
        targ_all = lax.all_gather(targ_loc, "dp", axis=0, tiled=True)

        ids = jnp.concatenate([cand_ids, targ_all]) - base
        kind = jnp.concatenate([jnp.zeros((cands,), jnp.int32), jnp.ones((toks,), jnp.int32)])
        key = jnp.where((ids >= 0) & (ids < rows_loc), 2 * ids + kind, 2 * rows_loc)
        offs = jnp.concatenate([log_q, jnp.full((toks,), EXCLUDED, F32)])
        bounds = jnp.arange(n_blk + 1, dtype=jnp.int32) * (2 * BLK)
        starts = jnp.sum((key[None, :] < bounds[:, None]).astype(jnp.int32), axis=1)
        nch = jnp.maximum(lax.div(starts[n_blk] + (CH - 1), CH), 1)
        key_s, offs_s = lax.sort((key, offs), num_keys=1, is_stable=False)
        repeat = jnp.concatenate([jnp.zeros((1,), bool), key_s[1:] == key_s[:-1]])
        used = (key_s < 2 * rows_loc) & ~repeat
        attr = jnp.stack([
            jnp.where(used, (key_s >> 1).astype(F32), NO_ROW),
            jnp.where(used, offs_s, EXCLUDED),
            jnp.where(used, (key_s & 1).astype(F32), 0.0),
        ])
        attr = jnp.pad(attr, ((0, 5), (0, 0)))
        pad = jnp.broadcast_to(jnp.array([NO_ROW, EXCLUDED, 0, 0, 0, 0, 0, 0], F32)[:, None], (8, 2 * WIN))
        attr = jnp.concatenate([attr, pad], axis=1).reshape(8, -1, WIN).transpose(1, 0, 2)
        tid = (targ_all - base).astype(F32)[None, :]
        nch1 = nch[None]

        rows = pl.pallas_call(
            gather_kernel,
            grid_spec=pltpu.PrefetchScalarGridSpec(
                num_scalar_prefetch=2, grid=(n_blk,),
                in_specs=[pl.BlockSpec((BLK, dim), lambda i, *_: (i, 0)), whole(attr.shape)],
                out_specs=pl.BlockSpec(memory_space=pl.ANY),
                scratch_shapes=[pltpu.VMEM((cap + CH, dim), BF), pltpu.SemaphoreType.DMA]),
            out_shape=sds(cap, dim, dtype=BF), compiler_params=params(), name="gather",
        )(starts, nch1, table, attr)

        def call(kernel, name, ins, outs, scratch=()):
            spec = lambda shape, vmem: whole(shape) if vmem else pl.BlockSpec(memory_space=pl.ANY)
            return pl.pallas_call(
                kernel,
                grid_spec=pltpu.PrefetchScalarGridSpec(
                    num_scalar_prefetch=1, grid=(1,), in_specs=[spec(a.shape, v) for a, v in ins],
                    out_specs=[spec(o.shape, v) for o, v in outs], scratch_shapes=list(scratch)),
                out_shape=[o for o, _ in outs], compiler_params=params(), name=name,
            )(nch1, *[a for a, _ in ins])

        bf_list, f_list = sds(cap, dim, dtype=BF), sds(cap, ff)
        vec, act, slope, z, stat = call(
            functools.partial(fwd_kernel, scale), "fwd",
            [(tid, True), (query, True), (wi_one, True), (wi_two, True), (rows, False), (attr, False)],
            [(bf_list, False), (sds(cap, ff, dtype=BF), False), (f_list, False), (sds(cap, toks), False), (sds(2, toks), True)],
            [pltpu.VMEM((8, toks), F32), pltpu.VMEM((8, toks), F32)])

        stats = lax.all_gather(stat, "dp", axis=0)
        top = jnp.max(stats[:, 0], axis=0)
        lse = top + jnp.log(jnp.sum(stats[:, 1] * jnp.exp(stats[:, 0] - top), axis=0))

        g, dht_part, zt = call(
            functools.partial(logit_back_kernel, scale), "logit_back",
            [(tid, True), ((lse + math.log(toks))[None, :], True), (query, True), (z, False), (vec, False), (attr, False)],
            [(bf_list, False), (sds(dim, toks), True), (sds(8, toks), True)])

        dht = (lax.psum_scatter(dht_part, "dp", scatter_dimension=0, tiled=True) * scale).astype(BF)
        dht = lax.all_gather(dht, "dp", axis=0, tiled=True)

        (dwi_two,) = call(dw_out_kernel, "dw_out", [(g, False), (act, False)], [(sds(ff, dim), True)], [pltpu.VMEM((dim, ff), F32)])
        dwi_two = lax.psum(dwi_two, "dp")
        drow, dwi_one = call(
            tower_back_kernel, "tower_back",
            [(wi_one, True), (wi_two, True), (g, False), (rows, False), (slope, False)], [(bf_list, False), (sds(dim, ff), True)])
        dwi_one = lax.psum(dwi_one, "dp")

        d_table = pl.pallas_call(
            table_kernel,
            grid_spec=pltpu.PrefetchScalarGridSpec(
                num_scalar_prefetch=2, grid=(n_blk,),
                in_specs=[whole(attr.shape), pl.BlockSpec(memory_space=pl.ANY)],
                out_specs=pl.BlockSpec((BLK, dim), lambda i, *_: (i, 0)),
                scratch_shapes=[pltpu.VMEM((cap + CH, dim), BF), pltpu.SemaphoreType.DMA]),
            out_shape=sds(rows_loc, dim), compiler_params=params(), name="table",
        )(starts, nch1, attr, drow)

        pre = jnp.dot(x_all, w_one, preferred_element_type=F32)
        hidden, gelu_back = jax.vjp(jax.nn.gelu, pre)
        dw_two = jnp.einsum("tf,dt->fd", hidden.astype(BF), dht, preferred_element_type=F32)
        grad_hidden = jnp.einsum("dt,fd->tf", dht, w_two, preferred_element_type=F32)
        grad_pre = gelu_back(grad_hidden)[0].astype(BF)
        dw_one = jnp.einsum("te,tf->ef", x_all, grad_pre, preferred_element_type=F32)

        loss = (jnp.sum(lse) - lax.psum(jnp.sum(zt), "dp")) / toks
        return loss, d_table, dw_one, dw_two, dwi_one, dwi_two

    return jax.shard_map(local_step, mesh=mesh, in_specs=(P("dp", None), P(), P(), P(), P(), P("dp", None), P(), P(), P("dp")), out_specs=(P(), P("dp", None), P(), P(), P(), P()), check_vma=False)
```

```python
import functools
import math
import jax
import jax.numpy as jnp
from jax import lax
from jax.experimental import pallas as pl
from jax.experimental.pallas import tpu as pltpu
from jax.sharding import PartitionSpec as P

SCORE_GAIN = 3.0
HIT_VALUE = -1e9
EXCLUDED = 3e38
NO_ROW = -1e9
CH = 512
BLK = 512
SUB = 8
TSUB = 4
PAIR = 2
WIN = 128
FB = 256
TB = 256
GELU_C = math.sqrt(2.0 / math.pi)
BF, F32 = jnp.bfloat16, jnp.float32
MESH = pl.DeviceIdType.MESH
VMEM_LIMIT = 60 * 1024 * 1024


def dot(a, b):
    return lax.dot_general(a, b, (((1,), (0,)), ((), ())), preferred_element_type=F32)


def dot_nt(a, b):
    return lax.dot_general(a, b, (((1,), (1,)), ((), ())), preferred_element_type=F32)


def gelu(x):
    half = 0.5 * x
    return half + half * jnp.tanh(x * (GELU_C + (GELU_C * 0.044715) * (x * x)))


def gelu_pair(x):
    sq = x * x
    th = jnp.tanh(x * (GELU_C + (GELU_C * 0.044715) * sq))
    half = 0.5 * x
    slope = (0.5 + 0.5 * th) + half * (1.0 - th * th) * (GELU_C + (3.0 * 0.044715 * GELU_C) * sq)
    return half + half * th, slope


def column(attr_ref, index, first, count):
    tiles = [attr_ref[first + i].T[:, index : index + 1] for i in range(count)]
    return jnp.concatenate(tiles, axis=0) if count > 1 else tiles[0]


def start_copies(nch_ref, copy):
    def step(i, carry):
        copy(i).start()
        return carry

    lax.fori_loop(0, nch_ref[0], step, 0)


def wait_copies(nch_ref, copy):
    def step(i, carry):
        copy(i).wait()
        return carry

    lax.fori_loop(0, nch_ref[0], step, 0)


def chunk_at(i):
    return pl.ds(pl.multiple_of(i * CH, CH), CH)


def gather_kernel(starts_ref, nch_ref, tbl_ref, attr_ref, rows_hbm, rows, keys, sem):
    step = pl.program_id(0)

    @pl.when(step == 0)
    def _():
        def prepare(i, carry):
            rows[chunk_at(i), :] = jnp.zeros((CH, rows.shape[1]), BF)
            for k in range(CH // WIN):
                at = pl.ds(pl.multiple_of(i * CH + k * WIN, WIN), WIN)
                key = attr_ref[i * (CH // WIN) + k].T[:, 0:1]
                keys[at, :] = jnp.broadcast_to(key, (WIN, WIN))
            return carry

        lax.fori_loop(0, nch_ref[0] + 1, prepare, 0)

    lanes = [(lax.broadcasted_iota(jnp.int32, (1, WIN), 1) + j).astype(F32) for j in range(0, BLK, WIN)]

    def picked(blk, part, at):
        key = keys[pl.ds(at, WIN), :] - (blk * BLK).astype(F32)
        pick = [jnp.where(key == lane, 1.0, 0.0).astype(BF) for lane in lanes]
        return dot(jnp.concatenate(pick, axis=1), tbl_ref[pl.ds(pl.multiple_of(part * BLK, BLK), BLK), :]).astype(BF)

    def some_blocks(i, carry):
        parts = [i * PAIR + k for k in range(PAIR)]
        blks = [step * SUB + part for part in parts]
        firsts = [(starts_ref[blk] >> 4) << 4 for blk in blks]
        gots = [picked(blk, part, pl.multiple_of(first, 16)) for blk, part, first in zip(blks, parts, firsts)]
        for blk, part, first, got in zip(blks, parts, firsts, gots):
            head = pl.ds(pl.multiple_of(first, 16), 16)
            rows[head, :] = rows[head, :] + got[:16]
            rows[pl.ds(pl.multiple_of(first + 16, 16), WIN - 16), :] = got[16:]

            def more(i, carry, blk=blk, part=part, first=first):
                at = pl.multiple_of(first + i * WIN, 16)
                rows[pl.ds(at, WIN), :] = picked(blk, part, at)
                return carry

            lax.fori_loop(1, (starts_ref[blk + 1] - first + (WIN - 1)) >> 7, more, 0)
        return carry

    lax.fori_loop(0, SUB // PAIR, some_blocks, 0)

    @pl.when(step == pl.num_programs(0) - 1)
    def _():
        copy = lambda i: pltpu.make_async_copy(rows.at[chunk_at(i), :], rows_hbm.at[chunk_at(i), :], sem)
        start_copies(nch_ref, copy)
        wait_copies(nch_ref, copy)


def stream(nch, body, ins, outs):
    specs = [[spec for spec, _ in part] for part in (ins, outs)]
    pltpu.emit_pipeline(body, grid=(nch,), in_specs=specs[0], out_specs=specs[1])(*[ref for _, ref in ins + outs])


def fwd_kernel(scale, nch_ref, tid_ref, h_ref, w1_ref, w2_ref, rows_hbm, attr_hbm, u_hbm, pre_hbm, z_hbm, stat_ref, m8, s8):
    m8[...] = jnp.full_like(m8, -EXCLUDED)
    s8[...] = jnp.zeros_like(s8)
    dim, ff, toks = rows_hbm.shape[1], w1_ref.shape[1], h_ref.shape[0]

    def body(rows_ref, attr_ref, u_ref, pre_ref, z_ref):
        rows = rows_ref[...]
        out = None
        for f in range(0, ff, FB):
            pre = dot(rows, w1_ref[:, f : f + FB])
            pre_ref[:, f : f + FB] = pre
            act = gelu(pre).astype(BF)
            part = dot(act, w2_ref[f : f + FB, :])
            out = part if out is None else out + part
        vec = out.astype(BF)
        u_ref[...] = vec
        loc = column(attr_ref, 0, 0, CH // WIN)
        off = column(attr_ref, 1, 0, CH // WIN)
        is_targ = column(attr_ref, 2, 0, CH // WIN) > 0.5
        for t in range(0, toks, TB):
            raw = dot_nt(vec, h_ref[t : t + TB, :]) * scale
            same = loc == tid_ref[:, t : t + TB]
            z = jnp.where(same, jnp.where(is_targ, raw, HIT_VALUE), raw - off)
            z_ref[:, t : t + TB] = z
            z3 = z.reshape(CH // 8, 8, TB)
            old = m8[:, t : t + TB]
            new = jnp.maximum(old, jnp.max(z3, axis=0))
            s8[:, t : t + TB] = s8[:, t : t + TB] * jnp.exp(old - new) + jnp.sum(jnp.exp(z3 - new[None]), axis=0)
            m8[:, t : t + TB] = new

    stream(nch_ref[0], body, [(chunk(dim), rows_hbm), (ATTR_CHUNK, attr_hbm)],
           [(chunk(dim), u_hbm), (chunk(ff), pre_hbm), (chunk(toks), z_hbm)])
    top = jnp.max(m8[...], axis=0, keepdims=True)
    stat_ref[0:1, :] = top
    stat_ref[1:2, :] = jnp.sum(s8[...] * jnp.exp(m8[...] - top), axis=0, keepdims=True)


def logit_back_kernel(scale, nch_ref, tid_ref, lse_ref, h_ref, z_hbm, u_hbm, attr_hbm, g_hbm, dht_ref):
    dht_ref[...] = jnp.zeros_like(dht_ref)
    dim, toks = u_hbm.shape[1], h_ref.shape[0]

    def body(z_ref, u_ref, attr_ref, g_ref):
        vec_t = u_ref[...].T
        loc = column(attr_ref, 0, 0, CH // WIN)
        is_targ = column(attr_ref, 2, 0, CH // WIN)
        shift = is_targ * (-1.0 / toks)
        grad = None
        log_toks = math.log(toks)
        for t in range(0, toks, TB):
            z = z_ref[:, t : t + TB]
            same = loc == tid_ref[:, t : t + TB]
            dz = (jnp.exp(z - (lse_ref[:, t : t + TB] + log_toks)) + jnp.where(same, shift, 0.0)).astype(BF)
            part = dot(dz, h_ref[t : t + TB, :])
            grad = part if grad is None else grad + part
            dht_ref[:dim, t : t + TB] += dot(vec_t, dz)
            zt = jnp.where(same, z * is_targ, 0.0)
            dht_ref[dim:, t : t + TB] += jnp.sum(zt.reshape(CH // 8, 8, TB), axis=0)
        g_ref[...] = (grad * scale).astype(BF)

    stream(nch_ref[0], body, [(chunk(toks), z_hbm), (chunk(dim), u_hbm), (ATTR_CHUNK, attr_hbm)], [(chunk(dim), g_hbm)])


def tower_back_kernel(nch_ref, w1_ref, w2_ref, g_hbm, rows_hbm, pre_hbm, drow_hbm, dw_ref):
    dw_ref[...] = jnp.zeros_like(dw_ref)
    dim, ff = w1_ref.shape

    def body(g_ref, rows_ref, pre_ref, drow_ref):
        g = g_ref[...]
        g_t, rows_t = g.T, rows_ref[...].T
        out = None
        for f in range(0, ff, FB):
            act, slope = gelu_pair(pre_ref[:, f : f + FB])
            q = (slope * dot_nt(g, w2_ref[f : f + FB, :])).astype(BF)
            dw_ref[dim:, f : f + FB] += dot(g_t, act.astype(BF))
            dw_ref[:dim, f : f + FB] += dot(rows_t, q)
            part = dot_nt(q, w1_ref[:, f : f + FB])
            out = part if out is None else out + part
        drow_ref[...] = out.astype(BF)

    stream(nch_ref[0], body, [(chunk(dim), g_hbm), (chunk(dim), rows_hbm), (chunk(ff), pre_hbm)], [(chunk(dim), drow_hbm)])


def query_back_kernel(scale, x_hbm, dht_hbm, w1_hbm, w2_hbm, part_hbm, dw1_ref, dw2t_ref, sum_ref,
                      x_ref, dht_ref, w1_ref, w2_ref, work, r0, r1, r2, load_sem, send_sem, recv_sem):
    me = lax.axis_index("dp")
    core, x, y = lax.rem(me, 2), lax.rem(lax.div(me, 2), 2), lax.div(me, 4)
    pair, x_peer, y_peer = me + 1 - 2 * core, me + 2 - 4 * x, me + 4 - 8 * y
    dim, ff = w1_ref.shape
    half = part_hbm.shape[0] // 2
    p1, p2, p3 = half // 2, half // 4, half // 8
    mine, other = core * half, (1 - core) * half

    barrier = pltpu.get_barrier_semaphore()
    for peer in (pair, x_peer, y_peer):
        pl.semaphore_signal(barrier, inc=1, device_id=(peer,), device_id_type=MESH)
    pl.semaphore_wait(barrier, 3)

    def rows(first, count):
        return pl.ds(pl.multiple_of(first, count), count)

    def send(k, src, dst, peer):
        copy = pltpu.make_async_remote_copy(
            src_ref=src, dst_ref=dst, send_sem=send_sem.at[k], recv_sem=recv_sem.at[k], device_id=(peer,), device_id_type=MESH)
        copy.start()
        return copy

    pair_copy = send(0, part_hbm.at[rows(other, half), :], r0, pair)
    loads = [(part_hbm.at[rows(mine, half), :], work), (x_hbm, x_ref), (dht_hbm.at[rows(0, dim), :], dht_ref), (w1_hbm, w1_ref), (w2_hbm, w2_ref)]
    loads = [pltpu.make_async_copy(src, dst, load_sem.at[i]) for i, (src, dst) in enumerate(loads)]
    for copy in loads:
        copy.start()
    dw1_ref[...] = jnp.zeros_like(dw1_ref)
    dw2t_ref[...] = jnp.zeros_like(dw2t_ref)
    for copy in loads:
        copy.wait()

    def unit(u, carry):
        tok = pl.ds(pl.multiple_of(lax.div(u, 2) * CH, CH), CH)
        first = lax.rem(u, 2) * (ff // 2)
        xs, grad_t = x_ref[tok, :], (dht_ref[:, tok] * scale).astype(BF)
        x_t, grad = xs.T, grad_t.T
        for f in range(0, ff // 2, FB):
            at = pl.ds(pl.multiple_of(first + f, FB), FB)
            act, slope = gelu_pair(dot(xs, w1_ref[:, at]))
            q = (slope * dot_nt(grad, w2_ref[at, :])).astype(BF)
            dw2t_ref[:, at] += dot(grad_t, act.astype(BF))
            dw1_ref[:, at] += dot(x_t, q)
        return carry

    pair_copy.wait()
    work[...] = work[...] + r0[...]
    step = [send(1, work.at[rows((1 - x) * p2, p2), :], r1.at[0], x_peer),
            send(2, work.at[rows(p1 + (1 - y) * p2, p2), :], r1.at[1], y_peer)]
    lax.fori_loop(0, 5, unit, 0)
    for copy in step:
        copy.wait()
    for at, k in ((rows(x * p2, p2), 0), (rows(p1 + y * p2, p2), 1)):
        work[at, :] = work[at, :] + r1[k]
    step = [send(3, work.at[rows(x * p2 + (1 - y) * p3, p3), :], r2.at[0], y_peer),
            send(4, work.at[rows(p1 + y * p2 + (1 - x) * p3, p3), :], r2.at[1], x_peer)]
    lax.fori_loop(5, 2 * (x_ref.shape[0] // CH), unit, 0)
    for copy in step:
        copy.wait()
    piece_a, piece_b = x * p2 + y * p3, p1 + y * p2 + x * p3
    step = []
    for k, piece, peer in ((0, piece_a, y_peer), (1, piece_b, x_peer)):
        at = rows(mine + piece, p3)
        sum_ref[at, :] = work[rows(piece, p3), :] + r2[k]
        step.append(send(5 + k, sum_ref.at[at, :], sum_ref.at[at, :], peer))
    for copy in step:
        copy.wait()
    at_a, at_b = rows(mine + x * p2, p2), rows(mine + p1 + y * p2, p2)
    step = [send(7, sum_ref.at[at_a, :], sum_ref.at[at_a, :], x_peer), send(8, sum_ref.at[at_b, :], sum_ref.at[at_b, :], y_peer)]
    last = [send(9, sum_ref.at[at_a, :], sum_ref.at[at_a, :], pair), send(10, sum_ref.at[at_b, :], sum_ref.at[at_b, :], pair)]
    for copy in step:
        copy.wait()
    at_a, at_b = rows(mine + (1 - x) * p2, p2), rows(mine + p1 + (1 - y) * p2, p2)
    last += [send(11, sum_ref.at[at_a, :], sum_ref.at[at_a, :], pair), send(12, sum_ref.at[at_b, :], sum_ref.at[at_b, :], pair)]
    for copy in last:
        copy.wait()


def table_kernel(starts_ref, nch_ref, attr_ref, drow_hbm, out_ref, drow, sem):
    step = pl.program_id(0)

    @pl.when(step == 0)
    def _():
        copy = lambda i: pltpu.make_async_copy(drow_hbm.at[chunk_at(i), :], drow.at[chunk_at(i), :], sem)
        start_copies(nch_ref, copy)
        drow[chunk_at(nch_ref[0]), :] = jnp.zeros((CH, drow.shape[1]), BF)
        wait_copies(nch_ref, copy)

    row = lax.broadcasted_iota(jnp.int32, (BLK, WIN), 0).astype(F32)

    def put(blk, tile):
        base = (blk * BLK).astype(F32)
        pick = [jnp.where(attr_ref[tile + k][0:1, :] - base == row, 1.0, 0.0).astype(BF) for k in range(2)]
        return dot(jnp.concatenate(pick, axis=1), drow[pl.ds(pl.multiple_of(tile * WIN, WIN), 2 * WIN), :])

    def some_blocks(i, carry):
        parts = [i * PAIR + k for k in range(PAIR)]
        firsts = [starts_ref[step * TSUB + part] >> 7 for part in parts]
        for part, first in zip(parts, firsts):
            out_ref[pl.ds(pl.multiple_of(part * BLK, BLK), BLK), :] = put(step * TSUB + part, first)
        for part, first in zip(parts, firsts):
            def more(i, carry, part=part, first=first):
                out_ref[pl.ds(pl.multiple_of(part * BLK, BLK), BLK), :] += put(step * TSUB + part, first + 2 * i)
                return carry

            hi = starts_ref[step * TSUB + part + 1]
            lax.fori_loop(1, (hi - first * WIN + (2 * WIN - 1)) >> 8, more, 0)
        return carry

    lax.fori_loop(0, TSUB // PAIR, some_blocks, 0)


def exchange(n, src_ref, all_ref, send_sem, recv_sem):
    me = lax.axis_index("dp")
    barrier = pltpu.get_barrier_semaphore()
    for k in range(1, n):
        pl.semaphore_signal(barrier, inc=1, device_id=(lax.rem(me + k, n),), device_id_type=MESH)
    pl.semaphore_wait(barrier, n - 1)
    copies = []
    for k in range(1, n):
        copies.append(pltpu.make_async_remote_copy(
            src_ref=src_ref, dst_ref=all_ref.at[me], send_sem=send_sem.at[k - 1], recv_sem=recv_sem.at[k - 1],
            device_id=(lax.rem(me + k, n),), device_id_type=MESH))
        copies[-1].start()
    all_ref[me] = src_ref[...]
    for copy in copies:
        copy.wait()


def targets_kernel(n, src_ref, out_ref, send_sem, recv_sem):
    exchange(n, src_ref, out_ref, send_sem, recv_sem)


def stats_kernel(n, src_ref, lse_ref, stats, send_sem, recv_sem):
    exchange(n, src_ref, stats, send_sem, recv_sem)
    top = stats[0, 0:1, :]
    for i in range(1, n):
        top = jnp.maximum(top, stats[i, 0:1, :])
    total = jnp.zeros_like(top)
    for i in range(n):
        total += stats[i, 1:2, :] * jnp.exp(stats[i, 0:1, :] - top)
    lse_ref[...] = top + jnp.log(total)


def share(kernel, ident, n, src, out, scratch=()):
    vmem = pl.BlockSpec(memory_space=pltpu.VMEM)
    return pl.pallas_call(
        functools.partial(kernel, n), out_shape=out, in_specs=[vmem], out_specs=vmem,
        scratch_shapes=[*scratch, pltpu.SemaphoreType.DMA((n - 1,)), pltpu.SemaphoreType.DMA((n - 1,))],
        compiler_params=pltpu.CompilerParams(collective_id=ident, has_side_effects=True),
    )(src)


def params(**kw):
    return pltpu.CompilerParams(vmem_limit_bytes=VMEM_LIMIT, dimension_semantics=("arbitrary",), **kw)


def cost(flops):
    return pl.CostEstimate(flops=flops, bytes_accessed=64 << 20, transcendentals=0)


def whole(shape):
    return pl.BlockSpec(shape, lambda i, *_: (0,) * len(shape))


def chunk(width):
    return pl.BlockSpec((CH, width), lambda i, *_: (i, 0))


ATTR_CHUNK = pl.BlockSpec((CH // WIN, 8, WIN), lambda i, *_: (i, 0, 0))


def sds(*shape, dtype=F32):
    return jax.ShapeDtypeStruct(shape, dtype)


def query_fwd(x, w_in, w_out):
    pre = jnp.dot(x, w_in, preferred_element_type=F32)
    hidden = jax.nn.gelu(pre).astype(BF)
    return jnp.dot(hidden, w_out, preferred_element_type=F32).astype(BF)


def solution(mesh):
    num_dev = mesh.shape["dp"]

    def local_step(tokens, w_one, w_two, wi_one, wi_two, table, cand_ids, log_q, targ_loc):
        dim = table.shape[1]
        ff = wi_one.shape[1]
        rows_loc = table.shape[0]
        toks = tokens.shape[0] * num_dev
        cands = cand_ids.shape[0]
        cap = cands + toks
        n_blk = rows_loc // BLK
        scale = SCORE_GAIN / math.sqrt(dim)
        base = lax.axis_index("dp") * rows_loc

        query_loc = query_fwd(tokens, w_one, w_two)
        query = lax.all_gather(query_loc, "dp", axis=0, tiled=True)
        x_all = lax.all_gather(tokens, "dp", axis=0, tiled=True)
        targ_all = share(targets_kernel, 0, num_dev, targ_loc[None, :], sds(num_dev, 1, targ_loc.shape[0], dtype=jnp.int32)).reshape(toks)

        ids = jnp.concatenate([cand_ids, targ_all]) - base
        kind = jnp.concatenate([jnp.zeros((cands,), jnp.int32), jnp.ones((toks,), jnp.int32)])
        key = jnp.where((ids >= 0) & (ids < rows_loc), 2 * ids + kind, 2 * rows_loc)
        offs = jnp.concatenate([log_q, jnp.full((toks,), EXCLUDED, F32)])
        bounds = jnp.arange(n_blk + 1, dtype=jnp.int32) * (2 * BLK)
        starts = jnp.sum((key[None, :] < bounds[:, None]).astype(jnp.int32), axis=1)
        nch = jnp.maximum(lax.div(starts[n_blk] + (CH - 1), CH), 1)
        key_s, offs_s = lax.sort((key, offs), num_keys=1, is_stable=False)
        repeat = jnp.concatenate([jnp.zeros((1,), bool), key_s[1:] == key_s[:-1]])
        used = (key_s < 2 * rows_loc) & ~repeat
        attr = jnp.stack([
            jnp.where(used, (key_s >> 1).astype(F32), NO_ROW),
            jnp.where(used, offs_s, EXCLUDED),
            jnp.where(used, (key_s & 1).astype(F32), 0.0),
        ])
        attr = jnp.pad(attr, ((0, 5), (0, 0)))
        pad = jnp.broadcast_to(jnp.array([NO_ROW, EXCLUDED, 0, 0, 0, 0, 0, 0], F32)[:, None], (8, CH))
        attr = jnp.concatenate([attr, pad], axis=1).reshape(8, -1, WIN).transpose(1, 0, 2)
        tid = (targ_all - base).astype(F32)[None, :]
        nch1 = nch[None]

        rows = pl.pallas_call(
            gather_kernel,
            grid_spec=pltpu.PrefetchScalarGridSpec(
                num_scalar_prefetch=2, grid=(n_blk // SUB,),
                in_specs=[pl.BlockSpec((SUB * BLK, dim), lambda i, *_: (i, 0)), whole(attr.shape)],
                out_specs=pl.BlockSpec(memory_space=pl.ANY),
                scratch_shapes=[pltpu.VMEM((cap + CH, dim), BF), pltpu.VMEM((cap + CH, WIN), F32), pltpu.SemaphoreType.DMA]),
            out_shape=sds(cap, dim, dtype=BF), compiler_params=params(), cost_estimate=cost(4 * rows_loc * WIN * dim), name="gather",
        )(starts, nch1, table, attr)

        def call(kernel, name, flops, ins, outs, scratch=()):
            spec = lambda shape, vmem: whole(shape) if vmem else pl.BlockSpec(memory_space=pl.ANY)
            return pl.pallas_call(
                kernel,
                grid_spec=pltpu.PrefetchScalarGridSpec(
                    num_scalar_prefetch=1, grid=(1,), in_specs=[spec(a.shape, v) for a, v in ins],
                    out_specs=[spec(o.shape, v) for o, v in outs], scratch_shapes=list(scratch)),
                out_shape=[o for o, _ in outs], compiler_params=params(), cost_estimate=cost(flops), name=name,
            )(nch1, *[a for a, _ in ins])

        bf_list, f_list = sds(cap, dim, dtype=BF), sds(cap, ff)
        vec, pre, z, stat = call(
            functools.partial(fwd_kernel, scale), "fwd", 6 * cap * dim * ff // 4,
            [(tid, True), (query, True), (wi_one, True), (wi_two, True), (rows, False), (attr, False)],
            [(bf_list, False), (f_list, False), (sds(cap, toks), False), (sds(2, toks), True)],
            [pltpu.VMEM((8, toks), F32), pltpu.VMEM((8, toks), F32)])

        stat, x_all = lax.optimization_barrier((stat, x_all))
        lse = share(stats_kernel, 1, num_dev, stat, sds(1, toks), [pltpu.VMEM((num_dev, 2, toks), F32)])

        g, dht_part = call(
            functools.partial(logit_back_kernel, scale), "logit_back", 4 * cap * dim * toks // 4,
            [(tid, True), (lse, True), (query, True), (z, False), (vec, False), (attr, False)],
            [(bf_list, False), (sds(dim + 8, toks), True)])

        dht = lax.psum(dht_part, "dp")
        drow, dwi_part = call(
            tower_back_kernel, "tower_back", 8 * cap * dim * ff // 4,
            [(wi_one, True), (wi_two, True), (g, False), (rows, False), (pre, False)],
            [(bf_list, False), (sds(2 * dim, ff), True)])

        d_table = pl.pallas_call(
            table_kernel,
            grid_spec=pltpu.PrefetchScalarGridSpec(
                num_scalar_prefetch=2, grid=(n_blk // TSUB,),
                in_specs=[whole(attr.shape), pl.BlockSpec(memory_space=pl.ANY)],
                out_specs=pl.BlockSpec((TSUB * BLK, dim), lambda i, *_: (i, 0)),
                scratch_shapes=[pltpu.VMEM((cap + CH, dim), BF), pltpu.SemaphoreType.DMA]),
            out_shape=sds(rows_loc, dim), compiler_params=params(), cost_estimate=cost(4 * rows_loc * WIN * dim), name="table",
        )(starts, nch1, attr, drow)

        any_spec, vmem = pl.BlockSpec(memory_space=pl.ANY), pl.BlockSpec(memory_space=pltpu.VMEM)
        dw_one, dw_two_t, dwi = pl.pallas_call(
            functools.partial(query_back_kernel, scale),
            in_specs=[any_spec] * 5, out_specs=[vmem] * 3,
            out_shape=[sds(dim, ff), sds(dim, ff), sds(2 * dim, ff)],
            scratch_shapes=[
                pltpu.VMEM((toks, dim), BF), pltpu.VMEM((dim, toks), F32), pltpu.VMEM((dim, ff), BF), pltpu.VMEM((ff, dim), BF),
                pltpu.VMEM((dim, ff), F32), pltpu.VMEM((dim, ff), F32),
                pltpu.VMEM((2, dim // 4, ff), F32), pltpu.VMEM((2, dim // 8, ff), F32),
                pltpu.SemaphoreType.DMA((5,)), pltpu.SemaphoreType.DMA((13,)), pltpu.SemaphoreType.DMA((13,))],
            compiler_params=pltpu.CompilerParams(vmem_limit_bytes=VMEM_LIMIT, collective_id=2, has_side_effects=True),
            cost_estimate=cost(8 * toks * dim * ff), name="query_back",
        )(x_all, dht, w_one, w_two, dwi_part)

        loss = (jnp.sum(lse) - jnp.sum(dht[dim:])) / toks
        dw_two, dwi_one, dwi_two = dw_two_t.T, dwi[:dim], dwi[dim:].T
        return loss, d_table, dw_one, dw_two, dwi_one, dwi_two

    return jax.shard_map(local_step, mesh=mesh, in_specs=(P("dp", None), P(), P(), P(), P(), P("dp", None), P(), P(), P("dp")), out_specs=(P(), P("dp", None), P(), P(), P(), P()), check_vma=False)
```

```python
import functools
import math
import jax
import jax.numpy as jnp
from jax import lax
from jax.experimental import pallas as pl
from jax.experimental.pallas import tpu as pltpu
from jax.sharding import PartitionSpec as P

SCORE_GAIN = 3.0
HIT_VALUE = -1e9
EXCLUDED = 3e38
NO_ROW = -1e9
CH = 512
BLK = 512
SUB = 8
PAIR = 2
WIN = 128
FB = 256
TB = 256
GELU_C = math.sqrt(2.0 / math.pi)
BF, F32 = jnp.bfloat16, jnp.float32
MESH = pl.DeviceIdType.MESH
VMEM_LIMIT = 60 * 1024 * 1024


def dot(a, b):
    return lax.dot_general(a, b, (((1,), (0,)), ((), ())), preferred_element_type=F32)


def dot_nt(a, b):
    return lax.dot_general(a, b, (((1,), (1,)), ((), ())), preferred_element_type=F32)


def gelu(x):
    half = 0.5 * x
    return half + half * jnp.tanh(x * (GELU_C + (GELU_C * 0.044715) * (x * x)))


def gelu_pair(x):
    sq = x * x
    th = jnp.tanh(x * (GELU_C + (GELU_C * 0.044715) * sq))
    half = 0.5 * x
    slope = (0.5 + 0.5 * th) + half * (1.0 - th * th) * (GELU_C + (3.0 * 0.044715 * GELU_C) * sq)
    return half + half * th, slope


def column(attr_ref, index, first, count):
    tiles = [attr_ref[first + i].T[:, index : index + 1] for i in range(count)]
    return jnp.concatenate(tiles, axis=0) if count > 1 else tiles[0]


def start_copies(nch_ref, copy):
    def step(i, carry):
        copy(i).start()
        return carry

    lax.fori_loop(0, nch_ref[0], step, 0)


def wait_copies(nch_ref, copy):
    def step(i, carry):
        copy(i).wait()
        return carry

    lax.fori_loop(0, nch_ref[0], step, 0)


def chunk_at(i):
    return pl.ds(pl.multiple_of(i * CH, CH), CH)


def gather_kernel(starts_ref, nch_ref, tbl_ref, attr_ref, rows_hbm, rows, keys, sem):
    step = pl.program_id(0)

    @pl.when(step == 0)
    def _():
        def prepare(i, carry):
            rows[chunk_at(i), :] = jnp.zeros((CH, rows.shape[1]), BF)
            for k in range(CH // WIN):
                at = pl.ds(pl.multiple_of(i * CH + k * WIN, WIN), WIN)
                key = attr_ref[i * (CH // WIN) + k].T[:, 0:1]
                keys[at, :] = jnp.broadcast_to(key, (WIN, WIN))
            return carry

        lax.fori_loop(0, nch_ref[0] + 1, prepare, 0)

    lanes = [(lax.broadcasted_iota(jnp.int32, (1, WIN), 1) + j).astype(F32) for j in range(0, BLK, WIN)]

    def picked(blk, part, at):
        key = keys[pl.ds(at, WIN), :] - (blk * BLK).astype(F32)
        pick = [jnp.where(key == lane, 1.0, 0.0).astype(BF) for lane in lanes]
        return dot(jnp.concatenate(pick, axis=1), tbl_ref[pl.ds(pl.multiple_of(part * BLK, BLK), BLK), :]).astype(BF)

    def some_blocks(i, carry):
        parts = [i * PAIR + k for k in range(PAIR)]
        blks = [step * SUB + part for part in parts]
        firsts = [(starts_ref[blk] >> 4) << 4 for blk in blks]
        gots = [picked(blk, part, pl.multiple_of(first, 16)) for blk, part, first in zip(blks, parts, firsts)]
        for blk, part, first, got in zip(blks, parts, firsts, gots):
            head = pl.ds(pl.multiple_of(first, 16), 16)
            rows[head, :] = rows[head, :] + got[:16]
            rows[pl.ds(pl.multiple_of(first + 16, 16), WIN - 16), :] = got[16:]

            def more(i, carry, blk=blk, part=part, first=first):
                at = pl.multiple_of(first + i * WIN, 16)
                rows[pl.ds(at, WIN), :] = picked(blk, part, at)
                return carry

            lax.fori_loop(1, (starts_ref[blk + 1] - first + (WIN - 1)) >> 7, more, 0)
        return carry

    lax.fori_loop(0, SUB // PAIR, some_blocks, 0)

    @pl.when(step == pl.num_programs(0) - 1)
    def _():
        copy = lambda i: pltpu.make_async_copy(rows.at[chunk_at(i), :], rows_hbm.at[chunk_at(i), :], sem)
        start_copies(nch_ref, copy)
        wait_copies(nch_ref, copy)


def stream(nch, body, ins, outs):
    specs = [[spec for spec, _ in part] for part in (ins, outs)]
    pltpu.emit_pipeline(body, grid=(nch,), in_specs=specs[0], out_specs=specs[1])(*[ref for _, ref in ins + outs])


def fwd_kernel(scale, nch_ref, tid_ref, h_ref, w1_ref, w2_ref, rows_hbm, attr_hbm, u_hbm, pre_hbm, z_hbm, stat_ref, m8, s8):
    m8[...] = jnp.full_like(m8, -EXCLUDED)
    s8[...] = jnp.zeros_like(s8)
    dim, ff, toks = rows_hbm.shape[1], w1_ref.shape[1], h_ref.shape[0]

    def body(rows_ref, attr_ref, u_ref, pre_ref, z_ref):
        rows = rows_ref[...]
        out = None
        for f in range(0, ff, FB):
            pre = dot(rows, w1_ref[:, f : f + FB])
            pre_ref[:, f : f + FB] = pre
            act = gelu(pre).astype(BF)
            part = dot(act, w2_ref[f : f + FB, :])
            out = part if out is None else out + part
        vec = out.astype(BF)
        u_ref[...] = vec
        loc = column(attr_ref, 0, 0, CH // WIN)
        off = column(attr_ref, 1, 0, CH // WIN)
        is_targ = column(attr_ref, 2, 0, CH // WIN) > 0.5
        for t in range(0, toks, TB):
            raw = dot_nt(vec, h_ref[t : t + TB, :]) * scale
            same = loc == tid_ref[:, t : t + TB]
            z = jnp.where(same, jnp.where(is_targ, raw, HIT_VALUE), raw - off)
            z_ref[:, t : t + TB] = z
            z3 = z.reshape(CH // 8, 8, TB)
            old = m8[:, t : t + TB]
            new = jnp.maximum(old, jnp.max(z3, axis=0))
            s8[:, t : t + TB] = s8[:, t : t + TB] * jnp.exp(old - new) + jnp.sum(jnp.exp(z3 - new[None]), axis=0)
            m8[:, t : t + TB] = new

    stream(nch_ref[0], body, [(chunk(dim), rows_hbm), (ATTR_CHUNK, attr_hbm)],
           [(chunk(dim), u_hbm), (chunk(ff), pre_hbm), (chunk(toks), z_hbm)])
    top = jnp.max(m8[...], axis=0, keepdims=True)
    stat_ref[0:1, :] = top
    stat_ref[1:2, :] = jnp.sum(s8[...] * jnp.exp(m8[...] - top), axis=0, keepdims=True)


def logit_back_kernel(scale, nch_ref, tid_ref, lse_ref, h_ref, z_hbm, u_hbm, attr_hbm, g_hbm, dht_ref):
    dht_ref[...] = jnp.zeros_like(dht_ref)
    dim, toks = u_hbm.shape[1], h_ref.shape[0]

    def body(z_ref, u_ref, attr_ref, g_ref):
        vec_t = u_ref[...].T
        loc = column(attr_ref, 0, 0, CH // WIN)
        is_targ = column(attr_ref, 2, 0, CH // WIN)
        shift = is_targ * (-1.0 / toks)
        grad = None
        log_toks = math.log(toks)
        for t in range(0, toks, TB):
            z = z_ref[:, t : t + TB]
            same = loc == tid_ref[:, t : t + TB]
            dz = (jnp.exp(z - (lse_ref[:, t : t + TB] + log_toks)) + jnp.where(same, shift, 0.0)).astype(BF)
            part = dot(dz, h_ref[t : t + TB, :])
            grad = part if grad is None else grad + part
            dht_ref[:dim, t : t + TB] += dot(vec_t, dz)
            zt = jnp.where(same, z * is_targ, 0.0)
            dht_ref[dim:, t : t + TB] += jnp.sum(zt.reshape(CH // 8, 8, TB), axis=0)
        g_ref[...] = (grad * scale).astype(BF)

    stream(nch_ref[0], body, [(chunk(toks), z_hbm), (chunk(dim), u_hbm), (ATTR_CHUNK, attr_hbm)], [(chunk(dim), g_hbm)])


def tower_back_kernel(nch_ref, starts_ref, w1_ref, w2_ref, attr_ref, g_hbm, rows_hbm, pre_hbm, table_hbm, dw_ref, drow, ring, state, ring_sem):
    dw_ref[...] = jnp.zeros_like(dw_ref)
    dim, ff = w1_ref.shape
    n_blk = table_hbm.shape[0] // BLK
    slots = ring.shape[0]
    state[0] = 0
    state[1] = 0

    def clear(i, carry):
        drow[chunk_at(i), :] = jnp.zeros((CH, dim), BF)
        return carry

    lax.fori_loop(0, nch_ref[0] + 1, clear, 0)
    row = lax.broadcasted_iota(jnp.int32, (BLK, WIN), 0).astype(F32)

    def put(blk, tile):
        base = (blk * BLK).astype(F32)
        pick = [jnp.where(attr_ref[tile + k][0:1, :] - base == row, 1.0, 0.0).astype(BF) for k in range(2)]
        return dot(jnp.concatenate(pick, axis=1), drow[pl.ds(pl.multiple_of(tile * WIN, WIN), 2 * WIN), :])

    def write(blk):
        slot = lax.rem(blk, slots)
        return pltpu.make_async_copy(ring.at[slot], table_hbm.at[pl.ds(pl.multiple_of(blk * BLK, BLK), BLK), :], ring_sem.at[slot])

    def build(blk):
        blks = [blk + k for k in range(PAIR)]

        @pl.when(blk >= slots)
        def _():
            for one in blks:
                write(one).wait()

        firsts = [starts_ref[one] >> 7 for one in blks]
        for one, first in zip(blks, firsts):
            ring[lax.rem(one, slots)] = put(one, first)
        for one, first in zip(blks, firsts):
            def more(i, carry, one=one, first=first):
                ring[lax.rem(one, slots)] += put(one, first + 2 * i)
                return carry

            lax.fori_loop(1, (starts_ref[one + 1] - first * WIN + (2 * WIN - 1)) >> 8, more, 0)
            write(one).start()
        return blk + PAIR

    def body(g_ref, rows_ref, pre_ref):
        g = g_ref[...]
        g_t, rows_t = g.T, rows_ref[...].T
        out = None
        for f in range(0, ff, FB):
            act, slope = gelu_pair(pre_ref[:, f : f + FB])
            q = (slope * dot_nt(g, w2_ref[f : f + FB, :])).astype(BF)
            dw_ref[dim:, f : f + FB] += dot(g_t, act.astype(BF))
            dw_ref[:dim, f : f + FB] += dot(rows_t, q)
            part = dot_nt(q, w1_ref[:, f : f + FB])
            out = part if out is None else out + part
        step = state[0]
        drow[chunk_at(step), :] = out.astype(BF)
        done = (step + 1) * CH
        ready = lambda blk: (blk < n_blk) & (starts_ref[jnp.minimum(blk + PAIR, n_blk)] <= done)
        state[1] = lax.while_loop(ready, build, state[1])
        state[0] = step + 1

    stream(nch_ref[0], body, [(chunk(dim), g_hbm), (chunk(dim), rows_hbm), (chunk(ff), pre_hbm)], [])
    for blk in range(n_blk - slots, n_blk):
        write(jnp.int32(blk)).wait()


def query_back_kernel(scale, x_hbm, dht_hbm, w1_hbm, w2_hbm, part_hbm, dw1_hbm, dw2_hbm, dwi1_hbm, dwi2_hbm,
                      dw1_ref, dw2t_ref, sum_ref, flip, x_ref, dht_ref, w1_ref, w2_ref, work, r0, r1, r2, load_sem, store_sem, send_sem, recv_sem):
    me = lax.axis_index("dp")
    core, x, y = lax.rem(me, 2), lax.rem(lax.div(me, 2), 2), lax.div(me, 4)
    pair, x_peer, y_peer = me + 1 - 2 * core, me + 2 - 4 * x, me + 4 - 8 * y
    dim, ff = w1_ref.shape
    half = part_hbm.shape[0] // 2
    p1, p2, p3 = half // 2, half // 4, half // 8
    mine, other = core * half, (1 - core) * half

    barrier = pltpu.get_barrier_semaphore()
    for peer in (pair, x_peer, y_peer):
        pl.semaphore_signal(barrier, inc=1, device_id=(peer,), device_id_type=MESH)
    pl.semaphore_wait(barrier, 3)

    def rows(first, count):
        return pl.ds(pl.multiple_of(first, count), count)

    def send(k, src, dst, peer):
        copy = pltpu.make_async_remote_copy(
            src_ref=src, dst_ref=dst, send_sem=send_sem.at[k], recv_sem=recv_sem.at[k], device_id=(peer,), device_id_type=MESH)
        copy.start()
        return copy

    pair_copy = send(0, part_hbm.at[rows(other, half), :], r0, pair)
    loads = [(part_hbm.at[rows(mine, half), :], work), (x_hbm, x_ref), (dht_hbm.at[rows(0, dim), :], dht_ref), (w1_hbm, w1_ref), (w2_hbm, w2_ref)]
    loads = [pltpu.make_async_copy(src, dst, load_sem.at[i]) for i, (src, dst) in enumerate(loads)]
    for copy in loads:
        copy.start()
    dw1_ref[...] = jnp.zeros_like(dw1_ref)
    dw2t_ref[...] = jnp.zeros_like(dw2t_ref)
    for copy in loads:
        copy.wait()

    def unit(u, carry):
        tok = pl.ds(pl.multiple_of(lax.div(u, 2) * CH, CH), CH)
        first = lax.rem(u, 2) * (ff // 2)
        xs, grad_t = x_ref[tok, :], (dht_ref[:, tok] * scale).astype(BF)
        x_t, grad = xs.T, grad_t.T
        for f in range(0, ff // 2, FB):
            at = pl.ds(pl.multiple_of(first + f, FB), FB)
            act, slope = gelu_pair(dot(xs, w1_ref[:, at]))
            q = (slope * dot_nt(grad, w2_ref[at, :])).astype(BF)
            dw2t_ref[:, at] += dot(grad_t, act.astype(BF))
            dw1_ref[:, at] += dot(x_t, q)
        return carry

    pair_copy.wait()
    work[...] = work[...] + r0[...]
    step = [send(1, work.at[rows((1 - x) * p2, p2), :], r1.at[0], x_peer),
            send(2, work.at[rows(p1 + (1 - y) * p2, p2), :], r1.at[1], y_peer)]
    lax.fori_loop(0, 5, unit, 0)
    for copy in step:
        copy.wait()
    for at, k in ((rows(x * p2, p2), 0), (rows(p1 + y * p2, p2), 1)):
        work[at, :] = work[at, :] + r1[k]
    step = [send(3, work.at[rows(x * p2 + (1 - y) * p3, p3), :], r2.at[0], y_peer),
            send(4, work.at[rows(p1 + y * p2 + (1 - x) * p3, p3), :], r2.at[1], x_peer)]
    lax.fori_loop(5, 2 * (x_ref.shape[0] // CH), unit, 0)
    for copy in step:
        copy.wait()
    piece_a, piece_b = x * p2 + y * p3, p1 + y * p2 + x * p3
    step = []
    for k, piece, peer in ((0, piece_a, y_peer), (1, piece_b, x_peer)):
        at = rows(mine + piece, p3)
        sum_ref[at, :] = work[rows(piece, p3), :] + r2[k]
        step.append(send(5 + k, sum_ref.at[at, :], sum_ref.at[at, :], peer))
    for copy in step:
        copy.wait()
    at_a, at_b = rows(mine + x * p2, p2), rows(mine + p1 + y * p2, p2)
    step = [send(7, sum_ref.at[at_a, :], sum_ref.at[at_a, :], x_peer), send(8, sum_ref.at[at_b, :], sum_ref.at[at_b, :], y_peer)]
    last = [send(9, sum_ref.at[at_a, :], sum_ref.at[at_a, :], pair), send(10, sum_ref.at[at_b, :], sum_ref.at[at_b, :], pair)]
    stores = [pltpu.make_async_copy(dw1_ref, dw1_hbm, store_sem.at[0]), pltpu.make_async_copy(flip.at[0], dw2_hbm, store_sem.at[1])]
    stores[0].start()
    for f in range(0, ff, FB):
        flip[0, f : f + FB, :] = dw2t_ref[:, f : f + FB].T
    stores[1].start()
    for copy in step:
        copy.wait()
    at_a, at_b = rows(mine + (1 - x) * p2, p2), rows(mine + p1 + (1 - y) * p2, p2)
    last += [send(11, sum_ref.at[at_a, :], sum_ref.at[at_a, :], pair), send(12, sum_ref.at[at_b, :], sum_ref.at[at_b, :], pair)]
    for copy in last:
        copy.wait()
    stores += [pltpu.make_async_copy(sum_ref.at[rows(0, dim), :], dwi1_hbm, store_sem.at[2]), pltpu.make_async_copy(flip.at[1], dwi2_hbm, store_sem.at[3])]
    stores[2].start()
    for f in range(0, ff, FB):
        flip[1, f : f + FB, :] = sum_ref[dim:, f : f + FB].T
    stores[3].start()
    for copy in stores:
        copy.wait()


def exchange(n, src_ref, all_ref, send_sem, recv_sem):
    me = lax.axis_index("dp")
    barrier = pltpu.get_barrier_semaphore()
    for k in range(1, n):
        pl.semaphore_signal(barrier, inc=1, device_id=(lax.rem(me + k, n),), device_id_type=MESH)
    pl.semaphore_wait(barrier, n - 1)
    copies = []
    for k in range(1, n):
        copies.append(pltpu.make_async_remote_copy(
            src_ref=src_ref, dst_ref=all_ref.at[me], send_sem=send_sem.at[k - 1], recv_sem=recv_sem.at[k - 1],
            device_id=(lax.rem(me + k, n),), device_id_type=MESH))
        copies[-1].start()
    all_ref[me] = src_ref[...]
    for copy in copies:
        copy.wait()


def targets_kernel(n, src_ref, out_ref, send_sem, recv_sem):
    exchange(n, src_ref, out_ref, send_sem, recv_sem)


def stats_kernel(n, src_ref, lse_ref, stats, send_sem, recv_sem):
    exchange(n, src_ref, stats, send_sem, recv_sem)
    top = stats[0, 0:1, :]
    for i in range(1, n):
        top = jnp.maximum(top, stats[i, 0:1, :])
    total = jnp.zeros_like(top)
    for i in range(n):
        total += stats[i, 1:2, :] * jnp.exp(stats[i, 0:1, :] - top)
    lse_ref[...] = top + jnp.log(total)


def share(kernel, ident, n, src, out, scratch=()):
    vmem = pl.BlockSpec(memory_space=pltpu.VMEM)
    return pl.pallas_call(
        functools.partial(kernel, n), out_shape=out, in_specs=[vmem], out_specs=vmem,
        scratch_shapes=[*scratch, pltpu.SemaphoreType.DMA((n - 1,)), pltpu.SemaphoreType.DMA((n - 1,))],
        compiler_params=pltpu.CompilerParams(collective_id=ident, has_side_effects=True),
    )(src)


def params(**kw):
    return pltpu.CompilerParams(vmem_limit_bytes=VMEM_LIMIT, dimension_semantics=("arbitrary",), **kw)


def cost(flops):
    return pl.CostEstimate(flops=flops, bytes_accessed=64 << 20, transcendentals=0)


def whole(shape):
    return pl.BlockSpec(shape, lambda i, *_: (0,) * len(shape))


def chunk(width):
    return pl.BlockSpec((CH, width), lambda i, *_: (i, 0))


ATTR_CHUNK = pl.BlockSpec((CH // WIN, 8, WIN), lambda i, *_: (i, 0, 0))


def sds(*shape, dtype=F32):
    return jax.ShapeDtypeStruct(shape, dtype)


def query_fwd(x, w_in, w_out):
    pre = jnp.dot(x, w_in, preferred_element_type=F32)
    hidden = jax.nn.gelu(pre).astype(BF)
    return jnp.dot(hidden, w_out, preferred_element_type=F32).astype(BF)


def solution(mesh):
    num_dev = mesh.shape["dp"]

    def local_step(tokens, w_one, w_two, wi_one, wi_two, table, cand_ids, log_q, targ_loc):
        dim = table.shape[1]
        ff = wi_one.shape[1]
        rows_loc = table.shape[0]
        toks = tokens.shape[0] * num_dev
        cands = cand_ids.shape[0]
        cap = cands + toks
        n_blk = rows_loc // BLK
        scale = SCORE_GAIN / math.sqrt(dim)
        base = lax.axis_index("dp") * rows_loc

        query_loc = query_fwd(tokens, w_one, w_two)
        query = lax.all_gather(query_loc, "dp", axis=0, tiled=True)
        x_all = lax.all_gather(tokens, "dp", axis=0, tiled=True)
        targ_all = share(targets_kernel, 0, num_dev, targ_loc[None, :], sds(num_dev, 1, targ_loc.shape[0], dtype=jnp.int32)).reshape(toks)

        ids = jnp.concatenate([cand_ids, targ_all]) - base
        kind = jnp.concatenate([jnp.zeros((cands,), jnp.int32), jnp.ones((toks,), jnp.int32)])
        key = jnp.where((ids >= 0) & (ids < rows_loc), 2 * ids + kind, 2 * rows_loc)
        offs = jnp.concatenate([log_q, jnp.full((toks,), EXCLUDED, F32)])
        bounds = jnp.arange(n_blk + 1, dtype=jnp.int32) * (2 * BLK)
        starts = jnp.sum((key[None, :] < bounds[:, None]).astype(jnp.int32), axis=1)
        nch = jnp.maximum(lax.div(starts[n_blk] + (CH - 1), CH), 1)
        key_s, offs_s = lax.sort((key, offs), num_keys=1, is_stable=False)
        repeat = jnp.concatenate([jnp.zeros((1,), bool), key_s[1:] == key_s[:-1]])
        used = (key_s < 2 * rows_loc) & ~repeat
        attr = jnp.stack([
            jnp.where(used, (key_s >> 1).astype(F32), NO_ROW),
            jnp.where(used, offs_s, EXCLUDED),
            jnp.where(used, (key_s & 1).astype(F32), 0.0),
        ])
        attr = jnp.pad(attr, ((0, 5), (0, 0)))
        pad = jnp.broadcast_to(jnp.array([NO_ROW, EXCLUDED, 0, 0, 0, 0, 0, 0], F32)[:, None], (8, CH))
        attr = jnp.concatenate([attr, pad], axis=1).reshape(8, -1, WIN).transpose(1, 0, 2)
        tid = (targ_all - base).astype(F32)[None, :]
        nch1 = nch[None]

        rows = pl.pallas_call(
            gather_kernel,
            grid_spec=pltpu.PrefetchScalarGridSpec(
                num_scalar_prefetch=2, grid=(n_blk // SUB,),
                in_specs=[pl.BlockSpec((SUB * BLK, dim), lambda i, *_: (i, 0)), whole(attr.shape)],
                out_specs=pl.BlockSpec(memory_space=pl.ANY),
                scratch_shapes=[pltpu.VMEM((cap + CH, dim), BF), pltpu.VMEM((cap + CH, WIN), F32), pltpu.SemaphoreType.DMA]),
            out_shape=sds(cap, dim, dtype=BF), compiler_params=params(), cost_estimate=cost(4 * rows_loc * WIN * dim), name="gather",
        )(starts, nch1, table, attr)

        def call(kernel, name, flops, ins, outs, scratch=()):
            spec = lambda place: pl.BlockSpec(memory_space={True: pltpu.VMEM, False: pl.ANY, None: pltpu.SMEM}[place])
            return pl.pallas_call(
                kernel, in_specs=[spec(None)] + [spec(p) for _, p in ins], out_specs=[spec(p) for _, p in outs],
                out_shape=[o for o, _ in outs], scratch_shapes=list(scratch),
                compiler_params=pltpu.CompilerParams(vmem_limit_bytes=VMEM_LIMIT), cost_estimate=cost(flops), name=name,
            )(nch1, *[a for a, _ in ins])

        bf_list, f_list = sds(cap, dim, dtype=BF), sds(cap, ff)
        vec, pre, z, stat = call(
            functools.partial(fwd_kernel, scale), "fwd", 6 * cap * dim * ff // 4,
            [(tid, True), (query, True), (wi_one, True), (wi_two, True), (rows, False), (attr, False)],
            [(bf_list, False), (f_list, False), (sds(cap, toks), False), (sds(2, toks), True)],
            [pltpu.VMEM((8, toks), F32), pltpu.VMEM((8, toks), F32)])

        stat, x_all = lax.optimization_barrier((stat, x_all))
        lse = share(stats_kernel, 1, num_dev, stat, sds(1, toks), [pltpu.VMEM((num_dev, 2, toks), F32)])

        g, dht_part = call(
            functools.partial(logit_back_kernel, scale), "logit_back", 4 * cap * dim * toks // 4,
            [(tid, True), (lse, True), (query, True), (z, False), (vec, False), (attr, False)],
            [(bf_list, False), (sds(dim + 8, toks), True)])

        dht = lax.psum(dht_part, "dp")
        d_table, dwi_part = call(
            tower_back_kernel, "tower_back", 8 * cap * dim * ff // 4,
            [(starts, None), (wi_one, True), (wi_two, True), (attr, True), (g, False), (rows, False), (pre, False)],
            [(sds(rows_loc, dim), False), (sds(2 * dim, ff), True)],
            [pltpu.VMEM((cap + CH, dim), BF), pltpu.VMEM((4, BLK, dim), F32), pltpu.SMEM((2,), jnp.int32), pltpu.SemaphoreType.DMA((4,))])

        any_spec = pl.BlockSpec(memory_space=pl.ANY)
        dw_one, dw_two, dwi_one, dwi_two = pl.pallas_call(
            functools.partial(query_back_kernel, scale),
            in_specs=[any_spec] * 5, out_specs=[any_spec] * 4,
            out_shape=[sds(dim, ff), sds(ff, dim), sds(dim, ff), sds(ff, dim)],
            scratch_shapes=[
                pltpu.VMEM((dim, ff), F32), pltpu.VMEM((dim, ff), F32), pltpu.VMEM((2 * dim, ff), F32), pltpu.VMEM((2, ff, dim), F32),
                pltpu.VMEM((toks, dim), BF), pltpu.VMEM((dim, toks), F32), pltpu.VMEM((dim, ff), BF), pltpu.VMEM((ff, dim), BF),
                pltpu.VMEM((dim, ff), F32), pltpu.VMEM((dim, ff), F32),
                pltpu.VMEM((2, dim // 4, ff), F32), pltpu.VMEM((2, dim // 8, ff), F32),
                pltpu.SemaphoreType.DMA((5,)), pltpu.SemaphoreType.DMA((4,)), pltpu.SemaphoreType.DMA((13,)), pltpu.SemaphoreType.DMA((13,))],
            compiler_params=pltpu.CompilerParams(vmem_limit_bytes=VMEM_LIMIT, collective_id=2, has_side_effects=True),
            cost_estimate=cost(8 * toks * dim * ff), name="query_back",
        )(x_all, dht, w_one, w_two, dwi_part)

        loss = (jnp.sum(lse) - jnp.sum(dht[dim:])) / toks
        return loss, d_table, dw_one, dw_two, dwi_one, dwi_two

    return jax.shard_map(local_step, mesh=mesh, in_specs=(P("dp", None), P(), P(), P(), P(), P("dp", None), P(), P(), P("dp")), out_specs=(P(), P("dp", None), P(), P(), P(), P()), check_vma=False)
```

```python
import functools
import math
import jax
import jax.numpy as jnp
from jax import lax
from jax.experimental import pallas as pl
from jax.experimental.pallas import tpu as pltpu
from jax.sharding import PartitionSpec as P

SCORE_GAIN = 3.0
HIT_VALUE = -1e9
EXCLUDED = 3e38
NO_ROW = -1e9
CH = 512
BLK = 512
TCH = 512
SUB = 8
PAIR = 2
WIN = 128
FB = 256
TB = 256
GELU_C = math.sqrt(2.0 / math.pi)
BF, F32 = jnp.bfloat16, jnp.float32
MESH = pl.DeviceIdType.MESH
VMEM_LIMIT = 60 * 1024 * 1024


def dot(a, b):
    return lax.dot_general(a, b, (((1,), (0,)), ((), ())), preferred_element_type=F32)


def dot_nt(a, b):
    return lax.dot_general(a, b, (((1,), (1,)), ((), ())), preferred_element_type=F32)


def gelu(x):
    half = 0.5 * x
    return half + half * jnp.tanh(x * (GELU_C + (GELU_C * 0.044715) * (x * x)))


def gelu_pair(x):
    sq = x * x
    th = jnp.tanh(x * (GELU_C + (GELU_C * 0.044715) * sq))
    half = 0.5 * x
    slope = (0.5 + 0.5 * th) + half * (1.0 - th * th) * (GELU_C + (3.0 * 0.044715 * GELU_C) * sq)
    return half + half * th, slope


def column(attr_ref, index, first, count):
    tiles = [attr_ref[first + i].T[:, index : index + 1] for i in range(count)]
    return jnp.concatenate(tiles, axis=0) if count > 1 else tiles[0]


def start_copies(nch_ref, copy):
    def step(i, carry):
        copy(i).start()
        return carry

    lax.fori_loop(0, nch_ref[0], step, 0)


def wait_copies(nch_ref, copy):
    def step(i, carry):
        copy(i).wait()
        return carry

    lax.fori_loop(0, nch_ref[0], step, 0)


def chunk_at(i):
    return pl.ds(pl.multiple_of(i * CH, CH), CH)


def gather_kernel(starts_ref, nch_ref, tbl_ref, attr_ref, rows_hbm, rows, keys, sem):
    step = pl.program_id(0)

    @pl.when(step == 0)
    def _():
        def prepare(i, carry):
            rows[chunk_at(i), :] = jnp.zeros((CH, rows.shape[1]), BF)
            for k in range(CH // WIN):
                at = pl.ds(pl.multiple_of(i * CH + k * WIN, WIN), WIN)
                key = attr_ref[i * (CH // WIN) + k].T[:, 0:1]
                keys[at, :] = jnp.broadcast_to(key, (WIN, WIN))
            return carry

        lax.fori_loop(0, nch_ref[0] + 1, prepare, 0)

    lanes = [(lax.broadcasted_iota(jnp.int32, (1, WIN), 1) + j).astype(F32) for j in range(0, BLK, WIN)]

    def picked(blk, part, at):
        key = keys[pl.ds(at, WIN), :] - (blk * BLK).astype(F32)
        pick = [jnp.where(key == lane, 1.0, 0.0).astype(BF) for lane in lanes]
        return dot(jnp.concatenate(pick, axis=1), tbl_ref[pl.ds(pl.multiple_of(part * BLK, BLK), BLK), :]).astype(BF)

    def some_blocks(i, carry):
        parts = [i * PAIR + k for k in range(PAIR)]
        blks = [step * SUB + part for part in parts]
        firsts = [(starts_ref[blk] >> 4) << 4 for blk in blks]
        gots = [picked(blk, part, pl.multiple_of(first, 16)) for blk, part, first in zip(blks, parts, firsts)]
        for blk, part, first, got in zip(blks, parts, firsts, gots):
            head = pl.ds(pl.multiple_of(first, 16), 16)
            rows[head, :] = rows[head, :] + got[:16]
            rows[pl.ds(pl.multiple_of(first + 16, 16), WIN - 16), :] = got[16:]

            def more(i, carry, blk=blk, part=part, first=first):
                at = pl.multiple_of(first + i * WIN, 16)
                rows[pl.ds(at, WIN), :] = picked(blk, part, at)
                return carry

            lax.fori_loop(1, (starts_ref[blk + 1] - first + (WIN - 1)) >> 7, more, 0)
        return carry

    lax.fori_loop(0, SUB // PAIR, some_blocks, 0)

    @pl.when(step == pl.num_programs(0) - 1)
    def _():
        copy = lambda i: pltpu.make_async_copy(rows.at[chunk_at(i), :], rows_hbm.at[chunk_at(i), :], sem)
        start_copies(nch_ref, copy)
        wait_copies(nch_ref, copy)


def stream(nch, body, ins, outs):
    specs = [[spec for spec, _ in part] for part in (ins, outs)]
    pltpu.emit_pipeline(body, grid=(nch,), in_specs=specs[0], out_specs=specs[1])(*[ref for _, ref in ins + outs])


def fwd_kernel(scale, nch_ref, tid_ref, h_ref, w1_ref, w2_ref, rows_hbm, attr_hbm, u_hbm, pre_hbm, z_hbm, stat_ref, m8, s8):
    m8[...] = jnp.full_like(m8, -EXCLUDED)
    s8[...] = jnp.zeros_like(s8)
    dim, ff, toks = rows_hbm.shape[1], w1_ref.shape[1], h_ref.shape[0]

    def body(rows_ref, attr_ref, u_ref, pre_ref, z_ref):
        rows = rows_ref[...]
        out = None
        for f in range(0, ff, FB):
            pre = dot(rows, w1_ref[:, f : f + FB])
            pre_ref[:, f : f + FB] = pre
            act = gelu(pre).astype(BF)
            part = dot(act, w2_ref[f : f + FB, :])
            out = part if out is None else out + part
        vec = out.astype(BF)
        u_ref[...] = vec
        loc = column(attr_ref, 0, 0, CH // WIN)
        off = column(attr_ref, 1, 0, CH // WIN)
        is_targ = column(attr_ref, 2, 0, CH // WIN) > 0.5
        for t in range(0, toks, TB):
            raw = dot_nt(vec, h_ref[t : t + TB, :]) * scale
            same = loc == tid_ref[:, t : t + TB]
            z = jnp.where(same, jnp.where(is_targ, raw, HIT_VALUE), raw - off)
            z_ref[:, t : t + TB] = z
            z3 = z.reshape(CH // 8, 8, TB)
            old = m8[:, t : t + TB]
            new = jnp.maximum(old, jnp.max(z3, axis=0))
            s8[:, t : t + TB] = s8[:, t : t + TB] * jnp.exp(old - new) + jnp.sum(jnp.exp(z3 - new[None]), axis=0)
            m8[:, t : t + TB] = new

    stream(nch_ref[0], body, [(chunk(dim), rows_hbm), (ATTR_CHUNK, attr_hbm)],
           [(chunk(dim), u_hbm), (chunk(ff), pre_hbm), (chunk(toks), z_hbm)])
    top = jnp.max(m8[...], axis=0, keepdims=True)
    stat_ref[0:1, :] = top
    stat_ref[1:2, :] = jnp.sum(s8[...] * jnp.exp(m8[...] - top), axis=0, keepdims=True)


def logit_back_kernel(scale, nch_ref, tid_ref, lse_ref, h_ref, z_hbm, u_hbm, attr_hbm, g_hbm, dht_ref):
    dht_ref[...] = jnp.zeros_like(dht_ref)
    dim, toks = u_hbm.shape[1], h_ref.shape[0]

    def body(z_ref, u_ref, attr_ref, g_ref):
        vec_t = u_ref[...].T
        loc = column(attr_ref, 0, 0, CH // WIN)
        is_targ = column(attr_ref, 2, 0, CH // WIN)
        shift = is_targ * (-1.0 / toks)
        grad = None
        log_toks = math.log(toks)
        for t in range(0, toks, TB):
            z = z_ref[:, t : t + TB]
            same = loc == tid_ref[:, t : t + TB]
            dz = (jnp.exp(z - (lse_ref[:, t : t + TB] + log_toks)) + jnp.where(same, shift, 0.0)).astype(BF)
            part = dot(dz, h_ref[t : t + TB, :])
            grad = part if grad is None else grad + part
            dht_ref[:dim, t : t + TB] += dot(vec_t, dz)
            zt = jnp.where(same, z * is_targ, 0.0)
            dht_ref[dim:, t : t + TB] += jnp.sum(zt.reshape(CH // 8, 8, TB), axis=0)
        g_ref[...] = (grad * scale).astype(BF)

    stream(nch_ref[0], body, [(chunk(toks), z_hbm), (chunk(dim), u_hbm), (ATTR_CHUNK, attr_hbm)], [(chunk(dim), g_hbm)])


def tower_back_kernel(nch_ref, starts_ref, w1_ref, w2_ref, attr_ref, g_hbm, rows_hbm, pre_hbm, table_hbm, dw_ref, drow, ring, state, ring_sem):
    dw_ref[...] = jnp.zeros_like(dw_ref)
    dim, ff = w1_ref.shape
    n_blk = table_hbm.shape[0] // BLK
    slots = ring.shape[0]
    state[0] = 0
    state[1] = 0

    def clear(i, carry):
        drow[chunk_at(i), :] = jnp.zeros((CH, dim), BF)
        return carry

    lax.fori_loop(0, nch_ref[0] + 1, clear, 0)
    row = lax.broadcasted_iota(jnp.int32, (BLK, WIN), 0).astype(F32)

    def put(blk, tile):
        base = (blk * BLK).astype(F32)
        pick = [jnp.where(attr_ref[tile + k][0:1, :] - base == row, 1.0, 0.0).astype(BF) for k in range(2)]
        return dot(jnp.concatenate(pick, axis=1), drow[pl.ds(pl.multiple_of(tile * WIN, WIN), 2 * WIN), :])

    def write(blk):
        slot = lax.rem(blk, slots)
        return pltpu.make_async_copy(ring.at[slot], table_hbm.at[pl.ds(pl.multiple_of(blk * BLK, BLK), BLK), :], ring_sem.at[slot])

    def build(blk):
        blks = [blk + k for k in range(PAIR)]

        @pl.when(blk >= slots)
        def _():
            for one in blks:
                write(one).wait()

        firsts = [starts_ref[one] >> 7 for one in blks]
        for one, first in zip(blks, firsts):
            ring[lax.rem(one, slots)] = put(one, first)
        for one, first in zip(blks, firsts):
            def more(i, carry, one=one, first=first):
                ring[lax.rem(one, slots)] += put(one, first + 2 * i)
                return carry

            lax.fori_loop(1, (starts_ref[one + 1] - first * WIN + (2 * WIN - 1)) >> 8, more, 0)
            write(one).start()
        return blk + PAIR

    def body(g_ref, rows_ref, pre_ref):
        g = g_ref[...]
        g_t, rows_t = g.T, rows_ref[...].T
        out = None
        for f in range(0, ff, FB):
            act, slope = gelu_pair(pre_ref[:, f : f + FB])
            q = (slope * dot_nt(g, w2_ref[f : f + FB, :])).astype(BF)
            dw_ref[dim:, f : f + FB] += dot(g_t, act.astype(BF))
            dw_ref[:dim, f : f + FB] += dot(rows_t, q)
            part = dot_nt(q, w1_ref[:, f : f + FB])
            out = part if out is None else out + part
        step = state[0]
        drow[chunk_at(step), :] = out.astype(BF)
        done = (step + 1) * CH
        ready = lambda blk: (blk < n_blk) & (starts_ref[jnp.minimum(blk + PAIR, n_blk)] <= done)
        state[1] = lax.while_loop(ready, build, state[1])
        state[0] = step + 1

    stream(nch_ref[0], body, [(chunk(dim), g_hbm), (chunk(dim), rows_hbm), (chunk(ff), pre_hbm)], [])
    for blk in range(n_blk - slots, n_blk):
        write(jnp.int32(blk)).wait()


def query_back_kernel(scale, x_hbm, dht_hbm, w1_hbm, w2_hbm, part_hbm, dw1_hbm, dw2_hbm, dwi1_hbm, dwi2_hbm,
                      dw1_ref, dw2t_ref, sum_ref, flip, x_ref, x_t, dht_ref, grad_t, grad, w1_ref, w2_ref, work, r0, r1, r2,
                      load_sem, store_sem, send_sem, recv_sem):
    me = lax.axis_index("dp")
    core, x, y = lax.rem(me, 2), lax.rem(lax.div(me, 2), 2), lax.div(me, 4)
    pair, x_peer, y_peer = me + 1 - 2 * core, me + 2 - 4 * x, me + 4 - 8 * y
    dim, ff = w1_ref.shape
    toks = x_ref.shape[0]
    half = dim // 2
    p1, p2, p3 = half // 2, half // 4, half // 8

    barrier = pltpu.get_barrier_semaphore()
    for peer in (pair, x_peer, y_peer):
        pl.semaphore_signal(barrier, inc=1, device_id=(peer,), device_id_type=MESH)
    pl.semaphore_wait(barrier, 3)

    def rows(first, count):
        return pl.ds(pl.multiple_of(first, count), count)

    def send(j, k, src, dst, peer):
        sems = send_sem.at[13 * j + k], recv_sem.at[13 * j + k]
        copy = pltpu.make_async_remote_copy(
            src_ref=src, dst_ref=dst, send_sem=sems[0], recv_sem=sems[1], device_id=(peer,), device_id_type=MESH)
        copy.start()
        return copy

    def wait(copies):
        for copy in copies:
            copy.wait()

    def mine(j):
        return j * dim + core * half

    def stage0(j):
        return [send(j, 0, part_hbm.at[rows(j * dim + (1 - core) * half, half), :], r0.at[j], pair)]

    def stage1(j):
        work[j] = work[j] + r0[j]
        return [send(j, 1, work.at[j, rows((1 - x) * p2, p2), :], r1.at[j, 0], x_peer),
                send(j, 2, work.at[j, rows(p1 + (1 - y) * p2, p2), :], r1.at[j, 1], y_peer)]

    def stage2(j):
        for at, k in ((rows(x * p2, p2), 0), (rows(p1 + y * p2, p2), 1)):
            work[j, at, :] = work[j, at, :] + r1[j, k]
        return [send(j, 3, work.at[j, rows(x * p2 + (1 - y) * p3, p3), :], r2.at[j, 0], y_peer),
                send(j, 4, work.at[j, rows(p1 + y * p2 + (1 - x) * p3, p3), :], r2.at[j, 1], x_peer)]

    def share_rows(j, k, first, count, peer):
        at = rows(mine(j) + first, count)
        return send(j, k, sum_ref.at[at, :], sum_ref.at[at, :], peer)

    def stage3(j):
        piece_a, piece_b = x * p2 + y * p3, p1 + y * p2 + x * p3
        for k, piece in ((0, piece_a), (1, piece_b)):
            sum_ref[rows(mine(j) + piece, p3), :] = work[j, rows(piece, p3), :] + r2[j, k]
        return [share_rows(j, 5, piece_a, p3, y_peer), share_rows(j, 6, piece_b, p3, x_peer)]

    def stage4(j):
        step = [share_rows(j, 7, x * p2, p2, x_peer), share_rows(j, 8, p1 + y * p2, p2, y_peer)]
        return step, [share_rows(j, 9, x * p2, p2, pair), share_rows(j, 10, p1 + y * p2, p2, pair)]

    def stage5(j):
        return [share_rows(j, 11, (1 - x) * p2, p2, pair), share_rows(j, 12, p1 + (1 - y) * p2, p2, pair)]

    step = [stage0(0), stage0(1)]
    loads = [(part_hbm.at[rows(mine(j), half), :], work.at[j]) for j in range(2)]
    loads += [(x_hbm, x_ref), (dht_hbm.at[rows(0, dim), :], dht_ref), (w1_hbm, w1_ref), (w2_hbm, w2_ref)]
    loads = [pltpu.make_async_copy(src, dst, load_sem.at[i]) for i, (src, dst) in enumerate(loads)]
    for copy in loads:
        copy.start()
    dw1_ref[...] = jnp.zeros_like(dw1_ref)
    dw2t_ref[...] = jnp.zeros_like(dw2t_ref)
    wait(loads)

    def turn(i, carry):
        tok = pl.ds(pl.multiple_of(i * TCH, TCH), TCH)
        x_t[:, tok] = x_ref[tok, :].T
        block = (dht_ref[:, tok] * scale).astype(BF)
        grad_t[:, tok] = block
        grad[tok, :] = block.T
        return carry

    blocks = ff // FB

    def unit(u, carry):
        tok = pl.ds(pl.multiple_of(lax.div(u, blocks) * TCH, TCH), TCH)
        at = pl.ds(pl.multiple_of(lax.rem(u, blocks) * FB, FB), FB)
        act, slope = gelu_pair(dot(x_ref[tok, :], w1_ref[:, at]))
        q = (slope * dot_nt(grad[tok, :], w2_ref[at, :])).astype(BF)
        dw2t_ref[:, at] += dot(grad_t[:, tok], act.astype(BF))
        dw1_ref[:, at] += dot(x_t[:, tok], q)
        return carry

    units = toks // TCH * blocks
    wait(step[0])
    step[0] = stage1(0)
    wait(step[1])
    step[1] = stage1(1)
    lax.fori_loop(0, toks // TCH, turn, 0)
    lax.fori_loop(0, units // 4, unit, 0)
    wait(step[0])
    step[0] = stage2(0)
    lax.fori_loop(units // 4, units // 2, unit, 0)
    wait(step[1])
    step[1] = stage2(1)
    lax.fori_loop(units // 2, units * 5 // 8, unit, 0)
    wait(step[0])
    step[0] = stage3(0)
    lax.fori_loop(units * 5 // 8, units * 3 // 4, unit, 0)
    wait(step[1])
    step[1] = stage3(1)
    lax.fori_loop(units * 3 // 4, units, unit, 0)
    wait(step[0])
    step[0], last0 = stage4(0)
    wait(step[1])
    step[1], last1 = stage4(1)
    stores = [pltpu.make_async_copy(dw1_ref, dw1_hbm, store_sem.at[0]), pltpu.make_async_copy(flip.at[0], dw2_hbm, store_sem.at[1])]
    stores[0].start()
    for f in range(0, ff, FB):
        flip[0, f : f + FB, :] = dw2t_ref[:, f : f + FB].T
    stores[1].start()
    wait(step[0])
    last0 += stage5(0)
    wait(last0)
    stores += [pltpu.make_async_copy(sum_ref.at[rows(0, dim), :], dwi1_hbm, store_sem.at[2]), pltpu.make_async_copy(flip.at[1], dwi2_hbm, store_sem.at[3])]
    stores[2].start()
    wait(step[1])
    last1 += stage5(1)
    wait(last1)
    for f in range(0, ff, FB):
        flip[1, f : f + FB, :] = sum_ref[dim:, f : f + FB].T
    stores[3].start()
    wait(stores)


def exchange(n, src_ref, all_ref, send_sem, recv_sem):
    me = lax.axis_index("dp")
    barrier = pltpu.get_barrier_semaphore()
    for k in range(1, n):
        pl.semaphore_signal(barrier, inc=1, device_id=(lax.rem(me + k, n),), device_id_type=MESH)
    pl.semaphore_wait(barrier, n - 1)
    copies = []
    for k in range(1, n):
        copies.append(pltpu.make_async_remote_copy(
            src_ref=src_ref, dst_ref=all_ref.at[me], send_sem=send_sem.at[k - 1], recv_sem=recv_sem.at[k - 1],
            device_id=(lax.rem(me + k, n),), device_id_type=MESH))
        copies[-1].start()
    all_ref[me] = src_ref[...]
    for copy in copies:
        copy.wait()


def targets_kernel(n, src_ref, out_ref, send_sem, recv_sem):
    exchange(n, src_ref, out_ref, send_sem, recv_sem)


def stats_kernel(n, src_ref, lse_ref, stats, send_sem, recv_sem):
    exchange(n, src_ref, stats, send_sem, recv_sem)
    top = stats[0, 0:1, :]
    for i in range(1, n):
        top = jnp.maximum(top, stats[i, 0:1, :])
    total = jnp.zeros_like(top)
    for i in range(n):
        total += stats[i, 1:2, :] * jnp.exp(stats[i, 0:1, :] - top)
    lse_ref[...] = top + jnp.log(total)


def share(kernel, ident, n, src, out, scratch=()):
    vmem = pl.BlockSpec(memory_space=pltpu.VMEM)
    return pl.pallas_call(
        functools.partial(kernel, n), out_shape=out, in_specs=[vmem], out_specs=vmem,
        scratch_shapes=[*scratch, pltpu.SemaphoreType.DMA((n - 1,)), pltpu.SemaphoreType.DMA((n - 1,))],
        compiler_params=pltpu.CompilerParams(collective_id=ident, has_side_effects=True),
    )(src)


def params(**kw):
    return pltpu.CompilerParams(vmem_limit_bytes=VMEM_LIMIT, dimension_semantics=("arbitrary",), **kw)


def cost(flops):
    return pl.CostEstimate(flops=flops, bytes_accessed=64 << 20, transcendentals=0)


def whole(shape):
    return pl.BlockSpec(shape, lambda i, *_: (0,) * len(shape))


def chunk(width):
    return pl.BlockSpec((CH, width), lambda i, *_: (i, 0))


ATTR_CHUNK = pl.BlockSpec((CH // WIN, 8, WIN), lambda i, *_: (i, 0, 0))


def sds(*shape, dtype=F32):
    return jax.ShapeDtypeStruct(shape, dtype)


def query_fwd(x, w_in, w_out):
    pre = jnp.dot(x, w_in, preferred_element_type=F32)
    hidden = jax.nn.gelu(pre).astype(BF)
    return jnp.dot(hidden, w_out, preferred_element_type=F32).astype(BF)


def solution(mesh):
    num_dev = mesh.shape["dp"]

    def local_step(tokens, w_one, w_two, wi_one, wi_two, table, cand_ids, log_q, targ_loc):
        dim = table.shape[1]
        ff = wi_one.shape[1]
        rows_loc = table.shape[0]
        toks = tokens.shape[0] * num_dev
        cands = cand_ids.shape[0]
        cap = cands + toks
        n_blk = rows_loc // BLK
        scale = SCORE_GAIN / math.sqrt(dim)
        base = lax.axis_index("dp") * rows_loc

        query_loc = query_fwd(tokens, w_one, w_two)
        query = lax.all_gather(query_loc, "dp", axis=0, tiled=True)
        x_all = lax.all_gather(tokens, "dp", axis=0, tiled=True)
        targ_all = share(targets_kernel, 0, num_dev, targ_loc[None, :], sds(num_dev, 1, targ_loc.shape[0], dtype=jnp.int32)).reshape(toks)

        ids = jnp.concatenate([cand_ids, targ_all]) - base
        kind = jnp.concatenate([jnp.zeros((cands,), jnp.int32), jnp.ones((toks,), jnp.int32)])
        key = jnp.where((ids >= 0) & (ids < rows_loc), 2 * ids + kind, 2 * rows_loc)
        offs = jnp.concatenate([log_q, jnp.full((toks,), EXCLUDED, F32)])
        bounds = jnp.arange(n_blk + 1, dtype=jnp.int32) * (2 * BLK)
        starts = jnp.sum((key[None, :] < bounds[:, None]).astype(jnp.int32), axis=1)
        nch = jnp.maximum(lax.div(starts[n_blk] + (CH - 1), CH), 1)
        key_s, offs_s = lax.sort((key, offs), num_keys=1, is_stable=False)
        repeat = jnp.concatenate([jnp.zeros((1,), bool), key_s[1:] == key_s[:-1]])
        used = (key_s < 2 * rows_loc) & ~repeat
        attr = jnp.stack([
            jnp.where(used, (key_s >> 1).astype(F32), NO_ROW),
            jnp.where(used, offs_s, EXCLUDED),
            jnp.where(used, (key_s & 1).astype(F32), 0.0),
        ])
        attr = jnp.pad(attr, ((0, 5), (0, 0)))
        pad = jnp.broadcast_to(jnp.array([NO_ROW, EXCLUDED, 0, 0, 0, 0, 0, 0], F32)[:, None], (8, CH))
        attr = jnp.concatenate([attr, pad], axis=1).reshape(8, -1, WIN).transpose(1, 0, 2)
        tid = (targ_all - base).astype(F32)[None, :]
        nch1 = nch[None]

        rows = pl.pallas_call(
            gather_kernel,
            grid_spec=pltpu.PrefetchScalarGridSpec(
                num_scalar_prefetch=2, grid=(n_blk // SUB,),
                in_specs=[pl.BlockSpec((SUB * BLK, dim), lambda i, *_: (i, 0)), whole(attr.shape)],
                out_specs=pl.BlockSpec(memory_space=pl.ANY),
                scratch_shapes=[pltpu.VMEM((cap + CH, dim), BF), pltpu.VMEM((cap + CH, WIN), F32), pltpu.SemaphoreType.DMA]),
            out_shape=sds(cap, dim, dtype=BF), compiler_params=params(), cost_estimate=cost(4 * rows_loc * WIN * dim), name="gather",
        )(starts, nch1, table, attr)

        def call(kernel, name, flops, ins, outs, scratch=()):
            spec = lambda place: pl.BlockSpec(memory_space={True: pltpu.VMEM, False: pl.ANY, None: pltpu.SMEM}[place])
            return pl.pallas_call(
                kernel, in_specs=[spec(None)] + [spec(p) for _, p in ins], out_specs=[spec(p) for _, p in outs],
                out_shape=[o for o, _ in outs], scratch_shapes=list(scratch),
                compiler_params=pltpu.CompilerParams(vmem_limit_bytes=VMEM_LIMIT), cost_estimate=cost(flops), name=name,
            )(nch1, *[a for a, _ in ins])

        bf_list, f_list = sds(cap, dim, dtype=BF), sds(cap, ff)
        vec, pre, z, stat = call(
            functools.partial(fwd_kernel, scale), "fwd", 6 * cap * dim * ff // 4,
            [(tid, True), (query, True), (wi_one, True), (wi_two, True), (rows, False), (attr, False)],
            [(bf_list, False), (f_list, False), (sds(cap, toks), False), (sds(2, toks), True)],
            [pltpu.VMEM((8, toks), F32), pltpu.VMEM((8, toks), F32)])

        stat, x_all = lax.optimization_barrier((stat, x_all))
        lse = share(stats_kernel, 1, num_dev, stat, sds(1, toks), [pltpu.VMEM((num_dev, 2, toks), F32)])

        g, dht_part = call(
            functools.partial(logit_back_kernel, scale), "logit_back", 4 * cap * dim * toks // 4,
            [(tid, True), (lse, True), (query, True), (z, False), (vec, False), (attr, False)],
            [(bf_list, False), (sds(dim + 8, toks), True)])

        dht = lax.psum(dht_part, "dp")
        d_table, dwi_part = call(
            tower_back_kernel, "tower_back", 8 * cap * dim * ff // 4,
            [(starts, None), (wi_one, True), (wi_two, True), (attr, True), (g, False), (rows, False), (pre, False)],
            [(sds(rows_loc, dim), False), (sds(2 * dim, ff), True)],
            [pltpu.VMEM((cap + CH, dim), BF), pltpu.VMEM((8, BLK, dim), F32), pltpu.SMEM((2,), jnp.int32), pltpu.SemaphoreType.DMA((8,))])

        any_spec = pl.BlockSpec(memory_space=pl.ANY)
        dw_one, dw_two, dwi_one, dwi_two = pl.pallas_call(
            functools.partial(query_back_kernel, scale),
            in_specs=[any_spec] * 5, out_specs=[any_spec] * 4,
            out_shape=[sds(dim, ff), sds(ff, dim), sds(dim, ff), sds(ff, dim)],
            scratch_shapes=[
                pltpu.VMEM((dim, ff), F32), pltpu.VMEM((dim, ff), F32), pltpu.VMEM((2 * dim, ff), F32), pltpu.VMEM((2, ff, dim), F32),
                pltpu.VMEM((toks, dim), BF), pltpu.VMEM((dim, toks), BF), pltpu.VMEM((dim, toks), F32), pltpu.VMEM((dim, toks), BF),
                pltpu.VMEM((toks, dim), BF), pltpu.VMEM((dim, ff), BF), pltpu.VMEM((ff, dim), BF),
                pltpu.VMEM((2, dim // 2, ff), F32), pltpu.VMEM((2, dim // 2, ff), F32),
                pltpu.VMEM((2, 2, dim // 8, ff), F32), pltpu.VMEM((2, 2, dim // 16, ff), F32),
                pltpu.SemaphoreType.DMA((6,)), pltpu.SemaphoreType.DMA((4,)), pltpu.SemaphoreType.DMA((26,)), pltpu.SemaphoreType.DMA((26,))],
            compiler_params=pltpu.CompilerParams(vmem_limit_bytes=VMEM_LIMIT, collective_id=2, has_side_effects=True),
            cost_estimate=cost(8 * toks * dim * ff), name="query_back",
        )(x_all, dht, w_one, w_two, dwi_part)

        loss = (jnp.sum(lse) - jnp.sum(dht[dim:])) / toks
        return loss, d_table, dw_one, dw_two, dwi_one, dwi_two

    return jax.shard_map(local_step, mesh=mesh, in_specs=(P("dp", None), P(), P(), P(), P(), P("dp", None), P(), P(), P("dp")), out_specs=(P(), P("dp", None), P(), P(), P(), P()), check_vma=False)
```

```python
import functools
import math
import jax
import jax.numpy as jnp
from jax import lax
from jax.experimental import pallas as pl
from jax.experimental.pallas import tpu as pltpu
from jax.sharding import PartitionSpec as P

SCORE_GAIN = 3.0
HIT_VALUE = -1e9
EXCLUDED = 3e38
NO_ROW = -1e9
CH = 512
BLK = 512
TCH = 512
SUB = 8
PAIR = 2
GROUP = 4
WIN = 128
FB = 256
TB = 256
GELU_C = math.sqrt(2.0 / math.pi)
BF, F32 = jnp.bfloat16, jnp.float32
MESH = pl.DeviceIdType.MESH
VMEM_LIMIT = 60 * 1024 * 1024


def dot(a, b):
    return lax.dot_general(a, b, (((1,), (0,)), ((), ())), preferred_element_type=F32)


def dot_nt(a, b):
    return lax.dot_general(a, b, (((1,), (1,)), ((), ())), preferred_element_type=F32)


def gelu(x):
    half = 0.5 * x
    return half + half * jnp.tanh(x * (GELU_C + (GELU_C * 0.044715) * (x * x)))


def gelu_pair(x):
    sq = x * x
    th = jnp.tanh(x * (GELU_C + (GELU_C * 0.044715) * sq))
    half = 0.5 * x
    slope = (0.5 + 0.5 * th) + half * (1.0 - th * th) * (GELU_C + (3.0 * 0.044715 * GELU_C) * sq)
    return half + half * th, slope


def column(attr_ref, index, first, count):
    tiles = [attr_ref[first + i].T[:, index : index + 1] for i in range(count)]
    return jnp.concatenate(tiles, axis=0) if count > 1 else tiles[0]


def start_copies(nch_ref, copy):
    def step(i, carry):
        copy(i).start()
        return carry

    lax.fori_loop(0, nch_ref[0], step, 0)


def wait_copies(nch_ref, copy):
    def step(i, carry):
        copy(i).wait()
        return carry

    lax.fori_loop(0, nch_ref[0], step, 0)


def chunk_at(i):
    return pl.ds(pl.multiple_of(i * CH, CH), CH)


def gather_kernel(starts_ref, nch_ref, tbl_ref, attr_ref, rows_hbm, rows, keys, sem):
    step = pl.program_id(0)

    @pl.when(step == 0)
    def _():
        def prepare(i, carry):
            rows[chunk_at(i), :] = jnp.zeros((CH, rows.shape[1]), BF)
            for k in range(CH // WIN):
                at = pl.ds(pl.multiple_of(i * CH + k * WIN, WIN), WIN)
                key = attr_ref[i * (CH // WIN) + k].T[:, 0:1]
                keys[at, :] = jnp.broadcast_to(key, (WIN, WIN))
            return carry

        lax.fori_loop(0, nch_ref[0] + 1, prepare, 0)

    lanes = [(lax.broadcasted_iota(jnp.int32, (1, WIN), 1) + j).astype(F32) for j in range(0, BLK, WIN)]

    def picked(blk, part, at):
        key = keys[pl.ds(at, WIN), :] - (blk * BLK).astype(F32)
        pick = [jnp.where(key == lane, 1.0, 0.0).astype(BF) for lane in lanes]
        return dot(jnp.concatenate(pick, axis=1), tbl_ref[pl.ds(pl.multiple_of(part * BLK, BLK), BLK), :]).astype(BF)

    def some_blocks(i, carry):
        parts = [i * GROUP + k for k in range(GROUP)]
        blks = [step * SUB + part for part in parts]
        firsts = [(starts_ref[blk] >> 4) << 4 for blk in blks]
        gots = [picked(blk, part, pl.multiple_of(first, 16)) for blk, part, first in zip(blks, parts, firsts)]
        for blk, part, first, got in zip(blks, parts, firsts, gots):
            head = pl.ds(pl.multiple_of(first, 16), 16)
            rows[head, :] = rows[head, :] + got[:16]
            rows[pl.ds(pl.multiple_of(first + 16, 16), WIN - 16), :] = got[16:]

            def more(i, carry, blk=blk, part=part, first=first):
                at = pl.multiple_of(first + i * WIN, 16)
                rows[pl.ds(at, WIN), :] = picked(blk, part, at)
                return carry

            lax.fori_loop(1, (starts_ref[blk + 1] - first + (WIN - 1)) >> 7, more, 0)
        return carry

    lax.fori_loop(0, SUB // GROUP, some_blocks, 0)

    @pl.when(step == pl.num_programs(0) - 1)
    def _():
        copy = lambda i: pltpu.make_async_copy(rows.at[chunk_at(i), :], rows_hbm.at[chunk_at(i), :], sem)
        start_copies(nch_ref, copy)
        wait_copies(nch_ref, copy)


def stream(nch, body, ins, outs):
    specs = [[spec for spec, _ in part] for part in (ins, outs)]
    pltpu.emit_pipeline(body, grid=(nch,), in_specs=specs[0], out_specs=specs[1])(*[ref for _, ref in ins + outs])


def fwd_kernel(scale, nch_ref, tid_ref, h_ref, w1_ref, w2_ref, rows_hbm, attr_hbm, u_hbm, pre_hbm, z_hbm, stat_ref, m8, s8):
    m8[...] = jnp.full_like(m8, -EXCLUDED)
    s8[...] = jnp.zeros_like(s8)
    dim, ff, toks = rows_hbm.shape[1], w1_ref.shape[1], h_ref.shape[0]

    def body(rows_ref, attr_ref, u_ref, pre_ref, z_ref):
        rows = rows_ref[...]
        out = None
        for f in range(0, ff, FB):
            pre = dot(rows, w1_ref[:, f : f + FB])
            pre_ref[:, f : f + FB] = pre
            act = gelu(pre).astype(BF)
            part = dot(act, w2_ref[f : f + FB, :])
            out = part if out is None else out + part
        vec = out.astype(BF)
        u_ref[...] = vec
        loc = column(attr_ref, 0, 0, CH // WIN)
        off = column(attr_ref, 1, 0, CH // WIN)
        for t in range(0, toks, TB):
            raw = dot_nt(vec, h_ref[t : t + TB, :]) * scale
            same = loc == tid_ref[:, t : t + TB]
            z = raw - jnp.where(same, 0.0, off)
            z_ref[:, t : t + TB] = z
            z3 = z.reshape(CH // 8, 8, TB)
            old = m8[:, t : t + TB]
            new = jnp.maximum(old, jnp.max(z3, axis=0))
            s8[:, t : t + TB] = s8[:, t : t + TB] * jnp.exp(old - new) + jnp.sum(jnp.exp(z3 - new[None]), axis=0)
            m8[:, t : t + TB] = new

    stream(nch_ref[0], body, [(chunk(dim), rows_hbm), (ATTR_CHUNK, attr_hbm)],
           [(chunk(dim), u_hbm), (chunk(ff), pre_hbm), (chunk(toks), z_hbm)])
    top = jnp.max(m8[...], axis=0, keepdims=True)
    stat_ref[0:1, :] = top
    stat_ref[1:2, :] = jnp.sum(s8[...] * jnp.exp(m8[...] - top), axis=0, keepdims=True)


def logit_back_kernel(scale, nch_ref, tid_ref, stat_ref, h_ref, z_hbm, u_hbm, attr_hbm, g_hbm, dht_ref):
    dht_ref[...] = jnp.zeros_like(dht_ref)
    dim, toks = u_hbm.shape[1], h_ref.shape[0]

    def body(z_ref, u_ref, attr_ref, g_ref):
        vec_t = u_ref[...].T
        loc = column(attr_ref, 0, 0, CH // WIN)
        grad = None
        for t in range(0, toks, TB):
            z = z_ref[:, t : t + TB]
            same = loc == tid_ref[:, t : t + TB]
            dz = (jnp.exp(z - stat_ref[1:2, t : t + TB]) + jnp.where(same, stat_ref[2:3, t : t + TB], 0.0)).astype(BF)
            part = dot(dz, h_ref[t : t + TB, :])
            grad = part if grad is None else grad + part
            dht_ref[:dim, t : t + TB] += dot(vec_t, dz)
            zt = jnp.where(same, z, 0.0)
            dht_ref[dim:, t : t + TB] += jnp.sum(zt.reshape(CH // 8, 8, TB), axis=0)
        g_ref[...] = (grad * scale).astype(BF)

    stream(nch_ref[0], body, [(chunk(toks), z_hbm), (chunk(dim), u_hbm), (ATTR_CHUNK, attr_hbm)], [(chunk(dim), g_hbm)])


def tower_back_kernel(nch_ref, starts_ref, w1_ref, w2_ref, attr_ref, g_hbm, rows_hbm, pre_hbm, table_hbm, dw_ref, drow, ring, state, ring_sem):
    dw_ref[...] = jnp.zeros_like(dw_ref)
    dim, ff = w1_ref.shape
    n_blk = table_hbm.shape[0] // BLK
    slots = ring.shape[0]
    state[0] = 0
    state[1] = 0

    def clear(i, carry):
        drow[chunk_at(i), :] = jnp.zeros((CH, dim), BF)
        return carry

    lax.fori_loop(0, nch_ref[0] + 1, clear, 0)
    row = lax.broadcasted_iota(jnp.int32, (BLK, WIN), 0).astype(F32)

    def put(blk, tile):
        base = (blk * BLK).astype(F32)
        pick = [jnp.where(attr_ref[tile + k][0:1, :] - base == row, 1.0, 0.0).astype(BF) for k in range(2)]
        return dot(jnp.concatenate(pick, axis=1), drow[pl.ds(pl.multiple_of(tile * WIN, WIN), 2 * WIN), :])

    def write(blk):
        slot = lax.rem(blk, slots)
        return pltpu.make_async_copy(ring.at[slot], table_hbm.at[pl.ds(pl.multiple_of(blk * BLK, BLK), BLK), :], ring_sem.at[slot])

    def build(blk):
        blks = [blk + k for k in range(PAIR)]

        @pl.when(blk >= slots)
        def _():
            for one in blks:
                write(one).wait()

        firsts = [starts_ref[one] >> 7 for one in blks]
        for one, first in zip(blks, firsts):
            ring[lax.rem(one, slots)] = put(one, first)
        for one, first in zip(blks, firsts):
            def more(i, carry, one=one, first=first):
                ring[lax.rem(one, slots)] += put(one, first + 2 * i)
                return carry

            lax.fori_loop(1, (starts_ref[one + 1] - first * WIN + (2 * WIN - 1)) >> 8, more, 0)
            write(one).start()
        return blk + PAIR

    def body(g_ref, rows_ref, pre_ref):
        g = g_ref[...]
        g_t, rows_t = g.T, rows_ref[...].T
        out = None
        for f in range(0, ff, FB):
            act, slope = gelu_pair(pre_ref[:, f : f + FB])
            q = (slope * dot_nt(g, w2_ref[f : f + FB, :])).astype(BF)
            dw_ref[dim:, f : f + FB] += dot(g_t, act.astype(BF))
            dw_ref[:dim, f : f + FB] += dot(rows_t, q)
            part = dot_nt(q, w1_ref[:, f : f + FB])
            out = part if out is None else out + part
        step = state[0]
        drow[chunk_at(step), :] = out.astype(BF)
        done = (step + 1) * CH
        ready = lambda blk: (blk < n_blk) & (starts_ref[jnp.minimum(blk + PAIR, n_blk)] <= done)
        state[1] = lax.while_loop(ready, build, state[1])
        state[0] = step + 1

    stream(nch_ref[0], body, [(chunk(dim), g_hbm), (chunk(dim), rows_hbm), (chunk(ff), pre_hbm)], [])
    for blk in range(n_blk - slots, n_blk):
        write(jnp.int32(blk)).wait()


def query_back_kernel(scale, x_hbm, dht_hbm, w1_hbm, w2_hbm, part_hbm, dw1_hbm, dw2_hbm, dwi1_hbm, dwi2_hbm,
                      dw1_ref, dw2t_ref, sum_ref, flip, x_ref, x_t, dht_ref, grad_t, grad, w1_ref, w2_ref, work, r0, r1, r2,
                      load_sem, store_sem, send_sem, recv_sem):
    me = lax.axis_index("dp")
    core, x, y = lax.rem(me, 2), lax.rem(lax.div(me, 2), 2), lax.div(me, 4)
    pair, x_peer, y_peer = me + 1 - 2 * core, me + 2 - 4 * x, me + 4 - 8 * y
    dim, ff = w1_ref.shape
    toks = x_ref.shape[0]
    half = dim // 2
    p1, p2, p3 = half // 2, half // 4, half // 8

    barrier = pltpu.get_barrier_semaphore()
    for peer in (pair, x_peer, y_peer):
        pl.semaphore_signal(barrier, inc=1, device_id=(peer,), device_id_type=MESH)
    pl.semaphore_wait(barrier, 3)

    def rows(first, count):
        return pl.ds(pl.multiple_of(first, count), count)

    def send(j, k, src, dst, peer):
        sems = send_sem.at[13 * j + k], recv_sem.at[13 * j + k]
        copy = pltpu.make_async_remote_copy(
            src_ref=src, dst_ref=dst, send_sem=sems[0], recv_sem=sems[1], device_id=(peer,), device_id_type=MESH)
        copy.start()
        return copy

    def wait(copies):
        for copy in copies:
            copy.wait()

    def mine(j):
        return j * dim + core * half

    def stage0(j):
        return [send(j, 0, part_hbm.at[rows(j * dim + (1 - core) * half, half), :], r0.at[j], pair)]

    def stage1(j):
        work[j] = work[j] + r0[j]
        return [send(j, 1, work.at[j, rows((1 - x) * p2, p2), :], r1.at[j, 0], x_peer),
                send(j, 2, work.at[j, rows(p1 + (1 - y) * p2, p2), :], r1.at[j, 1], y_peer)]

    def stage2(j):
        for at, k in ((rows(x * p2, p2), 0), (rows(p1 + y * p2, p2), 1)):
            work[j, at, :] = work[j, at, :] + r1[j, k]
        return [send(j, 3, work.at[j, rows(x * p2 + (1 - y) * p3, p3), :], r2.at[j, 0], y_peer),
                send(j, 4, work.at[j, rows(p1 + y * p2 + (1 - x) * p3, p3), :], r2.at[j, 1], x_peer)]

    def share_rows(j, k, first, count, peer):
        at = rows(mine(j) + first, count)
        return send(j, k, sum_ref.at[at, :], sum_ref.at[at, :], peer)

    def stage3(j):
        piece_a, piece_b = x * p2 + y * p3, p1 + y * p2 + x * p3
        for k, piece in ((0, piece_a), (1, piece_b)):
            sum_ref[rows(mine(j) + piece, p3), :] = work[j, rows(piece, p3), :] + r2[j, k]
        return [share_rows(j, 5, piece_a, p3, y_peer), share_rows(j, 6, piece_b, p3, x_peer)]

    def stage4(j):
        step = [share_rows(j, 7, x * p2, p2, x_peer), share_rows(j, 8, p1 + y * p2, p2, y_peer)]
        return step, [share_rows(j, 9, x * p2, p2, pair), share_rows(j, 10, p1 + y * p2, p2, pair)]

    def stage5(j):
        return [share_rows(j, 11, (1 - x) * p2, p2, pair), share_rows(j, 12, p1 + (1 - y) * p2, p2, pair)]

    step = [stage0(0), stage0(1)]
    loads = [(part_hbm.at[rows(mine(j), half), :], work.at[j]) for j in range(2)]
    loads += [(x_hbm, x_ref), (dht_hbm.at[rows(0, dim), :], dht_ref), (w1_hbm, w1_ref), (w2_hbm, w2_ref)]
    loads = [pltpu.make_async_copy(src, dst, load_sem.at[i]) for i, (src, dst) in enumerate(loads)]
    for copy in loads:
        copy.start()
    dw1_ref[...] = jnp.zeros_like(dw1_ref)
    dw2t_ref[...] = jnp.zeros_like(dw2t_ref)
    wait(loads)

    def turn(i, carry):
        tok = pl.ds(pl.multiple_of(i * TCH, TCH), TCH)
        x_t[:, tok] = x_ref[tok, :].T
        block = (dht_ref[:, tok] * scale).astype(BF)
        grad_t[:, tok] = block
        grad[tok, :] = block.T
        return carry

    blocks = ff // FB

    def unit(u, carry):
        tok = pl.ds(pl.multiple_of(lax.div(u, blocks) * TCH, TCH), TCH)
        at = pl.ds(pl.multiple_of(lax.rem(u, blocks) * FB, FB), FB)
        act, slope = gelu_pair(dot(x_ref[tok, :], w1_ref[:, at]))
        q = (slope * dot_nt(grad[tok, :], w2_ref[at, :])).astype(BF)
        dw2t_ref[:, at] += dot(grad_t[:, tok], act.astype(BF))
        dw1_ref[:, at] += dot(x_t[:, tok], q)
        return carry

    units = toks // TCH * blocks
    wait(step[0])
    step[0] = stage1(0)
    wait(step[1])
    step[1] = stage1(1)
    lax.fori_loop(0, toks // TCH, turn, 0)
    lax.fori_loop(0, units // 4, unit, 0)
    wait(step[0])
    step[0] = stage2(0)
    lax.fori_loop(units // 4, units // 2, unit, 0)
    wait(step[1])
    step[1] = stage2(1)
    lax.fori_loop(units // 2, units * 5 // 8, unit, 0)
    wait(step[0])
    step[0] = stage3(0)
    lax.fori_loop(units * 5 // 8, units * 3 // 4, unit, 0)
    wait(step[1])
    step[1] = stage3(1)
    lax.fori_loop(units * 3 // 4, units, unit, 0)
    wait(step[0])
    step[0], last0 = stage4(0)
    wait(step[1])
    step[1], last1 = stage4(1)
    stores = [pltpu.make_async_copy(dw1_ref, dw1_hbm, store_sem.at[0]), pltpu.make_async_copy(flip.at[0], dw2_hbm, store_sem.at[1])]
    stores[0].start()
    for f in range(0, ff, FB):
        flip[0, f : f + FB, :] = dw2t_ref[:, f : f + FB].T
    stores[1].start()
    wait(step[0])
    last0 += stage5(0)
    wait(last0)
    stores += [pltpu.make_async_copy(sum_ref.at[rows(0, dim), :], dwi1_hbm, store_sem.at[2]), pltpu.make_async_copy(flip.at[1], dwi2_hbm, store_sem.at[3])]
    stores[2].start()
    wait(step[1])
    last1 += stage5(1)
    wait(last1)
    for f in range(0, ff, FB):
        flip[1, f : f + FB, :] = sum_ref[dim:, f : f + FB].T
    stores[3].start()
    wait(stores)


def exchange(n, src_ref, all_ref, send_sem, recv_sem):
    me = lax.axis_index("dp")
    barrier = pltpu.get_barrier_semaphore()
    for k in range(1, n):
        pl.semaphore_signal(barrier, inc=1, device_id=(lax.rem(me + k, n),), device_id_type=MESH)
    pl.semaphore_wait(barrier, n - 1)
    copies = []
    for k in range(1, n):
        copies.append(pltpu.make_async_remote_copy(
            src_ref=src_ref, dst_ref=all_ref.at[me], send_sem=send_sem.at[k - 1], recv_sem=recv_sem.at[k - 1],
            device_id=(lax.rem(me + k, n),), device_id_type=MESH))
        copies[-1].start()
    all_ref[me] = src_ref[...]
    return copies


def query_kernel(n, targ_ref, x_hbm, w1_hbm, w2_hbm, all_ref, out_ref, x_ref, w1_ref, w2_ref, load_sem, send_sem, recv_sem):
    loads = [(x_hbm, x_ref), (w1_hbm, w1_ref), (w2_hbm, w2_ref)]
    loads = [pltpu.make_async_copy(src, dst, load_sem.at[i]) for i, (src, dst) in enumerate(loads)]
    for copy in loads:
        copy.start()
    copies = exchange(n, targ_ref, all_ref, send_sem, recv_sem)
    for copy in loads:
        copy.wait()
    out = None
    for f in range(0, w1_ref.shape[1], FB):
        part = dot(gelu(dot(x_ref[...], w1_ref[:, f : f + FB])).astype(BF), w2_ref[f : f + FB, :])
        out = part if out is None else out + part
    out_ref[...] = out.astype(BF)
    for copy in copies:
        copy.wait()


def stats_kernel(n, stat_ref, hit_ref, out_ref, stats, send_sem, recv_sem):
    for copy in exchange(n, stat_ref, stats, send_sem, recv_sem):
        copy.wait()
    toks = stat_ref.shape[1]
    hit = hit_ref[...] > 0.5
    top = jnp.where(hit, HIT_VALUE, -EXCLUDED)
    for i in range(n):
        top = jnp.maximum(top, stats[i, 0:1, :])
    total = jnp.where(hit, jnp.exp(HIT_VALUE - top), 0.0)
    for i in range(n):
        total += stats[i, 1:2, :] * jnp.exp(stats[i, 0:1, :] - top)
    lse = top + jnp.log(total)
    out_ref[0:1, :] = lse
    out_ref[1:2, :] = lse + math.log(toks)
    out_ref[2:3, :] = jnp.where(hit, jnp.exp(HIT_VALUE - (lse + math.log(toks))), 0.0) - 1.0 / toks


def share(kernel, ident, n, ins, out, scratch=()):
    spec = lambda place: pl.BlockSpec(memory_space=pltpu.VMEM if place else pl.ANY)
    return pl.pallas_call(
        functools.partial(kernel, n), out_shape=out, in_specs=[spec(p) for _, p in ins], out_specs=[spec(True) for _ in out],
        scratch_shapes=[*scratch, pltpu.SemaphoreType.DMA((n - 1,)), pltpu.SemaphoreType.DMA((n - 1,))],
        compiler_params=pltpu.CompilerParams(collective_id=ident, has_side_effects=True, vmem_limit_bytes=VMEM_LIMIT),
    )(*[a for a, _ in ins])


def params(**kw):
    return pltpu.CompilerParams(vmem_limit_bytes=VMEM_LIMIT, dimension_semantics=("arbitrary",), **kw)


def cost(flops):
    return pl.CostEstimate(flops=flops, bytes_accessed=64 << 20, transcendentals=0)


def whole(shape):
    return pl.BlockSpec(shape, lambda i, *_: (0,) * len(shape))


def chunk(width):
    return pl.BlockSpec((CH, width), lambda i, *_: (i, 0))


ATTR_CHUNK = pl.BlockSpec((CH // WIN, 8, WIN), lambda i, *_: (i, 0, 0))


def sds(*shape, dtype=F32):
    return jax.ShapeDtypeStruct(shape, dtype)


def solution(mesh):
    num_dev = mesh.shape["dp"]

    def local_step(tokens, w_one, w_two, wi_one, wi_two, table, cand_ids, log_q, targ_loc):
        dim = table.shape[1]
        ff = wi_one.shape[1]
        rows_loc = table.shape[0]
        toks = tokens.shape[0] * num_dev
        cands = cand_ids.shape[0]
        cap = cands + toks
        n_blk = rows_loc // BLK
        scale = SCORE_GAIN / math.sqrt(dim)
        base = lax.axis_index("dp") * rows_loc

        hit = jnp.any(targ_loc[:, None] == cand_ids[None, :], axis=1)
        coded, query_loc = share(
            query_kernel, 0, num_dev, [((2 * targ_loc + hit)[None, :], True), (tokens, False), (w_one, False), (w_two, False)],
            [sds(num_dev, 1, targ_loc.shape[0], dtype=jnp.int32), sds(*tokens.shape, dtype=BF)],
            [pltpu.VMEM(tokens.shape, BF), pltpu.VMEM(w_one.shape, BF), pltpu.VMEM(w_two.shape, BF), pltpu.SemaphoreType.DMA((3,))])
        coded = coded.reshape(toks)
        targ_all, hit_all = coded >> 1, coded & 1
        query = lax.all_gather(query_loc, "dp", axis=0, tiled=True)
        x_all = lax.all_gather(tokens, "dp", axis=0, tiled=True)

        ids = jnp.concatenate([cand_ids, jnp.where(hit_all == 1, -1, targ_all)]) - base
        kind = jnp.concatenate([jnp.zeros((cands,), jnp.int32), jnp.ones((toks,), jnp.int32)])
        key = jnp.where((ids >= 0) & (ids < rows_loc), 2 * ids + kind, 2 * rows_loc)
        offs = jnp.concatenate([log_q, jnp.full((toks,), EXCLUDED, F32)])
        bounds = jnp.arange(n_blk + 1, dtype=jnp.int32) * (2 * BLK)
        starts = jnp.sum((key[None, :] < bounds[:, None]).astype(jnp.int32), axis=1)
        nch = jnp.maximum(lax.div(starts[n_blk] + (CH - 1), CH), 1)
        key_s, offs_s = lax.sort((key, offs), num_keys=1, is_stable=False)
        repeat = jnp.concatenate([jnp.zeros((1,), bool), key_s[1:] == key_s[:-1]])
        used = (key_s < 2 * rows_loc) & ~repeat
        attr = jnp.stack([
            jnp.where(used, (key_s >> 1).astype(F32), NO_ROW),
            jnp.where(used, offs_s, EXCLUDED),
        ])
        attr = jnp.pad(attr, ((0, 6), (0, 0)))
        pad = jnp.broadcast_to(jnp.array([NO_ROW, EXCLUDED, 0, 0, 0, 0, 0, 0], F32)[:, None], (8, CH))
        attr = jnp.concatenate([attr, pad], axis=1).reshape(8, -1, WIN).transpose(1, 0, 2)
        tid = (targ_all - base).astype(F32)[None, :]
        nch1 = nch[None]

        rows = pl.pallas_call(
            gather_kernel,
            grid_spec=pltpu.PrefetchScalarGridSpec(
                num_scalar_prefetch=2, grid=(n_blk // SUB,),
                in_specs=[pl.BlockSpec((SUB * BLK, dim), lambda i, *_: (i, 0)), whole(attr.shape)],
                out_specs=pl.BlockSpec(memory_space=pl.ANY),
                scratch_shapes=[pltpu.VMEM((cap + CH, dim), BF), pltpu.VMEM((cap + CH, WIN), F32), pltpu.SemaphoreType.DMA]),
            out_shape=sds(cap, dim, dtype=BF), compiler_params=params(), cost_estimate=cost(4 * rows_loc * WIN * dim), name="gather",
        )(starts, nch1, table, attr)

        def call(kernel, name, flops, ins, outs, scratch=()):
            spec = lambda place: pl.BlockSpec(memory_space={True: pltpu.VMEM, False: pl.ANY, None: pltpu.SMEM}[place])
            return pl.pallas_call(
                kernel, in_specs=[spec(None)] + [spec(p) for _, p in ins], out_specs=[spec(p) for _, p in outs],
                out_shape=[o for o, _ in outs], scratch_shapes=list(scratch),
                compiler_params=pltpu.CompilerParams(vmem_limit_bytes=VMEM_LIMIT), cost_estimate=cost(flops), name=name,
            )(nch1, *[a for a, _ in ins])

        bf_list, f_list = sds(cap, dim, dtype=BF), sds(cap, ff)
        vec, pre, z, stat = call(
            functools.partial(fwd_kernel, scale), "fwd", 6 * cap * dim * ff // 4,
            [(tid, True), (query, True), (wi_one, True), (wi_two, True), (rows, False), (attr, False)],
            [(bf_list, False), (f_list, False), (sds(cap, toks), False), (sds(2, toks), True)],
            [pltpu.VMEM((8, toks), F32), pltpu.VMEM((8, toks), F32)])

        stat, x_all = lax.optimization_barrier((stat, x_all))
        (stat,) = share(
            stats_kernel, 1, num_dev, [(stat, True), (hit_all.astype(F32)[None, :], True)], [sds(3, toks)],
            [pltpu.VMEM((num_dev, 2, toks), F32)])

        g, dht_part = call(
            functools.partial(logit_back_kernel, scale), "logit_back", 4 * cap * dim * toks // 4,
            [(tid, True), (stat, True), (query, True), (z, False), (vec, False), (attr, False)],
            [(bf_list, False), (sds(dim + 8, toks), True)])

        dht = lax.psum(dht_part, "dp")
        d_table, dwi_part = call(
            tower_back_kernel, "tower_back", 8 * cap * dim * ff // 4,
            [(starts, None), (wi_one, True), (wi_two, True), (attr, True), (g, False), (rows, False), (pre, False)],
            [(sds(rows_loc, dim), False), (sds(2 * dim, ff), True)],
            [pltpu.VMEM((cap + CH, dim), BF), pltpu.VMEM((8, BLK, dim), F32), pltpu.SMEM((2,), jnp.int32), pltpu.SemaphoreType.DMA((8,))])

        loss = (jnp.sum(stat[0]) - jnp.sum(dht[dim:])) / toks
        dht, loss = lax.optimization_barrier((dht, loss))
        any_spec = pl.BlockSpec(memory_space=pl.ANY)
        dw_one, dw_two, dwi_one, dwi_two = pl.pallas_call(
            functools.partial(query_back_kernel, scale),
            in_specs=[any_spec] * 5, out_specs=[any_spec] * 4,
            out_shape=[sds(dim, ff), sds(ff, dim), sds(dim, ff), sds(ff, dim)],
            scratch_shapes=[
                pltpu.VMEM((dim, ff), F32), pltpu.VMEM((dim, ff), F32), pltpu.VMEM((2 * dim, ff), F32), pltpu.VMEM((2, ff, dim), F32),
                pltpu.VMEM((toks, dim), BF), pltpu.VMEM((dim, toks), BF), pltpu.VMEM((dim, toks), F32), pltpu.VMEM((dim, toks), BF),
                pltpu.VMEM((toks, dim), BF), pltpu.VMEM((dim, ff), BF), pltpu.VMEM((ff, dim), BF),
                pltpu.VMEM((2, dim // 2, ff), F32), pltpu.VMEM((2, dim // 2, ff), F32),
                pltpu.VMEM((2, 2, dim // 8, ff), F32), pltpu.VMEM((2, 2, dim // 16, ff), F32),
                pltpu.SemaphoreType.DMA((6,)), pltpu.SemaphoreType.DMA((4,)), pltpu.SemaphoreType.DMA((26,)), pltpu.SemaphoreType.DMA((26,))],
            compiler_params=pltpu.CompilerParams(vmem_limit_bytes=VMEM_LIMIT, collective_id=2, has_side_effects=True),
            cost_estimate=cost(8 * toks * dim * ff), name="query_back",
        )(x_all, dht, w_one, w_two, dwi_part)

        return loss, d_table, dw_one, dw_two, dwi_one, dwi_two

    return jax.shard_map(local_step, mesh=mesh, in_specs=(P("dp", None), P(), P(), P(), P(), P("dp", None), P(), P(), P("dp")), out_specs=(P(), P("dp", None), P(), P(), P(), P()), check_vma=False)
```

```python
import functools
import math
import jax
import jax.numpy as jnp
from jax import lax
from jax.experimental import pallas as pl
from jax.experimental.pallas import tpu as pltpu
from jax.sharding import PartitionSpec as P

SCORE_GAIN = 3.0
HIT_VALUE = -1e9
EXCLUDED = 3e38
NO_ROW = -1e9
CH = 512
BLK = 512
TCH = 512
SUB = 8
PAIR = 2
GROUP = 4
WIN = 128
FB = 256
FWD_FB = 512
TB = 512
GELU_C = math.sqrt(2.0 / math.pi)
BF, F32 = jnp.bfloat16, jnp.float32
MESH = pl.DeviceIdType.MESH
VMEM_LIMIT = 60 * 1024 * 1024


def dot(a, b):
    return lax.dot_general(a, b, (((1,), (0,)), ((), ())), preferred_element_type=F32)


def dot_nt(a, b):
    return lax.dot_general(a, b, (((1,), (1,)), ((), ())), preferred_element_type=F32)


def gelu(x):
    half = 0.5 * x
    return half + half * jnp.tanh(x * (GELU_C + (GELU_C * 0.044715) * (x * x)))


def gelu_pair(x):
    sq = x * x
    th = jnp.tanh(x * (GELU_C + (GELU_C * 0.044715) * sq))
    half = 0.5 * x
    slope = (0.5 + 0.5 * th) + half * (1.0 - th * th) * (GELU_C + (3.0 * 0.044715 * GELU_C) * sq)
    return half + half * th, slope


def column(attr_ref, index, first, count):
    tiles = [attr_ref[first + i].T[:, index : index + 1] for i in range(count)]
    return jnp.concatenate(tiles, axis=0) if count > 1 else tiles[0]


def start_copies(nch_ref, copy):
    def step(i, carry):
        copy(i).start()
        return carry

    lax.fori_loop(0, nch_ref[0], step, 0)


def wait_copies(nch_ref, copy):
    def step(i, carry):
        copy(i).wait()
        return carry

    lax.fori_loop(0, nch_ref[0], step, 0)


def chunk_at(i):
    return pl.ds(pl.multiple_of(i * CH, CH), CH)


def gather_kernel(starts_ref, nch_ref, tbl_ref, attr_ref, rows_hbm, rows, keys, sem):
    step = pl.program_id(0)

    @pl.when(step == 0)
    def _():
        def prepare(i, carry):
            rows[chunk_at(i), :] = jnp.zeros((CH, rows.shape[1]), BF)
            for k in range(CH // WIN):
                at = pl.ds(pl.multiple_of(i * CH + k * WIN, WIN), WIN)
                key = attr_ref[i * (CH // WIN) + k].T[:, 0:1]
                keys[at, :] = jnp.broadcast_to(key, (WIN, WIN))
            return carry

        lax.fori_loop(0, nch_ref[0] + 1, prepare, 0)

    lanes = [(lax.broadcasted_iota(jnp.int32, (1, WIN), 1) + j).astype(F32) for j in range(0, BLK, WIN)]

    def picked(blk, part, at):
        key = keys[pl.ds(at, WIN), :] - (blk * BLK).astype(F32)
        pick = [jnp.where(key == lane, 1.0, 0.0).astype(BF) for lane in lanes]
        return dot(jnp.concatenate(pick, axis=1), tbl_ref[pl.ds(pl.multiple_of(part * BLK, BLK), BLK), :]).astype(BF)

    def some_blocks(i, carry):
        parts = [i * GROUP + k for k in range(GROUP)]
        blks = [step * SUB + part for part in parts]
        firsts = [(starts_ref[blk] >> 4) << 4 for blk in blks]
        gots = [picked(blk, part, pl.multiple_of(first, 16)) for blk, part, first in zip(blks, parts, firsts)]
        for blk, part, first, got in zip(blks, parts, firsts, gots):
            head = pl.ds(pl.multiple_of(first, 16), 16)
            rows[head, :] = rows[head, :] + got[:16]
            rows[pl.ds(pl.multiple_of(first + 16, 16), WIN - 16), :] = got[16:]

            def more(i, carry, blk=blk, part=part, first=first):
                at = pl.multiple_of(first + i * WIN, 16)
                rows[pl.ds(at, WIN), :] = picked(blk, part, at)
                return carry

            lax.fori_loop(1, (starts_ref[blk + 1] - first + (WIN - 1)) >> 7, more, 0)
        return carry

    lax.fori_loop(0, SUB // GROUP, some_blocks, 0)

    @pl.when(step == pl.num_programs(0) - 1)
    def _():
        copy = lambda i: pltpu.make_async_copy(rows.at[chunk_at(i), :], rows_hbm.at[chunk_at(i), :], sem)
        start_copies(nch_ref, copy)
        wait_copies(nch_ref, copy)


def stream(nch, body, ins, outs):
    specs = [[spec for spec, _ in part] for part in (ins, outs)]
    pltpu.emit_pipeline(body, grid=(nch,), in_specs=specs[0], out_specs=specs[1])(*[ref for _, ref in ins + outs])


def fwd_kernel(scale, nch_ref, tid_ref, h_ref, w1_ref, w2_ref, rows_hbm, attr_hbm, u_hbm, pre_hbm, z_hbm, stat_ref, m8, s8):
    m8[...] = jnp.full_like(m8, -EXCLUDED)
    s8[...] = jnp.zeros_like(s8)
    dim, ff, toks = rows_hbm.shape[1], w1_ref.shape[1], h_ref.shape[0]

    def body(rows_ref, attr_ref, u_ref, pre_ref, z_ref):
        rows = rows_ref[...]
        out = None
        for f in range(0, ff, FWD_FB):
            pre = dot(rows, w1_ref[:, f : f + FWD_FB])
            pre_ref[:, f : f + FWD_FB] = pre
            act = gelu(pre).astype(BF)
            part = dot(act, w2_ref[f : f + FWD_FB, :])
            out = part if out is None else out + part
        vec = out.astype(BF)
        u_ref[...] = vec
        loc = column(attr_ref, 0, 0, CH // WIN)
        off = column(attr_ref, 1, 0, CH // WIN)
        for t in range(0, toks, TB):
            raw = dot_nt(vec, h_ref[t : t + TB, :]) * scale
            same = loc == tid_ref[:, t : t + TB]
            z = raw - jnp.where(same, 0.0, off)
            z_ref[:, t : t + TB] = z
            z3 = z.reshape(CH // 8, 8, TB)
            old = m8[:, t : t + TB]
            new = jnp.maximum(old, jnp.max(z3, axis=0))
            s8[:, t : t + TB] = s8[:, t : t + TB] * jnp.exp(old - new) + jnp.sum(jnp.exp(z3 - new[None]), axis=0)
            m8[:, t : t + TB] = new

    stream(nch_ref[0], body, [(chunk(dim), rows_hbm), (ATTR_CHUNK, attr_hbm)],
           [(chunk(dim), u_hbm), (chunk(ff), pre_hbm), (chunk(toks), z_hbm)])
    top = jnp.max(m8[...], axis=0, keepdims=True)
    stat_ref[0:1, :] = top
    stat_ref[1:2, :] = jnp.sum(s8[...] * jnp.exp(m8[...] - top), axis=0, keepdims=True)


def logit_back_kernel(scale, nch_ref, tid_ref, stat_ref, h_ref, z_hbm, u_hbm, attr_hbm, g_hbm, dht_ref):
    dht_ref[...] = jnp.zeros_like(dht_ref)
    dim, toks = u_hbm.shape[1], h_ref.shape[0]

    def body(z_ref, u_ref, attr_ref, g_ref):
        vec_t = u_ref[...].T
        loc = column(attr_ref, 0, 0, CH // WIN)
        grad = None
        for t in range(0, toks, TB):
            z = z_ref[:, t : t + TB]
            same = loc == tid_ref[:, t : t + TB]
            dz = (jnp.exp(z - stat_ref[1:2, t : t + TB]) + jnp.where(same, stat_ref[2:3, t : t + TB], 0.0)).astype(BF)
            part = dot(dz, h_ref[t : t + TB, :])
            grad = part if grad is None else grad + part
            dht_ref[:dim, t : t + TB] += dot(vec_t, dz)
            zt = jnp.where(same, z, 0.0)
            dht_ref[dim:, t : t + TB] += jnp.sum(zt.reshape(CH // 8, 8, TB), axis=0)
        g_ref[...] = (grad * scale).astype(BF)

    stream(nch_ref[0], body, [(chunk(toks), z_hbm), (chunk(dim), u_hbm), (ATTR_CHUNK, attr_hbm)], [(chunk(dim), g_hbm)])


def tower_back_kernel(nch_ref, starts_ref, w1_ref, w2_ref, attr_ref, g_hbm, rows_hbm, pre_hbm, table_hbm, dw_ref, drow, ring, state, ring_sem):
    dw_ref[...] = jnp.zeros_like(dw_ref)
    dim, ff = w1_ref.shape
    n_blk = table_hbm.shape[0] // BLK
    slots = ring.shape[0]
    state[0] = 0
    state[1] = 0

    def clear(i, carry):
        drow[chunk_at(i), :] = jnp.zeros((CH, dim), BF)
        return carry

    lax.fori_loop(0, nch_ref[0] + 1, clear, 0)
    row = lax.broadcasted_iota(jnp.int32, (BLK, WIN), 0).astype(F32)

    def put(blk, tile):
        base = (blk * BLK).astype(F32)
        pick = [jnp.where(attr_ref[tile + k][0:1, :] - base == row, 1.0, 0.0).astype(BF) for k in range(2)]
        return dot(jnp.concatenate(pick, axis=1), drow[pl.ds(pl.multiple_of(tile * WIN, WIN), 2 * WIN), :])

    def write(blk):
        slot = lax.rem(blk, slots)
        return pltpu.make_async_copy(ring.at[slot], table_hbm.at[pl.ds(pl.multiple_of(blk * BLK, BLK), BLK), :], ring_sem.at[slot])

    def build(blk):
        blks = [blk + k for k in range(PAIR)]

        @pl.when(blk >= slots)
        def _():
            for one in blks:
                write(one).wait()

        firsts = [starts_ref[one] >> 7 for one in blks]
        for one, first in zip(blks, firsts):
            ring[lax.rem(one, slots)] = put(one, first)
        for one, first in zip(blks, firsts):
            def more(i, carry, one=one, first=first):
                ring[lax.rem(one, slots)] += put(one, first + 2 * i)
                return carry

            lax.fori_loop(1, (starts_ref[one + 1] - first * WIN + (2 * WIN - 1)) >> 8, more, 0)
            write(one).start()
        return blk + PAIR

    def body(g_ref, rows_ref, pre_ref):
        g = g_ref[...]
        g_t, rows_t = g.T, rows_ref[...].T
        out = None
        for f in range(0, ff, FB):
            act, slope = gelu_pair(pre_ref[:, f : f + FB])
            q = (slope * dot_nt(g, w2_ref[f : f + FB, :])).astype(BF)
            dw_ref[dim:, f : f + FB] += dot(g_t, act.astype(BF))
            dw_ref[:dim, f : f + FB] += dot(rows_t, q)
            part = dot_nt(q, w1_ref[:, f : f + FB])
            out = part if out is None else out + part
        step = state[0]
        drow[chunk_at(step), :] = out.astype(BF)
        done = (step + 1) * CH
        ready = lambda blk: (blk < n_blk) & (starts_ref[jnp.minimum(blk + PAIR, n_blk)] <= done)
        state[1] = lax.while_loop(ready, build, state[1])
        state[0] = step + 1

    stream(nch_ref[0], body, [(chunk(dim), g_hbm), (chunk(dim), rows_hbm), (chunk(ff), pre_hbm)], [])
    for blk in range(n_blk - slots, n_blk):
        write(jnp.int32(blk)).wait()


def query_back_kernel(scale, stat_ref, x_hbm, dht_hbm, w1_hbm, w2_hbm, part_hbm, dw1_hbm, dw2_hbm, dwi1_hbm, dwi2_hbm, loss_ref,
                      zt_ref, dw1_ref, dw2t_ref, sum_ref, flip, x_ref, x_t, dht_ref, grad_t, grad, w1_ref, w2_ref, work, r0, r1, r2,
                      load_sem, store_sem, send_sem, recv_sem):
    me = lax.axis_index("dp")
    core, x, y = lax.rem(me, 2), lax.rem(lax.div(me, 2), 2), lax.div(me, 4)
    pair, x_peer, y_peer = me + 1 - 2 * core, me + 2 - 4 * x, me + 4 - 8 * y
    dim, ff = w1_ref.shape
    toks = x_ref.shape[0]
    half = dim // 2
    p1, p2, p3 = half // 2, half // 4, half // 8

    barrier = pltpu.get_barrier_semaphore()
    for peer in (pair, x_peer, y_peer):
        pl.semaphore_signal(barrier, inc=1, device_id=(peer,), device_id_type=MESH)
    pl.semaphore_wait(barrier, 3)

    def rows(first, count):
        return pl.ds(pl.multiple_of(first, count), count)

    def send(j, k, src, dst, peer):
        sems = send_sem.at[13 * j + k], recv_sem.at[13 * j + k]
        copy = pltpu.make_async_remote_copy(
            src_ref=src, dst_ref=dst, send_sem=sems[0], recv_sem=sems[1], device_id=(peer,), device_id_type=MESH)
        copy.start()
        return copy

    def wait(copies):
        for copy in copies:
            copy.wait()

    def mine(j):
        return j * dim + core * half

    def stage0(j):
        return [send(j, 0, part_hbm.at[rows(j * dim + (1 - core) * half, half), :], r0.at[j], pair)]

    def stage1(j):
        work[j] = work[j] + r0[j]
        return [send(j, 1, work.at[j, rows((1 - x) * p2, p2), :], r1.at[j, 0], x_peer),
                send(j, 2, work.at[j, rows(p1 + (1 - y) * p2, p2), :], r1.at[j, 1], y_peer)]

    def stage2(j):
        for at, k in ((rows(x * p2, p2), 0), (rows(p1 + y * p2, p2), 1)):
            work[j, at, :] = work[j, at, :] + r1[j, k]
        return [send(j, 3, work.at[j, rows(x * p2 + (1 - y) * p3, p3), :], r2.at[j, 0], y_peer),
                send(j, 4, work.at[j, rows(p1 + y * p2 + (1 - x) * p3, p3), :], r2.at[j, 1], x_peer)]

    def share_rows(j, k, first, count, peer):
        at = rows(mine(j) + first, count)
        return send(j, k, sum_ref.at[at, :], sum_ref.at[at, :], peer)

    def stage3(j):
        piece_a, piece_b = x * p2 + y * p3, p1 + y * p2 + x * p3
        for k, piece in ((0, piece_a), (1, piece_b)):
            sum_ref[rows(mine(j) + piece, p3), :] = work[j, rows(piece, p3), :] + r2[j, k]
        return [share_rows(j, 5, piece_a, p3, y_peer), share_rows(j, 6, piece_b, p3, x_peer)]

    def stage4(j):
        step = [share_rows(j, 7, x * p2, p2, x_peer), share_rows(j, 8, p1 + y * p2, p2, y_peer)]
        return step, [share_rows(j, 9, x * p2, p2, pair), share_rows(j, 10, p1 + y * p2, p2, pair)]

    def stage5(j):
        return [share_rows(j, 11, (1 - x) * p2, p2, pair), share_rows(j, 12, p1 + (1 - y) * p2, p2, pair)]

    step = [stage0(0), stage0(1)]
    loads = [(part_hbm.at[rows(mine(j), half), :], work.at[j]) for j in range(2)]
    loads += [(x_hbm, x_ref), (dht_hbm.at[rows(0, dim), :], dht_ref), (w1_hbm, w1_ref), (w2_hbm, w2_ref), (dht_hbm.at[rows(dim, 8), :], zt_ref)]
    loads = [pltpu.make_async_copy(src, dst, load_sem.at[i]) for i, (src, dst) in enumerate(loads)]
    for copy in loads:
        copy.start()
    dw1_ref[...] = jnp.zeros_like(dw1_ref)
    dw2t_ref[...] = jnp.zeros_like(dw2t_ref)
    wait(loads)

    total = jnp.sum(stat_ref[0:1, :], axis=1, keepdims=True) - jnp.sum(jnp.sum(zt_ref[...], axis=0, keepdims=True), axis=1, keepdims=True)
    loss_ref[...] = jnp.broadcast_to(total / toks, loss_ref.shape)

    def turn(i, carry):
        tok = pl.ds(pl.multiple_of(i * TCH, TCH), TCH)
        x_t[:, tok] = x_ref[tok, :].T
        block = (dht_ref[:, tok] * scale).astype(BF)
        grad_t[:, tok] = block
        grad[tok, :] = block.T
        return carry

    blocks = ff // FB

    def unit(u, carry):
        tok = pl.ds(pl.multiple_of(lax.div(u, blocks) * TCH, TCH), TCH)
        at = pl.ds(pl.multiple_of(lax.rem(u, blocks) * FB, FB), FB)
        act, slope = gelu_pair(dot(x_ref[tok, :], w1_ref[:, at]))
        q = (slope * dot_nt(grad[tok, :], w2_ref[at, :])).astype(BF)
        dw2t_ref[:, at] += dot(grad_t[:, tok], act.astype(BF))
        dw1_ref[:, at] += dot(x_t[:, tok], q)
        return carry

    units = toks // TCH * blocks
    wait(step[0])
    step[0] = stage1(0)
    wait(step[1])
    step[1] = stage1(1)
    lax.fori_loop(0, toks // TCH, turn, 0)
    lax.fori_loop(0, units // 4, unit, 0)
    wait(step[0])
    step[0] = stage2(0)
    lax.fori_loop(units // 4, units // 2, unit, 0)
    wait(step[1])
    step[1] = stage2(1)
    lax.fori_loop(units // 2, units * 5 // 8, unit, 0)
    wait(step[0])
    step[0] = stage3(0)
    lax.fori_loop(units * 5 // 8, units * 3 // 4, unit, 0)
    wait(step[1])
    step[1] = stage3(1)
    lax.fori_loop(units * 3 // 4, units, unit, 0)
    wait(step[0])
    step[0], last0 = stage4(0)
    wait(step[1])
    step[1], last1 = stage4(1)
    stores = [pltpu.make_async_copy(dw1_ref, dw1_hbm, store_sem.at[0]), pltpu.make_async_copy(flip.at[0], dw2_hbm, store_sem.at[1])]
    stores[0].start()
    for f in range(0, ff, FB):
        flip[0, f : f + FB, :] = dw2t_ref[:, f : f + FB].T
    stores[1].start()
    wait(step[0])
    last0 += stage5(0)
    wait(last0)
    stores += [pltpu.make_async_copy(sum_ref.at[rows(0, dim), :], dwi1_hbm, store_sem.at[2]), pltpu.make_async_copy(flip.at[1], dwi2_hbm, store_sem.at[3])]
    stores[2].start()
    wait(step[1])
    last1 += stage5(1)
    wait(last1)
    for f in range(0, ff, FB):
        flip[1, f : f + FB, :] = sum_ref[dim:, f : f + FB].T
    stores[3].start()
    wait(stores)


def finish_kernel(a_hbm, b_hbm, c_hbm, d_hbm, a_out, b_out, c_out, d_out, wide, tall, load_sem, store_sem):
    loads, stores = [], []
    for src, buf, dst in ((a_hbm, wide.at[0], a_out), (b_hbm, tall.at[0], b_out), (c_hbm, wide.at[1], c_out), (d_hbm, tall.at[1], d_out)):
        count = src.shape[0] // 4
        for first in range(0, src.shape[0], count):
            at, k = pl.ds(first, count), len(loads)
            loads.append(pltpu.make_async_copy(src.at[at, :], buf.at[at, :], load_sem.at[k]))
            stores.append(pltpu.make_async_copy(buf.at[at, :], dst.at[at, :], store_sem.at[k]))
    for copy in loads:
        copy.start()
    for load, store in zip(loads, stores):
        load.wait()
        store.start()
    for copy in stores:
        copy.wait()


def exchange(n, src_ref, all_ref, send_sem, recv_sem):
    me = lax.axis_index("dp")
    barrier = pltpu.get_barrier_semaphore()
    for k in range(1, n):
        pl.semaphore_signal(barrier, inc=1, device_id=(lax.rem(me + k, n),), device_id_type=MESH)
    pl.semaphore_wait(barrier, n - 1)
    copies = []
    for k in range(1, n):
        copies.append(pltpu.make_async_remote_copy(
            src_ref=src_ref, dst_ref=all_ref.at[me], send_sem=send_sem.at[k - 1], recv_sem=recv_sem.at[k - 1],
            device_id=(lax.rem(me + k, n),), device_id_type=MESH))
        copies[-1].start()
    all_ref[me] = src_ref[...]
    return copies


def query_kernel(n, targ_ref, x_hbm, w1_hbm, w2_hbm, all_ref, out_ref, x_ref, w1_ref, w2_ref, load_sem, send_sem, recv_sem):
    loads = [(x_hbm, x_ref), (w1_hbm, w1_ref), (w2_hbm, w2_ref)]
    loads = [pltpu.make_async_copy(src, dst, load_sem.at[i]) for i, (src, dst) in enumerate(loads)]
    for copy in loads:
        copy.start()
    copies = exchange(n, targ_ref, all_ref, send_sem, recv_sem)
    for copy in loads:
        copy.wait()
    out = None
    for f in range(0, w1_ref.shape[1], FB):
        part = dot(gelu(dot(x_ref[...], w1_ref[:, f : f + FB])).astype(BF), w2_ref[f : f + FB, :])
        out = part if out is None else out + part
    out_ref[...] = out.astype(BF)
    for copy in copies:
        copy.wait()


def stats_kernel(n, stat_ref, hit_ref, out_ref, stats, send_sem, recv_sem):
    for copy in exchange(n, stat_ref, stats, send_sem, recv_sem):
        copy.wait()
    toks = stat_ref.shape[1]
    hit = hit_ref[...] > 0.5
    top = jnp.where(hit, HIT_VALUE, -EXCLUDED)
    for i in range(n):
        top = jnp.maximum(top, stats[i, 0:1, :])
    total = jnp.where(hit, jnp.exp(HIT_VALUE - top), 0.0)
    for i in range(n):
        total += stats[i, 1:2, :] * jnp.exp(stats[i, 0:1, :] - top)
    lse = top + jnp.log(total)
    out_ref[0:1, :] = lse
    out_ref[1:2, :] = lse + math.log(toks)
    out_ref[2:3, :] = jnp.where(hit, jnp.exp(HIT_VALUE - (lse + math.log(toks))), 0.0) - 1.0 / toks


def share(kernel, ident, n, ins, out, scratch=()):
    spec = lambda place: pl.BlockSpec(memory_space=pltpu.VMEM if place else pl.ANY)
    return pl.pallas_call(
        functools.partial(kernel, n), out_shape=out, in_specs=[spec(p) for _, p in ins], out_specs=[spec(True) for _ in out],
        scratch_shapes=[*scratch, pltpu.SemaphoreType.DMA((n - 1,)), pltpu.SemaphoreType.DMA((n - 1,))],
        compiler_params=pltpu.CompilerParams(collective_id=ident, has_side_effects=True, vmem_limit_bytes=VMEM_LIMIT),
    )(*[a for a, _ in ins])


def params(**kw):
    return pltpu.CompilerParams(vmem_limit_bytes=VMEM_LIMIT, dimension_semantics=("arbitrary",), **kw)


def cost(flops):
    return pl.CostEstimate(flops=flops, bytes_accessed=64 << 20, transcendentals=0)


def whole(shape):
    return pl.BlockSpec(shape, lambda i, *_: (0,) * len(shape))


def chunk(width):
    return pl.BlockSpec((CH, width), lambda i, *_: (i, 0))


ATTR_CHUNK = pl.BlockSpec((CH // WIN, 8, WIN), lambda i, *_: (i, 0, 0))


def sds(*shape, dtype=F32):
    return jax.ShapeDtypeStruct(shape, dtype)


def solution(mesh):
    num_dev = mesh.shape["dp"]

    def local_step(tokens, w_one, w_two, wi_one, wi_two, table, cand_ids, log_q, targ_loc):
        dim = table.shape[1]
        ff = wi_one.shape[1]
        rows_loc = table.shape[0]
        toks = tokens.shape[0] * num_dev
        cands = cand_ids.shape[0]
        cap = cands + toks
        n_blk = rows_loc // BLK
        scale = SCORE_GAIN / math.sqrt(dim)
        base = lax.axis_index("dp") * rows_loc

        hit = jnp.any(targ_loc[:, None] == cand_ids[None, :], axis=1)
        coded, query_loc = share(
            query_kernel, 0, num_dev, [((2 * targ_loc + hit)[None, :], True), (tokens, False), (w_one, False), (w_two, False)],
            [sds(num_dev, 1, targ_loc.shape[0], dtype=jnp.int32), sds(*tokens.shape, dtype=BF)],
            [pltpu.VMEM(tokens.shape, BF), pltpu.VMEM(w_one.shape, BF), pltpu.VMEM(w_two.shape, BF), pltpu.SemaphoreType.DMA((3,))])
        coded = coded.reshape(toks)
        targ_all, hit_all = coded >> 1, coded & 1
        query = lax.all_gather(query_loc, "dp", axis=0, tiled=True)
        x_all = lax.all_gather(tokens, "dp", axis=0, tiled=True)

        ids = jnp.concatenate([cand_ids, jnp.where(hit_all == 1, -1, targ_all)]) - base
        kind = jnp.concatenate([jnp.zeros((cands,), jnp.int32), jnp.ones((toks,), jnp.int32)])
        key = jnp.where((ids >= 0) & (ids < rows_loc), 2 * ids + kind, 2 * rows_loc)
        offs = jnp.concatenate([log_q, jnp.full((toks,), EXCLUDED, F32)])
        bounds = jnp.arange(n_blk + 1, dtype=jnp.int32) * (2 * BLK)
        starts = jnp.sum((key[None, :] < bounds[:, None]).astype(jnp.int32), axis=1)
        nch = jnp.maximum(lax.div(starts[n_blk] + (CH - 1), CH), 1)
        key_s, offs_s = lax.sort((key, offs), num_keys=1, is_stable=False)
        repeat = jnp.concatenate([jnp.zeros((1,), bool), key_s[1:] == key_s[:-1]])
        used = (key_s < 2 * rows_loc) & ~repeat
        attr = jnp.stack([
            jnp.where(used, (key_s >> 1).astype(F32), NO_ROW),
            jnp.where(used, offs_s, EXCLUDED),
        ])
        attr = jnp.pad(attr, ((0, 6), (0, 0)))
        pad = jnp.broadcast_to(jnp.array([NO_ROW, EXCLUDED, 0, 0, 0, 0, 0, 0], F32)[:, None], (8, CH))
        attr = jnp.concatenate([attr, pad], axis=1).reshape(8, -1, WIN).transpose(1, 0, 2)
        tid = (targ_all - base).astype(F32)[None, :]
        nch1 = nch[None]

        rows = pl.pallas_call(
            gather_kernel,
            grid_spec=pltpu.PrefetchScalarGridSpec(
                num_scalar_prefetch=2, grid=(n_blk // SUB,),
                in_specs=[pl.BlockSpec((SUB * BLK, dim), lambda i, *_: (i, 0)), whole(attr.shape)],
                out_specs=pl.BlockSpec(memory_space=pl.ANY),
                scratch_shapes=[pltpu.VMEM((cap + CH, dim), BF), pltpu.VMEM((cap + CH, WIN), F32), pltpu.SemaphoreType.DMA]),
            out_shape=sds(cap, dim, dtype=BF), compiler_params=params(), cost_estimate=cost(4 * rows_loc * WIN * dim), name="gather",
        )(starts, nch1, table, attr)

        def call(kernel, name, flops, ins, outs, scratch=()):
            spec = lambda place: pl.BlockSpec(memory_space={True: pltpu.VMEM, False: pl.ANY, None: pltpu.SMEM}[place])
            return pl.pallas_call(
                kernel, in_specs=[spec(None)] + [spec(p) for _, p in ins], out_specs=[spec(p) for _, p in outs],
                out_shape=[o for o, _ in outs], scratch_shapes=list(scratch),
                compiler_params=pltpu.CompilerParams(vmem_limit_bytes=VMEM_LIMIT), cost_estimate=cost(flops), name=name,
            )(nch1, *[a for a, _ in ins])

        bf_list, f_list = sds(cap, dim, dtype=BF), sds(cap, ff)
        vec, pre, z, stat = call(
            functools.partial(fwd_kernel, scale), "fwd", 6 * cap * dim * ff // 4,
            [(tid, True), (query, True), (wi_one, True), (wi_two, True), (rows, False), (attr, False)],
            [(bf_list, False), (f_list, False), (sds(cap, toks), False), (sds(2, toks), True)],
            [pltpu.VMEM((8, toks), F32), pltpu.VMEM((8, toks), F32)])

        stat, x_all = lax.optimization_barrier((stat, x_all))
        (stat,) = share(
            stats_kernel, 1, num_dev, [(stat, True), (hit_all.astype(F32)[None, :], True)], [sds(3, toks)],
            [pltpu.VMEM((num_dev, 2, toks), F32)])

        g, dht_part = call(
            functools.partial(logit_back_kernel, scale), "logit_back", 4 * cap * dim * toks // 4,
            [(tid, True), (stat, True), (query, True), (z, False), (vec, False), (attr, False)],
            [(bf_list, False), (sds(dim + 8, toks), True)])

        dht = lax.psum(dht_part, "dp")
        d_table, dwi_part = call(
            tower_back_kernel, "tower_back", 8 * cap * dim * ff // 4,
            [(starts, None), (wi_one, True), (wi_two, True), (attr, True), (g, False), (rows, False), (pre, False)],
            [(sds(rows_loc, dim), False), (sds(2 * dim, ff), True)],
            [pltpu.VMEM((cap + CH, dim), BF), pltpu.VMEM((8, BLK, dim), F32), pltpu.SMEM((2,), jnp.int32), pltpu.SemaphoreType.DMA((8,))])

        any_spec = pl.BlockSpec(memory_space=pl.ANY)
        *weight_grads, loss = pl.pallas_call(
            functools.partial(query_back_kernel, scale),
            in_specs=[pl.BlockSpec(memory_space=pltpu.VMEM)] + [any_spec] * 5, out_specs=[any_spec] * 4 + [pl.BlockSpec(memory_space=pltpu.VMEM)],
            out_shape=[sds(dim, ff), sds(ff, dim), sds(dim, ff), sds(ff, dim), sds(8, 128)],
            scratch_shapes=[pltpu.VMEM((8, toks), F32),
                pltpu.VMEM((dim, ff), F32), pltpu.VMEM((dim, ff), F32), pltpu.VMEM((2 * dim, ff), F32), pltpu.VMEM((2, ff, dim), F32),
                pltpu.VMEM((toks, dim), BF), pltpu.VMEM((dim, toks), BF), pltpu.VMEM((dim, toks), F32), pltpu.VMEM((dim, toks), BF),
                pltpu.VMEM((toks, dim), BF), pltpu.VMEM((dim, ff), BF), pltpu.VMEM((ff, dim), BF),
                pltpu.VMEM((2, dim // 2, ff), F32), pltpu.VMEM((2, dim // 2, ff), F32),
                pltpu.VMEM((2, 2, dim // 8, ff), F32), pltpu.VMEM((2, 2, dim // 16, ff), F32),
                pltpu.SemaphoreType.DMA((7,)), pltpu.SemaphoreType.DMA((4,)), pltpu.SemaphoreType.DMA((26,)), pltpu.SemaphoreType.DMA((26,))],
            compiler_params=pltpu.CompilerParams(vmem_limit_bytes=VMEM_LIMIT, collective_id=2, has_side_effects=True),
            cost_estimate=cost(8 * toks * dim * ff), name="query_back",
        )(stat, x_all, dht, w_one, w_two, dwi_part)
        weight_grads = pl.pallas_call(
            finish_kernel, in_specs=[any_spec] * 4, out_specs=[any_spec] * 4, out_shape=[sds(*a.shape) for a in weight_grads],
            scratch_shapes=[pltpu.VMEM((2, dim, ff), F32), pltpu.VMEM((2, ff, dim), F32), pltpu.SemaphoreType.DMA((16,)), pltpu.SemaphoreType.DMA((16,))],
            compiler_params=pltpu.CompilerParams(vmem_limit_bytes=VMEM_LIMIT), name="finish",
        )(*weight_grads)

        return (loss[0, 0], d_table, *weight_grads)

    return jax.shard_map(local_step, mesh=mesh, in_specs=(P("dp", None), P(), P(), P(), P(), P("dp", None), P(), P(), P("dp")), out_specs=(P(), P("dp", None), P(), P(), P(), P()), check_vma=False)
```

```python
import functools
import math
import jax
import jax.numpy as jnp
from jax import lax
from jax.experimental import pallas as pl
from jax.experimental.pallas import tpu as pltpu
from jax.sharding import PartitionSpec as P

SCORE_GAIN = 3.0
HIT_VALUE = -1e9
EXCLUDED = 3e38
NO_ROW = -1e9
CH = 512
BLK = 512
TCH = 512
SUB = 8
PAIR = 4
GROUP = 8
RING = 12
WIN = 128
FB = 256
FWD_FB = 512
TB = 512
GELU_C = math.sqrt(2.0 / math.pi)
BF, F32 = jnp.bfloat16, jnp.float32
MESH = pl.DeviceIdType.MESH
VMEM_LIMIT = 60 * 1024 * 1024


def dot(a, b):
    return lax.dot_general(a, b, (((1,), (0,)), ((), ())), preferred_element_type=F32)


def dot_nt(a, b):
    return lax.dot_general(a, b, (((1,), (1,)), ((), ())), preferred_element_type=F32)


def gelu(x):
    half = 0.5 * x
    return half + half * jnp.tanh(x * (GELU_C + (GELU_C * 0.044715) * (x * x)))


def gelu_pair(x):
    sq = x * x
    th = jnp.tanh(x * (GELU_C + (GELU_C * 0.044715) * sq))
    half = 0.5 * x
    slope = (0.5 + 0.5 * th) + half * (1.0 - th * th) * (GELU_C + (3.0 * 0.044715 * GELU_C) * sq)
    return half + half * th, slope


def column(attr_ref, index, first, count):
    tiles = [attr_ref[first + i].T[:, index : index + 1] for i in range(count)]
    return jnp.concatenate(tiles, axis=0) if count > 1 else tiles[0]


def start_copies(nch_ref, copy):
    def step(i, carry):
        copy(i).start()
        return carry

    lax.fori_loop(0, nch_ref[0], step, 0)


def wait_copies(nch_ref, copy):
    def step(i, carry):
        copy(i).wait()
        return carry

    lax.fori_loop(0, nch_ref[0], step, 0)


def chunk_at(i):
    return pl.ds(pl.multiple_of(i * CH, CH), CH)


def gather_kernel(starts_ref, nch_ref, tbl_ref, attr_ref, rows_hbm, rows, keys, sem):
    step = pl.program_id(0)

    @pl.when(step == 0)
    def _():
        def prepare(i, carry):
            rows[chunk_at(i), :] = jnp.zeros((CH, rows.shape[1]), BF)
            for k in range(CH // WIN):
                at = pl.ds(pl.multiple_of(i * CH + k * WIN, WIN), WIN)
                key = attr_ref[i * (CH // WIN) + k].T[:, 0:1]
                keys[at, :] = jnp.broadcast_to(key, (WIN, WIN))
            return carry

        lax.fori_loop(0, nch_ref[0] + 1, prepare, 0)

    lanes = [(lax.broadcasted_iota(jnp.int32, (1, WIN), 1) + j).astype(F32) for j in range(0, BLK, WIN)]

    def picked(blk, part, at):
        key = keys[pl.ds(at, WIN), :] - (blk * BLK).astype(F32)
        pick = [jnp.where(key == lane, 1.0, 0.0).astype(BF) for lane in lanes]
        return dot(jnp.concatenate(pick, axis=1), tbl_ref[pl.ds(pl.multiple_of(part * BLK, BLK), BLK), :]).astype(BF)

    def some_blocks(i, carry):
        parts = [i * GROUP + k for k in range(GROUP)]
        blks = [step * SUB + part for part in parts]
        firsts = [(starts_ref[blk] >> 4) << 4 for blk in blks]
        gots = [picked(blk, part, pl.multiple_of(first, 16)) for blk, part, first in zip(blks, parts, firsts)]
        for blk, part, first, got in zip(blks, parts, firsts, gots):
            head = pl.ds(pl.multiple_of(first, 16), 16)
            rows[head, :] = rows[head, :] + got[:16]
            rows[pl.ds(pl.multiple_of(first + 16, 16), WIN - 16), :] = got[16:]

            def more(i, carry, blk=blk, part=part, first=first):
                at = pl.multiple_of(first + i * WIN, 16)
                rows[pl.ds(at, WIN), :] = picked(blk, part, at)
                return carry

            lax.fori_loop(1, (starts_ref[blk + 1] - first + (WIN - 1)) >> 7, more, 0)
        return carry

    lax.fori_loop(0, SUB // GROUP, some_blocks, 0)

    @pl.when(step == pl.num_programs(0) - 1)
    def _():
        copy = lambda i: pltpu.make_async_copy(rows.at[chunk_at(i), :], rows_hbm.at[chunk_at(i), :], sem)
        start_copies(nch_ref, copy)
        wait_copies(nch_ref, copy)


def stream(nch, body, ins, outs):
    specs = [[spec for spec, _ in part] for part in (ins, outs)]
    pltpu.emit_pipeline(body, grid=(nch,), in_specs=specs[0], out_specs=specs[1])(*[ref for _, ref in ins + outs])


def fwd_kernel(scale, nch_ref, tid_ref, h_ref, w1_ref, w2_ref, rows_hbm, attr_hbm, u_hbm, pre_hbm, z_hbm, stat_ref, m8, s8):
    m8[...] = jnp.full_like(m8, -EXCLUDED)
    s8[...] = jnp.zeros_like(s8)
    dim, ff, toks = rows_hbm.shape[1], w1_ref.shape[1], h_ref.shape[0]

    def body(rows_ref, attr_ref, u_ref, pre_ref, z_ref):
        rows = rows_ref[...]
        out = None
        for f in range(0, ff, FWD_FB):
            pre = dot(rows, w1_ref[:, f : f + FWD_FB])
            pre_ref[:, f : f + FWD_FB] = pre
            act = gelu(pre).astype(BF)
            part = dot(act, w2_ref[f : f + FWD_FB, :])
            out = part if out is None else out + part
        vec = out.astype(BF)
        u_ref[...] = vec
        loc = column(attr_ref, 0, 0, CH // WIN)
        off = column(attr_ref, 1, 0, CH // WIN)
        for t in range(0, toks, TB):
            raw = dot_nt(vec, h_ref[t : t + TB, :]) * scale
            same = loc == tid_ref[:, t : t + TB]
            z = raw - jnp.where(same, 0.0, off)
            z_ref[:, t : t + TB] = z
            z3 = z.reshape(CH // 8, 8, TB)
            old = m8[:, t : t + TB]
            new = jnp.maximum(old, jnp.max(z3, axis=0))
            s8[:, t : t + TB] = s8[:, t : t + TB] * jnp.exp(old - new) + jnp.sum(jnp.exp(z3 - new[None]), axis=0)
            m8[:, t : t + TB] = new

    stream(nch_ref[0], body, [(chunk(dim), rows_hbm), (ATTR_CHUNK, attr_hbm)],
           [(chunk(dim), u_hbm), (chunk(ff), pre_hbm), (chunk(toks), z_hbm)])
    top = jnp.max(m8[...], axis=0, keepdims=True)
    stat_ref[0:1, :] = top
    stat_ref[1:2, :] = jnp.sum(s8[...] * jnp.exp(m8[...] - top), axis=0, keepdims=True)


def logit_back_kernel(scale, nch_ref, tid_ref, stat_ref, h_ref, z_hbm, u_hbm, attr_hbm, g_hbm, dht_ref):
    dht_ref[...] = jnp.zeros_like(dht_ref)
    dim, toks = u_hbm.shape[1], h_ref.shape[0]

    def body(z_ref, u_ref, attr_ref, g_ref):
        vec_t = u_ref[...].T
        loc = column(attr_ref, 0, 0, CH // WIN)
        grad = None
        for t in range(0, toks, TB):
            z = z_ref[:, t : t + TB]
            same = loc == tid_ref[:, t : t + TB]
            dz = (jnp.exp(z - stat_ref[1:2, t : t + TB]) + jnp.where(same, stat_ref[2:3, t : t + TB], 0.0)).astype(BF)
            part = dot(dz, h_ref[t : t + TB, :])
            grad = part if grad is None else grad + part
            dht_ref[:dim, t : t + TB] += dot(vec_t, dz)
            zt = jnp.where(same, z, 0.0)
            dht_ref[dim:, t : t + TB] += jnp.sum(zt.reshape(CH // 8, 8, TB), axis=0)
        g_ref[...] = (grad * scale).astype(BF)

    stream(nch_ref[0], body, [(chunk(toks), z_hbm), (chunk(dim), u_hbm), (ATTR_CHUNK, attr_hbm)], [(chunk(dim), g_hbm)])


def tower_back_kernel(nch_ref, starts_ref, w1_ref, w2_ref, attr_ref, g_hbm, rows_hbm, pre_hbm, table_hbm, dw_ref, drow, ring, state, ring_sem):
    dw_ref[...] = jnp.zeros_like(dw_ref)
    dim, ff = w1_ref.shape
    n_blk = table_hbm.shape[0] // BLK
    slots = ring.shape[0]
    state[0] = 0
    state[1] = 0

    def clear(i, carry):
        drow[chunk_at(i), :] = jnp.zeros((CH, dim), BF)
        return carry

    lax.fori_loop(0, nch_ref[0] + 1, clear, 0)
    row = lax.broadcasted_iota(jnp.int32, (BLK, WIN), 0).astype(F32)

    def put(blk, tile):
        base = (blk * BLK).astype(F32)
        pick = [jnp.where(attr_ref[tile + k][0:1, :] - base == row, 1.0, 0.0).astype(BF) for k in range(2)]
        return dot(jnp.concatenate(pick, axis=1), drow[pl.ds(pl.multiple_of(tile * WIN, WIN), 2 * WIN), :])

    def write(blk):
        slot = lax.rem(blk, slots)
        return pltpu.make_async_copy(ring.at[slot], table_hbm.at[pl.ds(pl.multiple_of(blk * BLK, BLK), BLK), :], ring_sem.at[slot])

    def build(blk):
        blks = [blk + k for k in range(PAIR)]

        @pl.when(blk >= slots)
        def _():
            for one in blks:
                write(one).wait()

        firsts = [starts_ref[one] >> 7 for one in blks]
        for one, first in zip(blks, firsts):
            ring[lax.rem(one, slots)] = put(one, first)
        for one, first in zip(blks, firsts):
            def more(i, carry, one=one, first=first):
                ring[lax.rem(one, slots)] += put(one, first + 2 * i)
                return carry

            lax.fori_loop(1, (starts_ref[one + 1] - first * WIN + (2 * WIN - 1)) >> 8, more, 0)
            write(one).start()
        return blk + PAIR

    def body(g_ref, rows_ref, pre_ref):
        g = g_ref[...]
        g_t, rows_t = g.T, rows_ref[...].T
        out = None
        for f in range(0, ff, FB):
            act, slope = gelu_pair(pre_ref[:, f : f + FB])
            q = (slope * dot_nt(g, w2_ref[f : f + FB, :])).astype(BF)
            dw_ref[dim:, f : f + FB] += dot(g_t, act.astype(BF))
            dw_ref[:dim, f : f + FB] += dot(rows_t, q)
            part = dot_nt(q, w1_ref[:, f : f + FB])
            out = part if out is None else out + part
        step = state[0]
        drow[chunk_at(step), :] = out.astype(BF)
        done = (step + 1) * CH
        ready = lambda blk: (blk < n_blk) & (starts_ref[jnp.minimum(blk + PAIR, n_blk)] <= done)
        state[1] = lax.while_loop(ready, build, state[1])
        state[0] = step + 1

    stream(nch_ref[0], body, [(chunk(dim), g_hbm), (chunk(dim), rows_hbm), (chunk(ff), pre_hbm)], [])
    for blk in range(n_blk - slots, n_blk):
        write(jnp.int32(blk)).wait()


def query_back_kernel(scale, stat_ref, x_hbm, dht_hbm, w1_hbm, w2_hbm, part_hbm, dw1_hbm, dw2_hbm, dwi1_hbm, dwi2_hbm, loss_ref,
                      zt_ref, dw1_ref, dw2t_ref, sum_ref, flip, x_ref, x_t, dht_ref, grad_t, grad, w1_ref, w2_ref, work, r0, r1, r2,
                      load_sem, store_sem, send_sem, recv_sem):
    me = lax.axis_index("dp")
    core, x, y = lax.rem(me, 2), lax.rem(lax.div(me, 2), 2), lax.div(me, 4)
    pair, x_peer, y_peer = me + 1 - 2 * core, me + 2 - 4 * x, me + 4 - 8 * y
    dim, ff = w1_ref.shape
    toks = x_ref.shape[0]
    half = dim // 2
    p1, p2, p3 = half // 2, half // 4, half // 8

    barrier = pltpu.get_barrier_semaphore()
    for peer in (pair, x_peer, y_peer):
        pl.semaphore_signal(barrier, inc=1, device_id=(peer,), device_id_type=MESH)
    pl.semaphore_wait(barrier, 3)

    def rows(first, count):
        return pl.ds(pl.multiple_of(first, count), count)

    def send(j, k, src, dst, peer):
        sems = send_sem.at[13 * j + k], recv_sem.at[13 * j + k]
        copy = pltpu.make_async_remote_copy(
            src_ref=src, dst_ref=dst, send_sem=sems[0], recv_sem=sems[1], device_id=(peer,), device_id_type=MESH)
        copy.start()
        return copy

    def wait(copies):
        for copy in copies:
            copy.wait()

    def mine(j):
        return j * dim + core * half

    def stage0(j):
        return [send(j, 0, part_hbm.at[rows(j * dim + (1 - core) * half, half), :], r0.at[j], pair)]

    def stage1(j):
        work[j] = work[j] + r0[j]
        return [send(j, 1, work.at[j, rows((1 - x) * p2, p2), :], r1.at[j, 0], x_peer),
                send(j, 2, work.at[j, rows(p1 + (1 - y) * p2, p2), :], r1.at[j, 1], y_peer)]

    def stage2(j):
        for at, k in ((rows(x * p2, p2), 0), (rows(p1 + y * p2, p2), 1)):
            work[j, at, :] = work[j, at, :] + r1[j, k]
        return [send(j, 3, work.at[j, rows(x * p2 + (1 - y) * p3, p3), :], r2.at[j, 0], y_peer),
                send(j, 4, work.at[j, rows(p1 + y * p2 + (1 - x) * p3, p3), :], r2.at[j, 1], x_peer)]

    def share_rows(j, k, first, count, peer):
        at = rows(mine(j) + first, count)
        return send(j, k, sum_ref.at[at, :], sum_ref.at[at, :], peer)

    def stage3(j):
        piece_a, piece_b = x * p2 + y * p3, p1 + y * p2 + x * p3
        for k, piece in ((0, piece_a), (1, piece_b)):
            sum_ref[rows(mine(j) + piece, p3), :] = work[j, rows(piece, p3), :] + r2[j, k]
        return [share_rows(j, 5, piece_a, p3, y_peer), share_rows(j, 6, piece_b, p3, x_peer)]

    def stage4(j):
        step = [share_rows(j, 7, x * p2, p2, x_peer), share_rows(j, 8, p1 + y * p2, p2, y_peer)]
        return step, [share_rows(j, 9, x * p2, p2, pair), share_rows(j, 10, p1 + y * p2, p2, pair)]

    def stage5(j):
        return [share_rows(j, 11, (1 - x) * p2, p2, pair), share_rows(j, 12, p1 + (1 - y) * p2, p2, pair)]

    step = [stage0(0), stage0(1)]
    loads = [(part_hbm.at[rows(mine(j), half), :], work.at[j]) for j in range(2)]
    loads += [(x_hbm, x_ref), (dht_hbm.at[rows(0, dim), :], dht_ref), (w1_hbm, w1_ref), (w2_hbm, w2_ref), (dht_hbm.at[rows(dim, 8), :], zt_ref)]
    loads = [pltpu.make_async_copy(src, dst, load_sem.at[i]) for i, (src, dst) in enumerate(loads)]
    for copy in loads:
        copy.start()
    dw1_ref[...] = jnp.zeros_like(dw1_ref)
    dw2t_ref[...] = jnp.zeros_like(dw2t_ref)
    wait(loads)

    total = jnp.sum(stat_ref[0:1, :], axis=1, keepdims=True) - jnp.sum(jnp.sum(zt_ref[...], axis=0, keepdims=True), axis=1, keepdims=True)
    loss_ref[...] = jnp.broadcast_to(total / toks, loss_ref.shape)

    def turn(i, carry):
        tok = pl.ds(pl.multiple_of(i * TCH, TCH), TCH)
        x_t[:, tok] = x_ref[tok, :].T
        block = (dht_ref[:, tok] * scale).astype(BF)
        grad_t[:, tok] = block
        grad[tok, :] = block.T
        return carry

    blocks = ff // FB

    def unit(u, carry):
        tok = pl.ds(pl.multiple_of(lax.div(u, blocks) * TCH, TCH), TCH)
        at = pl.ds(pl.multiple_of(lax.rem(u, blocks) * FB, FB), FB)
        act, slope = gelu_pair(dot(x_ref[tok, :], w1_ref[:, at]))
        q = (slope * dot_nt(grad[tok, :], w2_ref[at, :])).astype(BF)
        dw2t_ref[:, at] += dot(grad_t[:, tok], act.astype(BF))
        dw1_ref[:, at] += dot(x_t[:, tok], q)
        return carry

    units = toks // TCH * blocks
    wait(step[0])
    step[0] = stage1(0)
    wait(step[1])
    step[1] = stage1(1)
    lax.fori_loop(0, toks // TCH, turn, 0)
    lax.fori_loop(0, units // 4, unit, 0)
    wait(step[0])
    step[0] = stage2(0)
    lax.fori_loop(units // 4, units // 2, unit, 0)
    wait(step[1])
    step[1] = stage2(1)
    lax.fori_loop(units // 2, units * 5 // 8, unit, 0)
    wait(step[0])
    step[0] = stage3(0)
    lax.fori_loop(units * 5 // 8, units * 3 // 4, unit, 0)
    wait(step[1])
    step[1] = stage3(1)
    lax.fori_loop(units * 3 // 4, units, unit, 0)
    wait(step[0])
    step[0], last0 = stage4(0)
    wait(step[1])
    step[1], last1 = stage4(1)
    stores = [pltpu.make_async_copy(dw1_ref, dw1_hbm, store_sem.at[0]), pltpu.make_async_copy(flip.at[0], dw2_hbm, store_sem.at[1])]
    stores[0].start()
    for f in range(0, ff, FB):
        flip[0, f : f + FB, :] = dw2t_ref[:, f : f + FB].T
    stores[1].start()
    wait(step[0])
    last0 += stage5(0)
    wait(last0)
    stores += [pltpu.make_async_copy(sum_ref.at[rows(0, dim), :], dwi1_hbm, store_sem.at[2]), pltpu.make_async_copy(flip.at[1], dwi2_hbm, store_sem.at[3])]
    stores[2].start()
    wait(step[1])
    last1 += stage5(1)
    wait(last1)
    for f in range(0, ff, FB):
        flip[1, f : f + FB, :] = sum_ref[dim:, f : f + FB].T
    stores[3].start()
    wait(stores)


def finish_kernel(loss_ref, a_hbm, b_hbm, c_hbm, d_hbm, loss_out, a_out, b_out, c_out, d_out, wide, tall, load_sem, store_sem):
    loads, stores = [], []
    for src, buf, dst in ((a_hbm, wide.at[0], a_out), (b_hbm, tall.at[0], b_out), (c_hbm, wide.at[1], c_out), (d_hbm, tall.at[1], d_out)):
        count = src.shape[0] // 4
        for first in range(0, src.shape[0], count):
            at, k = pl.ds(first, count), len(loads)
            loads.append(pltpu.make_async_copy(src.at[at, :], buf.at[at, :], load_sem.at[k]))
            stores.append(pltpu.make_async_copy(buf.at[at, :], dst.at[at, :], store_sem.at[k]))
    for copy in loads:
        copy.start()
    loss_out[...] = loss_ref[0:1, 0:1]
    for load, store in zip(loads, stores):
        load.wait()
        store.start()
    for copy in stores:
        copy.wait()


def exchange(n, src_ref, all_ref, send_sem, recv_sem):
    me = lax.axis_index("dp")
    barrier = pltpu.get_barrier_semaphore()
    for k in range(1, n):
        pl.semaphore_signal(barrier, inc=1, device_id=(lax.rem(me + k, n),), device_id_type=MESH)
    pl.semaphore_wait(barrier, n - 1)
    copies = []
    for k in range(1, n):
        copies.append(pltpu.make_async_remote_copy(
            src_ref=src_ref, dst_ref=all_ref.at[me], send_sem=send_sem.at[k - 1], recv_sem=recv_sem.at[k - 1],
            device_id=(lax.rem(me + k, n),), device_id_type=MESH))
        copies[-1].start()
    all_ref[me] = src_ref[...]
    return copies


def query_kernel(n, targ_ref, x_hbm, w1_hbm, w2_hbm, all_ref, out_ref, x_ref, w1_ref, w2_ref, load_sem, send_sem, recv_sem):
    loads = [(x_hbm, x_ref), (w1_hbm, w1_ref), (w2_hbm, w2_ref)]
    loads = [pltpu.make_async_copy(src, dst, load_sem.at[i]) for i, (src, dst) in enumerate(loads)]
    for copy in loads:
        copy.start()
    copies = exchange(n, targ_ref, all_ref, send_sem, recv_sem)
    for copy in loads:
        copy.wait()
    out = None
    for f in range(0, w1_ref.shape[1], FB):
        part = dot(gelu(dot(x_ref[...], w1_ref[:, f : f + FB])).astype(BF), w2_ref[f : f + FB, :])
        out = part if out is None else out + part
    out_ref[...] = out.astype(BF)
    for copy in copies:
        copy.wait()


def stats_kernel(n, stat_ref, hit_ref, out_ref, stats, send_sem, recv_sem):
    for copy in exchange(n, stat_ref, stats, send_sem, recv_sem):
        copy.wait()
    toks = stat_ref.shape[1]
    hit = hit_ref[...] > 0.5
    top = jnp.where(hit, HIT_VALUE, -EXCLUDED)
    for i in range(n):
        top = jnp.maximum(top, stats[i, 0:1, :])
    total = jnp.where(hit, jnp.exp(HIT_VALUE - top), 0.0)
    for i in range(n):
        total += stats[i, 1:2, :] * jnp.exp(stats[i, 0:1, :] - top)
    lse = top + jnp.log(total)
    out_ref[0:1, :] = lse
    out_ref[1:2, :] = lse + math.log(toks)
    out_ref[2:3, :] = jnp.where(hit, jnp.exp(HIT_VALUE - (lse + math.log(toks))), 0.0) - 1.0 / toks


def share(kernel, ident, n, ins, out, scratch=()):
    spec = lambda place: pl.BlockSpec(memory_space=pltpu.VMEM if place else pl.ANY)
    return pl.pallas_call(
        functools.partial(kernel, n), out_shape=out, in_specs=[spec(p) for _, p in ins], out_specs=[spec(True) for _ in out],
        scratch_shapes=[*scratch, pltpu.SemaphoreType.DMA((n - 1,)), pltpu.SemaphoreType.DMA((n - 1,))],
        compiler_params=pltpu.CompilerParams(collective_id=ident, has_side_effects=True, vmem_limit_bytes=VMEM_LIMIT),
    )(*[a for a, _ in ins])


def params(**kw):
    return pltpu.CompilerParams(vmem_limit_bytes=VMEM_LIMIT, dimension_semantics=("arbitrary",), **kw)


def cost(flops):
    return pl.CostEstimate(flops=flops, bytes_accessed=64 << 20, transcendentals=0)


def whole(shape):
    return pl.BlockSpec(shape, lambda i, *_: (0,) * len(shape))


def chunk(width):
    return pl.BlockSpec((CH, width), lambda i, *_: (i, 0))


ATTR_CHUNK = pl.BlockSpec((CH // WIN, 8, WIN), lambda i, *_: (i, 0, 0))


def sds(*shape, dtype=F32):
    return jax.ShapeDtypeStruct(shape, dtype)


def solution(mesh):
    num_dev = mesh.shape["dp"]

    def local_step(tokens, w_one, w_two, wi_one, wi_two, table, cand_ids, log_q, targ_loc):
        dim = table.shape[1]
        ff = wi_one.shape[1]
        rows_loc = table.shape[0]
        toks = tokens.shape[0] * num_dev
        cands = cand_ids.shape[0]
        cap = cands + toks
        n_blk = rows_loc // BLK
        scale = SCORE_GAIN / math.sqrt(dim)
        base = lax.axis_index("dp") * rows_loc

        hit = jnp.any(targ_loc[:, None] == cand_ids[None, :], axis=1)
        coded, query_loc = share(
            query_kernel, 0, num_dev, [((2 * targ_loc + hit)[None, :], True), (tokens, False), (w_one, False), (w_two, False)],
            [sds(num_dev, 1, targ_loc.shape[0], dtype=jnp.int32), sds(*tokens.shape, dtype=BF)],
            [pltpu.VMEM(tokens.shape, BF), pltpu.VMEM(w_one.shape, BF), pltpu.VMEM(w_two.shape, BF), pltpu.SemaphoreType.DMA((3,))])
        coded = coded.reshape(toks)
        targ_all, hit_all = coded >> 1, coded & 1
        query = lax.all_gather(query_loc, "dp", axis=0, tiled=True)
        x_all = lax.all_gather(tokens, "dp", axis=0, tiled=True)

        ids = jnp.concatenate([cand_ids, jnp.where(hit_all == 1, -1, targ_all)]) - base
        kind = jnp.concatenate([jnp.zeros((cands,), jnp.int32), jnp.ones((toks,), jnp.int32)])
        key = jnp.where((ids >= 0) & (ids < rows_loc), 2 * ids + kind, 2 * rows_loc)
        offs = jnp.concatenate([log_q, jnp.full((toks,), EXCLUDED, F32)])
        bounds = jnp.arange(n_blk + 1, dtype=jnp.int32) * (2 * BLK)
        starts = jnp.sum((key[None, :] < bounds[:, None]).astype(jnp.int32), axis=1)
        nch = jnp.maximum(lax.div(starts[n_blk] + (CH - 1), CH), 1)
        key_s, offs_s = lax.sort((key, offs), num_keys=1, is_stable=False)
        repeat = jnp.concatenate([jnp.zeros((1,), bool), key_s[1:] == key_s[:-1]])
        used = (key_s < 2 * rows_loc) & ~repeat
        attr = jnp.stack([
            jnp.where(used, (key_s >> 1).astype(F32), NO_ROW),
            jnp.where(used, offs_s, EXCLUDED),
        ])
        attr = jnp.pad(attr, ((0, 6), (0, 0)))
        pad = jnp.broadcast_to(jnp.array([NO_ROW, EXCLUDED, 0, 0, 0, 0, 0, 0], F32)[:, None], (8, CH))
        attr = jnp.concatenate([attr, pad], axis=1).reshape(8, -1, WIN).transpose(1, 0, 2)
        tid = (targ_all - base).astype(F32)[None, :]
        nch1 = nch[None]

        rows = pl.pallas_call(
            gather_kernel,
            grid_spec=pltpu.PrefetchScalarGridSpec(
                num_scalar_prefetch=2, grid=(n_blk // SUB,),
                in_specs=[pl.BlockSpec((SUB * BLK, dim), lambda i, *_: (i, 0)), whole(attr.shape)],
                out_specs=pl.BlockSpec(memory_space=pl.ANY),
                scratch_shapes=[pltpu.VMEM((cap + CH, dim), BF), pltpu.VMEM((cap + CH, WIN), F32), pltpu.SemaphoreType.DMA]),
            out_shape=sds(cap, dim, dtype=BF), compiler_params=params(), cost_estimate=cost(4 * rows_loc * WIN * dim), name="gather",
        )(starts, nch1, table, attr)

        def call(kernel, name, flops, ins, outs, scratch=()):
            spec = lambda place: pl.BlockSpec(memory_space={True: pltpu.VMEM, False: pl.ANY, None: pltpu.SMEM}[place])
            return pl.pallas_call(
                kernel, in_specs=[spec(None)] + [spec(p) for _, p in ins], out_specs=[spec(p) for _, p in outs],
                out_shape=[o for o, _ in outs], scratch_shapes=list(scratch),
                compiler_params=pltpu.CompilerParams(vmem_limit_bytes=VMEM_LIMIT), cost_estimate=cost(flops), name=name,
            )(nch1, *[a for a, _ in ins])

        bf_list, f_list = sds(cap, dim, dtype=BF), sds(cap, ff)
        vec, pre, z, stat = call(
            functools.partial(fwd_kernel, scale), "fwd", 6 * cap * dim * ff // 4,
            [(tid, True), (query, True), (wi_one, True), (wi_two, True), (rows, False), (attr, False)],
            [(bf_list, False), (f_list, False), (sds(cap, toks), False), (sds(2, toks), True)],
            [pltpu.VMEM((8, toks), F32), pltpu.VMEM((8, toks), F32)])

        stat, x_all = lax.optimization_barrier((stat, x_all))
        (stat,) = share(
            stats_kernel, 1, num_dev, [(stat, True), (hit_all.astype(F32)[None, :], True)], [sds(3, toks)],
            [pltpu.VMEM((num_dev, 2, toks), F32)])

        g, dht_part = call(
            functools.partial(logit_back_kernel, scale), "logit_back", 4 * cap * dim * toks // 4,
            [(tid, True), (stat, True), (query, True), (z, False), (vec, False), (attr, False)],
            [(bf_list, False), (sds(dim + 8, toks), True)])

        dht = lax.psum(dht_part, "dp")
        d_table, dwi_part = call(
            tower_back_kernel, "tower_back", 8 * cap * dim * ff // 4,
            [(starts, None), (wi_one, True), (wi_two, True), (attr, True), (g, False), (rows, False), (pre, False)],
            [(sds(rows_loc, dim), False), (sds(2 * dim, ff), True)],
            [pltpu.VMEM((cap + CH, dim), BF), pltpu.VMEM((RING, BLK, dim), F32), pltpu.SMEM((2,), jnp.int32), pltpu.SemaphoreType.DMA((RING,))])

        any_spec = pl.BlockSpec(memory_space=pl.ANY)
        *weight_grads, loss = pl.pallas_call(
            functools.partial(query_back_kernel, scale),
            in_specs=[pl.BlockSpec(memory_space=pltpu.VMEM)] + [any_spec] * 5, out_specs=[any_spec] * 4 + [pl.BlockSpec(memory_space=pltpu.VMEM)],
            out_shape=[sds(dim, ff), sds(ff, dim), sds(dim, ff), sds(ff, dim), sds(8, 128)],
            scratch_shapes=[pltpu.VMEM((8, toks), F32),
                pltpu.VMEM((dim, ff), F32), pltpu.VMEM((dim, ff), F32), pltpu.VMEM((2 * dim, ff), F32), pltpu.VMEM((2, ff, dim), F32),
                pltpu.VMEM((toks, dim), BF), pltpu.VMEM((dim, toks), BF), pltpu.VMEM((dim, toks), F32), pltpu.VMEM((dim, toks), BF),
                pltpu.VMEM((toks, dim), BF), pltpu.VMEM((dim, ff), BF), pltpu.VMEM((ff, dim), BF),
                pltpu.VMEM((2, dim // 2, ff), F32), pltpu.VMEM((2, dim // 2, ff), F32),
                pltpu.VMEM((2, 2, dim // 8, ff), F32), pltpu.VMEM((2, 2, dim // 16, ff), F32),
                pltpu.SemaphoreType.DMA((7,)), pltpu.SemaphoreType.DMA((4,)), pltpu.SemaphoreType.DMA((26,)), pltpu.SemaphoreType.DMA((26,))],
            compiler_params=pltpu.CompilerParams(vmem_limit_bytes=VMEM_LIMIT, collective_id=2, has_side_effects=True),
            cost_estimate=cost(8 * toks * dim * ff), name="query_back",
        )(stat, x_all, dht, w_one, w_two, dwi_part)
        vmem_spec = pl.BlockSpec(memory_space=pltpu.VMEM)
        loss, *weight_grads = pl.pallas_call(
            finish_kernel, in_specs=[vmem_spec] + [any_spec] * 4, out_specs=[vmem_spec] + [any_spec] * 4,
            out_shape=[sds(1, 1)] + [sds(*a.shape) for a in weight_grads],
            scratch_shapes=[pltpu.VMEM((2, dim, ff), F32), pltpu.VMEM((2, ff, dim), F32), pltpu.SemaphoreType.DMA((16,)), pltpu.SemaphoreType.DMA((16,))],
            compiler_params=pltpu.CompilerParams(vmem_limit_bytes=VMEM_LIMIT), name="finish",
        )(loss, *weight_grads)

        return (loss.reshape(()), d_table, *weight_grads)

    return jax.shard_map(local_step, mesh=mesh, in_specs=(P("dp", None), P(), P(), P(), P(), P("dp", None), P(), P(), P("dp")), out_specs=(P(), P("dp", None), P(), P(), P(), P()), check_vma=False)
```

```python
import functools
import math
import jax
import jax.numpy as jnp
from jax import lax
from jax.experimental import pallas as pl
from jax.experimental.pallas import tpu as pltpu
from jax.sharding import PartitionSpec as P

SCORE_GAIN = 3.0
HIT_VALUE = -1e9
EXCLUDED = 3e38
NO_ROW = -1e9
CH = 512
BLK = 512
TCH = 512
SUB = 8
PAIR = 4
GROUP = 4
RING = 12
WIN = 128
FB = 256
FWD_FB = 512
TB = 512
GELU_C = math.sqrt(2.0 / math.pi)
BF, F32 = jnp.bfloat16, jnp.float32
MESH = pl.DeviceIdType.MESH
VMEM_LIMIT = 60 * 1024 * 1024


def dot(a, b):
    return lax.dot_general(a, b, (((1,), (0,)), ((), ())), preferred_element_type=F32)


def dot_nt(a, b):
    return lax.dot_general(a, b, (((1,), (1,)), ((), ())), preferred_element_type=F32)


def gelu(x):
    half = 0.5 * x
    return half + half * jnp.tanh(x * (GELU_C + (GELU_C * 0.044715) * (x * x)))


def gelu_pair(x):
    sq = x * x
    th = jnp.tanh(x * (GELU_C + (GELU_C * 0.044715) * sq))
    half = 0.5 * x
    slope = (0.5 + 0.5 * th) + half * (1.0 - th * th) * (GELU_C + (3.0 * 0.044715 * GELU_C) * sq)
    return half + half * th, slope


def column(attr_ref, index, first, count):
    tiles = [attr_ref[first + i].T[:, index : index + 1] for i in range(count)]
    return jnp.concatenate(tiles, axis=0) if count > 1 else tiles[0]


def start_copies(nch_ref, copy):
    def step(i, carry):
        copy(i).start()
        return carry

    lax.fori_loop(0, nch_ref[0], step, 0)


def wait_copies(nch_ref, copy):
    def step(i, carry):
        copy(i).wait()
        return carry

    lax.fori_loop(0, nch_ref[0], step, 0)


def chunk_at(i):
    return pl.ds(pl.multiple_of(i * CH, CH), CH)


def gather_kernel(starts_ref, nch_ref, tbl_ref, attr_ref, rows_hbm, rows, keys, sem):
    step = pl.program_id(0)

    @pl.when(step == 0)
    def _():
        def prepare(i, carry):
            rows[chunk_at(i), :] = jnp.zeros((CH, rows.shape[1]), BF)
            for k in range(CH // WIN):
                at = pl.ds(pl.multiple_of(i * CH + k * WIN, WIN), WIN)
                key = attr_ref[i * (CH // WIN) + k].T[:, 0:1]
                keys[at, :] = jnp.broadcast_to(key, (WIN, WIN))
            return carry

        lax.fori_loop(0, nch_ref[0] + 1, prepare, 0)

    lanes = [(lax.broadcasted_iota(jnp.int32, (1, WIN), 1) + j).astype(F32) for j in range(0, BLK, WIN)]

    def picked(blk, part, at):
        key = keys[pl.ds(at, WIN), :] - (blk * BLK).astype(F32)
        pick = [jnp.where(key == lane, 1.0, 0.0).astype(BF) for lane in lanes]
        return dot(jnp.concatenate(pick, axis=1), tbl_ref[pl.ds(pl.multiple_of(part * BLK, BLK), BLK), :]).astype(BF)

    def some_blocks(i, carry):
        parts = [i * GROUP + k for k in range(GROUP)]
        blks = [step * SUB + part for part in parts]
        firsts = [(starts_ref[blk] >> 4) << 4 for blk in blks]
        gots = [picked(blk, part, pl.multiple_of(first, 16)) for blk, part, first in zip(blks, parts, firsts)]
        for blk, part, first, got in zip(blks, parts, firsts, gots):
            head = pl.ds(pl.multiple_of(first, 16), 16)
            rows[head, :] = rows[head, :] + got[:16]
            rows[pl.ds(pl.multiple_of(first + 16, 16), WIN - 16), :] = got[16:]

            def more(i, carry, blk=blk, part=part, first=first):
                at = pl.multiple_of(first + i * WIN, 16)
                rows[pl.ds(at, WIN), :] = picked(blk, part, at)
                return carry

            lax.fori_loop(1, (starts_ref[blk + 1] - first + (WIN - 1)) >> 7, more, 0)
        return carry

    lax.fori_loop(0, SUB // GROUP, some_blocks, 0)

    @pl.when(step == pl.num_programs(0) - 1)
    def _():
        copy = lambda i: pltpu.make_async_copy(rows.at[chunk_at(i), :], rows_hbm.at[chunk_at(i), :], sem)
        start_copies(nch_ref, copy)
        wait_copies(nch_ref, copy)


def stream(nch, body, ins, outs):
    specs = [[spec for spec, _ in part] for part in (ins, outs)]
    pltpu.emit_pipeline(body, grid=(nch,), in_specs=specs[0], out_specs=specs[1])(*[ref for _, ref in ins + outs])


def fwd_kernel(scale, nch_ref, tid_ref, h_ref, w1_ref, w2_ref, rows_hbm, attr_hbm, u_hbm, pre_hbm, z_hbm, stat_ref, m8, s8):
    m8[...] = jnp.full_like(m8, -EXCLUDED)
    s8[...] = jnp.zeros_like(s8)
    dim, ff, toks = rows_hbm.shape[1], w1_ref.shape[1], h_ref.shape[0]

    def body(rows_ref, attr_ref, u_ref, pre_ref, z_ref):
        rows = rows_ref[...]
        out = None
        for f in range(0, ff, FWD_FB):
            pre = dot(rows, w1_ref[:, f : f + FWD_FB])
            pre_ref[:, f : f + FWD_FB] = pre
            act = gelu(pre).astype(BF)
            part = dot(act, w2_ref[f : f + FWD_FB, :])
            out = part if out is None else out + part
        vec = out.astype(BF)
        u_ref[...] = vec
        loc = column(attr_ref, 0, 0, CH // WIN)
        off = column(attr_ref, 1, 0, CH // WIN)
        for t in range(0, toks, TB):
            raw = dot_nt(vec, h_ref[t : t + TB, :]) * scale
            same = loc == tid_ref[:, t : t + TB]
            z = raw - jnp.where(same, 0.0, off)
            z_ref[:, t : t + TB] = z
            z3 = z.reshape(CH // 8, 8, TB)
            old = m8[:, t : t + TB]
            new = jnp.maximum(old, jnp.max(z3, axis=0))
            s8[:, t : t + TB] = s8[:, t : t + TB] * jnp.exp(old - new) + jnp.sum(jnp.exp(z3 - new[None]), axis=0)
            m8[:, t : t + TB] = new

    stream(nch_ref[0], body, [(chunk(dim), rows_hbm), (ATTR_CHUNK, attr_hbm)],
           [(chunk(dim), u_hbm), (chunk(ff), pre_hbm), (chunk(toks), z_hbm)])
    top = jnp.max(m8[...], axis=0, keepdims=True)
    stat_ref[0:1, :] = top
    stat_ref[1:2, :] = jnp.sum(s8[...] * jnp.exp(m8[...] - top), axis=0, keepdims=True)


def logit_back_kernel(scale, nch_ref, tid_ref, stat_ref, h_ref, z_hbm, u_hbm, attr_hbm, g_hbm, dht_ref):
    dht_ref[...] = jnp.zeros_like(dht_ref)
    dim, toks = u_hbm.shape[1], h_ref.shape[0]

    def body(z_ref, u_ref, attr_ref, g_ref):
        vec_t = u_ref[...].T
        loc = column(attr_ref, 0, 0, CH // WIN)
        grad = None
        for t in range(0, toks, TB):
            z = z_ref[:, t : t + TB]
            same = loc == tid_ref[:, t : t + TB]
            dz = (jnp.exp(z - stat_ref[1:2, t : t + TB]) + jnp.where(same, stat_ref[2:3, t : t + TB], 0.0)).astype(BF)
            part = dot(dz, h_ref[t : t + TB, :])
            grad = part if grad is None else grad + part
            dht_ref[:dim, t : t + TB] += dot(vec_t, dz)
            zt = jnp.where(same, z, 0.0)
            dht_ref[dim:, t : t + TB] += jnp.sum(zt.reshape(CH // 8, 8, TB), axis=0)
        g_ref[...] = (grad * scale).astype(BF)

    stream(nch_ref[0], body, [(chunk(toks), z_hbm), (chunk(dim), u_hbm), (ATTR_CHUNK, attr_hbm)], [(chunk(dim), g_hbm)])


def tower_back_kernel(nch_ref, starts_ref, w1_ref, w2_ref, attr_ref, g_hbm, rows_hbm, pre_hbm, table_hbm, dw_ref, drow, ring, state, ring_sem):
    dw_ref[...] = jnp.zeros_like(dw_ref)
    dim, ff = w1_ref.shape
    n_blk = table_hbm.shape[0] // BLK
    slots = ring.shape[0]
    state[0] = 0
    state[1] = 0

    def clear(i, carry):
        drow[chunk_at(i), :] = jnp.zeros((CH, dim), BF)
        return carry

    lax.fori_loop(0, nch_ref[0] + 1, clear, 0)
    row = lax.broadcasted_iota(jnp.int32, (BLK, WIN), 0).astype(F32)

    def put(blk, tile):
        base = (blk * BLK).astype(F32)
        pick = [jnp.where(attr_ref[tile + k][0:1, :] - base == row, 1.0, 0.0).astype(BF) for k in range(2)]
        return dot(jnp.concatenate(pick, axis=1), drow[pl.ds(pl.multiple_of(tile * WIN, WIN), 2 * WIN), :])

    def write(blk):
        slot = lax.rem(blk, slots)
        return pltpu.make_async_copy(ring.at[slot], table_hbm.at[pl.ds(pl.multiple_of(blk * BLK, BLK), BLK), :], ring_sem.at[slot])

    def build(blk):
        blks = [blk + k for k in range(PAIR)]

        @pl.when(blk >= slots)
        def _():
            for one in blks:
                write(one).wait()

        firsts = [starts_ref[one] >> 7 for one in blks]
        for one, first in zip(blks, firsts):
            ring[lax.rem(one, slots)] = put(one, first)
        for one, first in zip(blks, firsts):
            def more(i, carry, one=one, first=first):
                ring[lax.rem(one, slots)] += put(one, first + 2 * i)
                return carry

            lax.fori_loop(1, (starts_ref[one + 1] - first * WIN + (2 * WIN - 1)) >> 8, more, 0)
            write(one).start()
        return blk + PAIR

    def body(g_ref, rows_ref, pre_ref):
        g = g_ref[...]
        g_t, rows_t = g.T, rows_ref[...].T
        out = None
        for f in range(0, ff, FB):
            act, slope = gelu_pair(pre_ref[:, f : f + FB])
            q = (slope * dot_nt(g, w2_ref[f : f + FB, :])).astype(BF)
            dw_ref[dim:, f : f + FB] += dot(g_t, act.astype(BF))
            dw_ref[:dim, f : f + FB] += dot(rows_t, q)
            part = dot_nt(q, w1_ref[:, f : f + FB])
            out = part if out is None else out + part
        step = state[0]
        drow[chunk_at(step), :] = out.astype(BF)
        done = (step + 1) * CH
        ready = lambda blk: (blk < n_blk) & (starts_ref[jnp.minimum(blk + PAIR, n_blk)] <= done)
        state[1] = lax.while_loop(ready, build, state[1])
        state[0] = step + 1

    stream(nch_ref[0], body, [(chunk(dim), g_hbm), (chunk(dim), rows_hbm), (chunk(ff), pre_hbm)], [])
    for blk in range(n_blk - slots, n_blk):
        write(jnp.int32(blk)).wait()


def query_back_kernel(scale, stat_ref, x_hbm, dht_hbm, w1_hbm, w2_hbm, part_hbm, dw1_hbm, dw2_hbm, dwi1_hbm, dwi2_hbm, loss_ref,
                      zt_ref, dw1_ref, dw2t_ref, sum_ref, flip, x_ref, x_t, dht_ref, grad_t, grad, w1_ref, w2_ref, work, r0, r1, r2,
                      load_sem, store_sem, send_sem, recv_sem):
    me = lax.axis_index("dp")
    core, x, y = lax.rem(me, 2), lax.rem(lax.div(me, 2), 2), lax.div(me, 4)
    pair, x_peer, y_peer = me + 1 - 2 * core, me + 2 - 4 * x, me + 4 - 8 * y
    dim, ff = w1_ref.shape
    toks = x_ref.shape[0]
    half = dim // 2
    p1, p2, p3 = half // 2, half // 4, half // 8

    barrier = pltpu.get_barrier_semaphore()
    for peer in (pair, x_peer, y_peer):
        pl.semaphore_signal(barrier, inc=1, device_id=(peer,), device_id_type=MESH)
    pl.semaphore_wait(barrier, 3)

    def rows(first, count):
        return pl.ds(pl.multiple_of(first, count), count)

    def send(j, k, src, dst, peer):
        sems = send_sem.at[13 * j + k], recv_sem.at[13 * j + k]
        copy = pltpu.make_async_remote_copy(
            src_ref=src, dst_ref=dst, send_sem=sems[0], recv_sem=sems[1], device_id=(peer,), device_id_type=MESH)
        copy.start()
        return copy

    def wait(copies):
        for copy in copies:
            copy.wait()

    def mine(j):
        return j * dim + core * half

    def stage0(j):
        return [send(j, 0, part_hbm.at[rows(j * dim + (1 - core) * half, half), :], r0.at[j], pair)]

    def stage1(j):
        work[j] = work[j] + r0[j]
        return [send(j, 1, work.at[j, rows((1 - x) * p2, p2), :], r1.at[j, 0], x_peer),
                send(j, 2, work.at[j, rows(p1 + (1 - y) * p2, p2), :], r1.at[j, 1], y_peer)]

    def stage2(j):
        for at, k in ((rows(x * p2, p2), 0), (rows(p1 + y * p2, p2), 1)):
            work[j, at, :] = work[j, at, :] + r1[j, k]
        return [send(j, 3, work.at[j, rows(x * p2 + (1 - y) * p3, p3), :], r2.at[j, 0], y_peer),
                send(j, 4, work.at[j, rows(p1 + y * p2 + (1 - x) * p3, p3), :], r2.at[j, 1], x_peer)]

    def share_rows(j, k, first, count, peer):
        at = rows(mine(j) + first, count)
        return send(j, k, sum_ref.at[at, :], sum_ref.at[at, :], peer)

    def stage3(j):
        piece_a, piece_b = x * p2 + y * p3, p1 + y * p2 + x * p3
        for k, piece in ((0, piece_a), (1, piece_b)):
            sum_ref[rows(mine(j) + piece, p3), :] = work[j, rows(piece, p3), :] + r2[j, k]
        return [share_rows(j, 5, piece_a, p3, y_peer), share_rows(j, 6, piece_b, p3, x_peer)]

    def stage4(j):
        step = [share_rows(j, 7, x * p2, p2, x_peer), share_rows(j, 8, p1 + y * p2, p2, y_peer)]
        return step, [share_rows(j, 9, x * p2, p2, pair), share_rows(j, 10, p1 + y * p2, p2, pair)]

    def stage5(j):
        return [share_rows(j, 11, (1 - x) * p2, p2, pair), share_rows(j, 12, p1 + (1 - y) * p2, p2, pair)]

    step = [stage0(0), stage0(1)]
    loads = [(part_hbm.at[rows(mine(j), half), :], work.at[j]) for j in range(2)]
    loads += [(x_hbm, x_ref), (dht_hbm.at[rows(0, dim), :], dht_ref), (w1_hbm, w1_ref), (w2_hbm, w2_ref), (dht_hbm.at[rows(dim, 8), :], zt_ref)]
    loads = [pltpu.make_async_copy(src, dst, load_sem.at[i]) for i, (src, dst) in enumerate(loads)]
    for copy in loads:
        copy.start()
    dw1_ref[...] = jnp.zeros_like(dw1_ref)
    dw2t_ref[...] = jnp.zeros_like(dw2t_ref)
    wait(loads)

    total = jnp.sum(stat_ref[0:1, :], axis=1, keepdims=True) - jnp.sum(jnp.sum(zt_ref[...], axis=0, keepdims=True), axis=1, keepdims=True)
    loss_ref[...] = jnp.broadcast_to(total / toks, loss_ref.shape)

    def turn(i, carry):
        tok = pl.ds(pl.multiple_of(i * TCH, TCH), TCH)
        x_t[:, tok] = x_ref[tok, :].T
        block = (dht_ref[:, tok] * scale).astype(BF)
        grad_t[:, tok] = block
        grad[tok, :] = block.T
        return carry

    blocks = ff // FB

    def unit(u, carry):
        tok = pl.ds(pl.multiple_of(lax.div(u, blocks) * TCH, TCH), TCH)
        at = pl.ds(pl.multiple_of(lax.rem(u, blocks) * FB, FB), FB)
        act, slope = gelu_pair(dot(x_ref[tok, :], w1_ref[:, at]))
        q = (slope * dot_nt(grad[tok, :], w2_ref[at, :])).astype(BF)
        dw2t_ref[:, at] += dot(grad_t[:, tok], act.astype(BF))
        dw1_ref[:, at] += dot(x_t[:, tok], q)
        return carry

    units = toks // TCH * blocks
    wait(step[0])
    step[0] = stage1(0)
    wait(step[1])
    step[1] = stage1(1)
    lax.fori_loop(0, toks // TCH, turn, 0)
    lax.fori_loop(0, units // 2, unit, 0)
    wait(step[0])
    step[0] = stage2(0)
    wait(step[1])
    step[1] = stage2(1)
    lax.fori_loop(units // 2, units * 3 // 4, unit, 0)
    wait(step[0])
    step[0] = stage3(0)
    wait(step[1])
    step[1] = stage3(1)
    lax.fori_loop(units * 3 // 4, units, unit, 0)
    wait(step[0])
    step[0], last0 = stage4(0)
    wait(step[1])
    step[1], last1 = stage4(1)
    stores = [pltpu.make_async_copy(dw1_ref, dw1_hbm, store_sem.at[0]), pltpu.make_async_copy(flip.at[0], dw2_hbm, store_sem.at[1])]
    stores[0].start()
    for f in range(0, ff, FB):
        flip[0, f : f + FB, :] = dw2t_ref[:, f : f + FB].T
    stores[1].start()
    wait(step[0])
    last0 += stage5(0)
    wait(last0)
    stores += [pltpu.make_async_copy(sum_ref.at[rows(0, dim), :], dwi1_hbm, store_sem.at[2]), pltpu.make_async_copy(flip.at[1], dwi2_hbm, store_sem.at[3])]
    stores[2].start()
    wait(step[1])
    last1 += stage5(1)
    wait(last1)
    for f in range(0, ff, FB):
        flip[1, f : f + FB, :] = sum_ref[dim:, f : f + FB].T
    stores[3].start()
    wait(stores)


def finish_kernel(loss_ref, a_hbm, b_hbm, c_hbm, d_hbm, loss_out, a_out, b_out, c_out, d_out, wide, tall, load_sem, store_sem):
    loads, stores = [], []
    for src, buf, dst in ((a_hbm, wide.at[0], a_out), (b_hbm, tall.at[0], b_out), (c_hbm, wide.at[1], c_out), (d_hbm, tall.at[1], d_out)):
        count = src.shape[0] // 4
        for first in range(0, src.shape[0], count):
            at, k = pl.ds(first, count), len(loads)
            loads.append(pltpu.make_async_copy(src.at[at, :], buf.at[at, :], load_sem.at[k]))
            stores.append(pltpu.make_async_copy(buf.at[at, :], dst.at[at, :], store_sem.at[k]))
    for copy in loads:
        copy.start()
    loss_out[...] = loss_ref[0:1, 0:1]
    for load, store in zip(loads, stores):
        load.wait()
        store.start()
    for copy in stores:
        copy.wait()


def exchange(n, src_ref, all_ref, send_sem, recv_sem):
    me = lax.axis_index("dp")
    barrier = pltpu.get_barrier_semaphore()
    for k in range(1, n):
        pl.semaphore_signal(barrier, inc=1, device_id=(lax.rem(me + k, n),), device_id_type=MESH)
    pl.semaphore_wait(barrier, n - 1)
    copies = []
    for k in range(1, n):
        copies.append(pltpu.make_async_remote_copy(
            src_ref=src_ref, dst_ref=all_ref.at[me], send_sem=send_sem.at[k - 1], recv_sem=recv_sem.at[k - 1],
            device_id=(lax.rem(me + k, n),), device_id_type=MESH))
        copies[-1].start()
    all_ref[me] = src_ref[...]
    return copies


def query_kernel(n, targ_ref, x_hbm, w1_hbm, w2_hbm, all_ref, out_ref, x_ref, w1_ref, w2_ref, load_sem, send_sem, recv_sem):
    loads = [(x_hbm, x_ref), (w1_hbm, w1_ref), (w2_hbm, w2_ref)]
    loads = [pltpu.make_async_copy(src, dst, load_sem.at[i]) for i, (src, dst) in enumerate(loads)]
    for copy in loads:
        copy.start()
    copies = exchange(n, targ_ref, all_ref, send_sem, recv_sem)
    for copy in loads:
        copy.wait()
    out = None
    for f in range(0, w1_ref.shape[1], FB):
        part = dot(gelu(dot(x_ref[...], w1_ref[:, f : f + FB])).astype(BF), w2_ref[f : f + FB, :])
        out = part if out is None else out + part
    out_ref[...] = out.astype(BF)
    for copy in copies:
        copy.wait()


def stats_kernel(n, stat_ref, hit_ref, out_ref, stats, send_sem, recv_sem):
    for copy in exchange(n, stat_ref, stats, send_sem, recv_sem):
        copy.wait()
    toks = stat_ref.shape[1]
    hit = hit_ref[...] > 0.5
    top = jnp.where(hit, HIT_VALUE, -EXCLUDED)
    for i in range(n):
        top = jnp.maximum(top, stats[i, 0:1, :])
    total = jnp.where(hit, jnp.exp(HIT_VALUE - top), 0.0)
    for i in range(n):
        total += stats[i, 1:2, :] * jnp.exp(stats[i, 0:1, :] - top)
    lse = top + jnp.log(total)
    out_ref[0:1, :] = lse
    out_ref[1:2, :] = lse + math.log(toks)
    out_ref[2:3, :] = jnp.where(hit, jnp.exp(HIT_VALUE - (lse + math.log(toks))), 0.0) - 1.0 / toks


def share(kernel, ident, n, ins, out, scratch=()):
    spec = lambda place: pl.BlockSpec(memory_space=pltpu.VMEM if place else pl.ANY)
    return pl.pallas_call(
        functools.partial(kernel, n), out_shape=out, in_specs=[spec(p) for _, p in ins], out_specs=[spec(True) for _ in out],
        scratch_shapes=[*scratch, pltpu.SemaphoreType.DMA((n - 1,)), pltpu.SemaphoreType.DMA((n - 1,))],
        compiler_params=pltpu.CompilerParams(collective_id=ident, has_side_effects=True, vmem_limit_bytes=VMEM_LIMIT),
    )(*[a for a, _ in ins])


def params(**kw):
    return pltpu.CompilerParams(vmem_limit_bytes=VMEM_LIMIT, dimension_semantics=("arbitrary",), **kw)


def cost(flops):
    return pl.CostEstimate(flops=flops, bytes_accessed=64 << 20, transcendentals=0)


def whole(shape):
    return pl.BlockSpec(shape, lambda i, *_: (0,) * len(shape))


def chunk(width):
    return pl.BlockSpec((CH, width), lambda i, *_: (i, 0))


ATTR_CHUNK = pl.BlockSpec((CH // WIN, 8, WIN), lambda i, *_: (i, 0, 0))


def sds(*shape, dtype=F32):
    return jax.ShapeDtypeStruct(shape, dtype)


def solution(mesh):
    num_dev = mesh.shape["dp"]

    def local_step(tokens, w_one, w_two, wi_one, wi_two, table, cand_ids, log_q, targ_loc):
        dim = table.shape[1]
        ff = wi_one.shape[1]
        rows_loc = table.shape[0]
        toks = tokens.shape[0] * num_dev
        cands = cand_ids.shape[0]
        cap = cands + toks
        n_blk = rows_loc // BLK
        scale = SCORE_GAIN / math.sqrt(dim)
        base = lax.axis_index("dp") * rows_loc

        hit = jnp.any(targ_loc[:, None] == cand_ids[None, :], axis=1)
        coded, query_loc = share(
            query_kernel, 0, num_dev, [((2 * targ_loc + hit)[None, :], True), (tokens, False), (w_one, False), (w_two, False)],
            [sds(num_dev, 1, targ_loc.shape[0], dtype=jnp.int32), sds(*tokens.shape, dtype=BF)],
            [pltpu.VMEM(tokens.shape, BF), pltpu.VMEM(w_one.shape, BF), pltpu.VMEM(w_two.shape, BF), pltpu.SemaphoreType.DMA((3,))])
        coded = coded.reshape(toks)
        targ_all, hit_all = coded >> 1, coded & 1
        query = lax.all_gather(query_loc, "dp", axis=0, tiled=True)
        x_all = lax.all_gather(tokens, "dp", axis=0, tiled=True)

        ids = jnp.concatenate([cand_ids, jnp.where(hit_all == 1, -1, targ_all)]) - base
        kind = jnp.concatenate([jnp.zeros((cands,), jnp.int32), jnp.ones((toks,), jnp.int32)])
        key = jnp.where((ids >= 0) & (ids < rows_loc), 2 * ids + kind, 2 * rows_loc)
        offs = jnp.concatenate([log_q, jnp.full((toks,), EXCLUDED, F32)])
        bounds = jnp.arange(n_blk + 1, dtype=jnp.int32) * (2 * BLK)
        starts = jnp.sum((key[None, :] < bounds[:, None]).astype(jnp.int32), axis=1)
        nch = jnp.maximum(lax.div(starts[n_blk] + (CH - 1), CH), 1)
        key_s, offs_s = lax.sort((key, offs), num_keys=1, is_stable=False)
        repeat = jnp.concatenate([jnp.zeros((1,), bool), key_s[1:] == key_s[:-1]])
        used = (key_s < 2 * rows_loc) & ~repeat
        attr = jnp.stack([
            jnp.where(used, (key_s >> 1).astype(F32), NO_ROW),
            jnp.where(used, offs_s, EXCLUDED),
        ])
        attr = jnp.pad(attr, ((0, 6), (0, 0)))
        pad = jnp.broadcast_to(jnp.array([NO_ROW, EXCLUDED, 0, 0, 0, 0, 0, 0], F32)[:, None], (8, CH))
        attr = jnp.concatenate([attr, pad], axis=1).reshape(8, -1, WIN).transpose(1, 0, 2)
        tid = (targ_all - base).astype(F32)[None, :]
        nch1 = nch[None]

        rows = pl.pallas_call(
            gather_kernel,
            grid_spec=pltpu.PrefetchScalarGridSpec(
                num_scalar_prefetch=2, grid=(n_blk // SUB,),
                in_specs=[pl.BlockSpec((SUB * BLK, dim), lambda i, *_: (i, 0)), whole(attr.shape)],
                out_specs=pl.BlockSpec(memory_space=pl.ANY),
                scratch_shapes=[pltpu.VMEM((cap + CH, dim), BF), pltpu.VMEM((cap + CH, WIN), F32), pltpu.SemaphoreType.DMA]),
            out_shape=sds(cap, dim, dtype=BF), compiler_params=params(), cost_estimate=cost(4 * rows_loc * WIN * dim), name="gather",
        )(starts, nch1, table, attr)

        def call(kernel, name, flops, ins, outs, scratch=()):
            spec = lambda place: pl.BlockSpec(memory_space={True: pltpu.VMEM, False: pl.ANY, None: pltpu.SMEM}[place])
            return pl.pallas_call(
                kernel, in_specs=[spec(None)] + [spec(p) for _, p in ins], out_specs=[spec(p) for _, p in outs],
                out_shape=[o for o, _ in outs], scratch_shapes=list(scratch),
                compiler_params=pltpu.CompilerParams(vmem_limit_bytes=VMEM_LIMIT), cost_estimate=cost(flops), name=name,
            )(nch1, *[a for a, _ in ins])

        bf_list, f_list = sds(cap, dim, dtype=BF), sds(cap, ff)
        vec, pre, z, stat = call(
            functools.partial(fwd_kernel, scale), "fwd", 6 * cap * dim * ff // 4,
            [(tid, True), (query, True), (wi_one, True), (wi_two, True), (rows, False), (attr, False)],
            [(bf_list, False), (f_list, False), (sds(cap, toks), False), (sds(2, toks), True)],
            [pltpu.VMEM((8, toks), F32), pltpu.VMEM((8, toks), F32)])

        stat, x_all = lax.optimization_barrier((stat, x_all))
        (stat,) = share(
            stats_kernel, 1, num_dev, [(stat, True), (hit_all.astype(F32)[None, :], True)], [sds(3, toks)],
            [pltpu.VMEM((num_dev, 2, toks), F32)])

        g, dht_part = call(
            functools.partial(logit_back_kernel, scale), "logit_back", 4 * cap * dim * toks // 4,
            [(tid, True), (stat, True), (query, True), (z, False), (vec, False), (attr, False)],
            [(bf_list, False), (sds(dim + 8, toks), True)])

        dht = lax.psum(dht_part, "dp")
        d_table, dwi_part = call(
            tower_back_kernel, "tower_back", 8 * cap * dim * ff // 4,
            [(starts, None), (wi_one, True), (wi_two, True), (attr, True), (g, False), (rows, False), (pre, False)],
            [(sds(rows_loc, dim), False), (sds(2 * dim, ff), True)],
            [pltpu.VMEM((cap + CH, dim), BF), pltpu.VMEM((RING, BLK, dim), F32), pltpu.SMEM((2,), jnp.int32), pltpu.SemaphoreType.DMA((RING,))])

        any_spec = pl.BlockSpec(memory_space=pl.ANY)
        *weight_grads, loss = pl.pallas_call(
            functools.partial(query_back_kernel, scale),
            in_specs=[pl.BlockSpec(memory_space=pltpu.VMEM)] + [any_spec] * 5, out_specs=[any_spec] * 4 + [pl.BlockSpec(memory_space=pltpu.VMEM)],
            out_shape=[sds(dim, ff), sds(ff, dim), sds(dim, ff), sds(ff, dim), sds(8, 128)],
            scratch_shapes=[pltpu.VMEM((8, toks), F32),
                pltpu.VMEM((dim, ff), F32), pltpu.VMEM((dim, ff), F32), pltpu.VMEM((2 * dim, ff), F32), pltpu.VMEM((2, ff, dim), F32),
                pltpu.VMEM((toks, dim), BF), pltpu.VMEM((dim, toks), BF), pltpu.VMEM((dim, toks), F32), pltpu.VMEM((dim, toks), BF),
                pltpu.VMEM((toks, dim), BF), pltpu.VMEM((dim, ff), BF), pltpu.VMEM((ff, dim), BF),
                pltpu.VMEM((2, dim // 2, ff), F32), pltpu.VMEM((2, dim // 2, ff), F32),
                pltpu.VMEM((2, 2, dim // 8, ff), F32), pltpu.VMEM((2, 2, dim // 16, ff), F32),
                pltpu.SemaphoreType.DMA((7,)), pltpu.SemaphoreType.DMA((4,)), pltpu.SemaphoreType.DMA((26,)), pltpu.SemaphoreType.DMA((26,))],
            compiler_params=pltpu.CompilerParams(vmem_limit_bytes=VMEM_LIMIT, collective_id=2, has_side_effects=True),
            cost_estimate=cost(8 * toks * dim * ff), name="query_back",
        )(stat, x_all, dht, w_one, w_two, dwi_part)
        vmem_spec = pl.BlockSpec(memory_space=pltpu.VMEM)
        loss, *weight_grads = pl.pallas_call(
            finish_kernel, in_specs=[vmem_spec] + [any_spec] * 4, out_specs=[vmem_spec] + [any_spec] * 4,
            out_shape=[sds(1, 1)] + [sds(*a.shape) for a in weight_grads],
            scratch_shapes=[pltpu.VMEM((2, dim, ff), F32), pltpu.VMEM((2, ff, dim), F32), pltpu.SemaphoreType.DMA((16,)), pltpu.SemaphoreType.DMA((16,))],
            compiler_params=pltpu.CompilerParams(vmem_limit_bytes=VMEM_LIMIT), name="finish",
        )(loss, *weight_grads)

        return (loss.reshape(()), d_table, *weight_grads)

    return jax.shard_map(local_step, mesh=mesh, in_specs=(P("dp", None), P(), P(), P(), P(), P("dp", None), P(), P(), P("dp")), out_specs=(P(), P("dp", None), P(), P(), P(), P()), check_vma=False)
```
